128 devices in a mesh: sp: 2 (over core), dp: 64 (over z, y, x).
Axes of the slice: x: 4, y: 4, z: 4, core: 2. Of those that a mesh axis runs over, the one named last changes fastest.
Arguments:
- node_lat: bfloat16 [64, 512, 512], P('dp', 'sp')
- edge_lat: bfloat16 [64, 4096, 512], P('dp', 'sp')
- senders: int32 [4096], P('sp')
- edge_mask: int32 [4096], P('sp')
- node_cot: bfloat16 [64, 512, 512], P('dp', 'sp')
- edge_cot: bfloat16 [64, 4096, 512], P('dp', 'sp')
- w_edge1: float32 [2, 1536, 512], P(None, 'dp')
- w_edge2: float32 [2, 512, 512], P(None, 'dp')
- w_node1: float32 [2, 1024, 512], P(None, 'dp')
- w_node2: float32 [2, 512, 512], P(None, 'dp')
- norm_par: float32 [2, 4, 512], P(None, None, 'dp')
- mom_edge1: float32 [2, 1536, 512], P(None, 'dp')
- mom_edge2: float32 [2, 512, 512], P(None, 'dp')
- mom_node1: float32 [2, 1024, 512], P(None, 'dp')
- mom_node2: float32 [2, 512, 512], P(None, 'dp')
- mom_norm: float32 [2, 4, 512], P(None, None, 'dp')
- vel_edge1: float32 [2, 1536, 512], P(None, 'dp')
- vel_edge2: float32 [2, 512, 512], P(None, 'dp')
- vel_node1: float32 [2, 1024, 512], P(None, 'dp')
- vel_node2: float32 [2, 512, 512], P(None, 'dp')
- vel_norm: float32 [2, 4, 512], P(None, None, 'dp')
Outputs:
- output 1: float32 [2, 1536, 512], P(None, 'dp')
- output 2: float32 [2, 512, 512], P(None, 'dp')
- output 3: float32 [2, 1024, 512], P(None, 'dp')
- output 4: float32 [2, 512, 512], P(None, 'dp')
- output 5: float32 [2, 4, 512], P(None, None, 'dp')
- output 6: float32 [2, 1536, 512], P(None, 'dp')
- output 7: float32 [2, 512, 512], P(None, 'dp')
- output 8: float32 [2, 1024, 512], P(None, 'dp')
- output 9: float32 [2, 512, 512], P(None, 'dp')
- output 10: float32 [2, 4, 512], P(None, None, 'dp')
- output 11: float32 [2, 1536, 512], P(None, 'dp')
- output 12: float32 [2, 512, 512], P(None, 'dp')
- output 13: float32 [2, 1024, 512], P(None, 'dp')
- output 14: float32 [2, 512, 512], P(None, 'dp')
- output 15: float32 [2, 4, 512], P(None, None, 'dp')
- output 16: bfloat16 [64, 512, 512], P('dp', 'sp')
- output 17: bfloat16 [64, 4096, 512], P('dp', 'sp')
All inputs are finite; a program needn't handle non-finite values.
Results may differ from the reference program's by a relative error of at most 0.02.
Values are sent between devices in bfloat16 or wider.
A program may use at most 1 GiB of HBM per device.

```python
import jax
import jax.numpy as jnp
from jax import lax

BATCH = 64
TILES = 2
NODES_TILE = 256
DEG = 8
LATENT = 512
HIDDEN = 512
LAYERS = 2
STEP = 10
NODES = TILES * NODES_TILE
EDGES = NODES * DEG
LEARN_RATE = 1e-3
BETA_ONE = 0.9
BETA_TWO = 0.95
ADAM_EPS = 1e-8
DECAY = 0.1
NORM_EPS = 1e-5


def draw_senders(base_key):
    share_key, coin_key, shift_key, local_key = jax.random.split(base_key, 4)
    tile_edges = NODES_TILE * DEG
    share_num = jax.random.randint(share_key, (TILES, 1), 1, 8)
    coin_draw = jax.random.randint(coin_key, (TILES, tile_edges), 0, 16)
    remote = (coin_draw < share_num).astype(jnp.int32)
    tile_shift = jax.random.randint(shift_key, (TILES, tile_edges), 1, TILES)
    own_tile = jnp.arange(TILES, dtype=jnp.int32)[:, None]
    src_tile = (own_tile + remote * tile_shift) % TILES
    local_id = jax.random.randint(local_key, (TILES, tile_edges), 0, NODES_TILE)
    sender_ids = (src_tile * NODES_TILE + local_id).reshape(EDGES).astype(jnp.int32)
    return sender_ids.at[0].set(NODES - 1).at[EDGES - 1].set(0)


def setup_inputs(seed: int = 0) -> dict:
    sub_keys = jax.random.split(jax.random.key(seed), 24)
    lat_shape = (BATCH, NODES, LATENT)
    edge_shape = (BATCH, EDGES, LATENT)
    node_lat = jax.random.normal(sub_keys[0], lat_shape, jnp.float32).astype(jnp.bfloat16)
    edge_lat = jax.random.normal(sub_keys[1], edge_shape, jnp.float32).astype(jnp.bfloat16)
    senders = draw_senders(sub_keys[2])
    edge_mask = (jax.random.randint(sub_keys[3], (EDGES,), 0, 8) != 0).astype(jnp.int32)
    node_cot = jax.random.normal(sub_keys[4], lat_shape, jnp.float32).astype(jnp.bfloat16)
    edge_cot = jax.random.normal(sub_keys[5], edge_shape, jnp.float32).astype(jnp.bfloat16)
    mat_shapes = [(LAYERS, 3 * LATENT, HIDDEN), (LAYERS, HIDDEN, LATENT), (LAYERS, 2 * LATENT, HIDDEN), (LAYERS, HIDDEN, LATENT)]
    masters = [jax.random.normal(sub_keys[6 + slot], mat_shape, jnp.float32) * mat_shape[1] ** -0.5 for slot, mat_shape in enumerate(mat_shapes)]
    norm_base = jnp.array([1.0, 0.0, 1.0, 0.0], jnp.float32)[None, :, None]
    masters.append(norm_base + 0.2 * jax.random.normal(sub_keys[10], (LAYERS, 4, LATENT), jnp.float32))
    edge_rows = float(BATCH * EDGES)
    node_rows = float(BATCH * NODES)
    norm_rows = jnp.array([edge_rows, edge_rows, node_rows, node_rows], jnp.float32)[None, :, None]
    row_counts = [edge_rows, edge_rows, node_rows, node_rows, norm_rows]
    moments_one = [0.1 * jnp.sqrt(row_counts[slot]) * jax.random.normal(sub_keys[11 + slot], masters[slot].shape, jnp.float32) for slot in range(5)]
    moments_two = [0.1 * row_counts[slot] * jax.random.uniform(sub_keys[16 + slot], masters[slot].shape, jnp.float32, 0.5, 1.5) for slot in range(5)]
    return dict(node_lat=node_lat, edge_lat=edge_lat, senders=senders, edge_mask=edge_mask, node_cot=node_cot, edge_cot=edge_cot, w_edge1=masters[0], w_edge2=masters[1], w_node1=masters[2], w_node2=masters[3], norm_par=masters[4], mom_edge1=moments_one[0], mom_edge2=moments_one[1], mom_node1=moments_one[2], mom_node2=moments_one[3], mom_norm=moments_one[4], vel_edge1=moments_two[0], vel_edge2=moments_two[1], vel_node1=moments_two[2], vel_node2=moments_two[3], vel_norm=moments_two[4])


def snap_bf16(values):
    return values.astype(jnp.bfloat16).astype(jnp.float32)


def layer_norm(values, norm_gain, norm_bias):
    row_mean = jnp.mean(values, axis=-1, keepdims=True)
    centered = values - row_mean
    row_var = jnp.mean(centered * centered, axis=-1, keepdims=True)
    return centered * lax.rsqrt(row_var + NORM_EPS) * norm_gain + norm_bias


def mlp_branch(features, w_one, w_two, norm_gain, norm_bias):
    pre_act = snap_bf16(jnp.dot(features, w_one, preferred_element_type=jnp.float32))
    hidden_act = snap_bf16(jax.nn.silu(pre_act))
    out_b = snap_bf16(jnp.dot(hidden_act, w_two, preferred_element_type=jnp.float32))
    return layer_norm(out_b, norm_gain, norm_bias)


def processor_layer(layer_carry, layer_wts, senders, mask_f):
    node_x, edge_x = layer_carry
    w_e1, w_e2, w_n1, w_n2, norm_rows = layer_wts
    sender_lat = jnp.take(node_x, senders, axis=0)
    recv_lat = jnp.repeat(node_x, DEG, axis=0)
    edge_in = jnp.concatenate([edge_x, sender_lat, recv_lat], axis=1)
    edge_new = snap_bf16(edge_x + mlp_branch(edge_in, w_e1, w_e2, norm_rows[0], norm_rows[1]))
    node_sum = snap_bf16(jnp.sum((edge_new * mask_f[:, None]).reshape(NODES, DEG, LATENT), axis=1))
    node_in = jnp.concatenate([node_x, node_sum], axis=1)
    node_new = snap_bf16(node_x + mlp_branch(node_in, w_n1, w_n2, norm_rows[2], norm_rows[3]))
    return node_new, edge_new


def sample_objective(all_wts, node_b, edge_b, node_g, edge_g, senders, mask_f):
    def layer_step(layer_carry, layer_wts):
        return processor_layer(layer_carry, layer_wts, senders, mask_f), None
    final_carry, _ = lax.scan(layer_step, (node_b.astype(jnp.float32), edge_b.astype(jnp.float32)), all_wts)
    node_out, edge_out = final_carry
    return jnp.sum(node_out * node_g.astype(jnp.float32)) + jnp.sum(edge_out * edge_g.astype(jnp.float32))


def adamw_update(master, grad_sum, moment_one, moment_two):
    corr_one = 1.0 - BETA_ONE ** STEP
    corr_two = 1.0 - BETA_TWO ** STEP
    one_new = BETA_ONE * moment_one + (1.0 - BETA_ONE) * grad_sum
    two_new = BETA_TWO * moment_two + (1.0 - BETA_TWO) * grad_sum * grad_sum
    direction = (one_new / corr_one) / (jnp.sqrt(two_new / corr_two) + ADAM_EPS)
    return master - LEARN_RATE * (direction + DECAY * master), one_new, two_new


def reference(node_lat, edge_lat, senders, edge_mask, node_cot, edge_cot, w_edge1, w_edge2, w_node1, w_node2, norm_par, mom_edge1, mom_edge2, mom_node1, mom_node2, mom_norm, vel_edge1, vel_edge2, vel_node1, vel_node2, vel_norm):
    masters = (w_edge1, w_edge2, w_node1, w_node2, norm_par)
    moments_one = (mom_edge1, mom_edge2, mom_node1, mom_node2, mom_norm)
    moments_two = (vel_edge1, vel_edge2, vel_node1, vel_node2, vel_norm)
    compute = tuple(snap_bf16(master) for master in masters)
    mask_f = edge_mask.astype(jnp.float32)

    def per_sample(grad_total, sample):
        node_b, edge_b, node_g, edge_g = sample

        def objective(all_wts, node_in, edge_in):
            return sample_objective(all_wts, node_in, edge_in, node_g, edge_g, senders, mask_f)
        _, pullback = jax.vjp(objective, compute, node_b, edge_b)
        d_wts, d_node, d_edge = pullback(jnp.ones((), jnp.float32))
        grad_total = tuple(run_sum + part for run_sum, part in zip(grad_total, d_wts))
        return grad_total, (d_node, d_edge)

    zero_grads = tuple(jnp.zeros_like(weight) for weight in compute)
    grads, sample_grads = lax.scan(per_sample, zero_grads, (node_lat, edge_lat, node_cot, edge_cot))
    new_state = [adamw_update(masters[slot], grads[slot], moments_one[slot], moments_two[slot]) for slot in range(5)]
    return (new_state[0][0], new_state[1][0], new_state[2][0], new_state[3][0], new_state[4][0], new_state[0][1], new_state[1][1], new_state[2][1], new_state[3][1], new_state[4][1], new_state[0][2], new_state[1][2], new_state[2][2], new_state[3][2], new_state[4][2], sample_grads[0], sample_grads[1])
```

```python
import functools

import jax
import jax.numpy as jnp
from jax import lax
from jax.experimental import pallas as pl
from jax.experimental.pallas import tpu as pltpu
from jax.sharding import PartitionSpec as P

NORM_EPS = 1e-5
LEARN_RATE = 1e-3
BETA_ONE = 0.9
BETA_TWO = 0.95
ADAM_EPS = 1e-8
DECAY = 0.1
STEP = 10


def contract(left_op, right_op, left_dims, right_dims):
    return lax.dot_general(left_op, right_op, ((left_dims, right_dims), ((), ())), preferred_element_type=jnp.float32)


def norm_forward(out_b, norm_gain, norm_bias):
    values = out_b.astype(jnp.float32)
    centered = values - jnp.mean(values, axis=-1, keepdims=True)
    inv_std = lax.rsqrt(jnp.mean(centered * centered, axis=-1, keepdims=True) + NORM_EPS)
    normed = centered * inv_std
    return normed * norm_gain + norm_bias, normed, inv_std


def mlp_tail(pre_act, w_two, norm_gain, norm_bias):
    pre_b = pre_act.astype(jnp.bfloat16)
    hidden_act = jax.nn.silu(pre_b.astype(jnp.float32)).astype(jnp.bfloat16)
    last_dim = hidden_act.ndim - 1
    out_b = contract(hidden_act, w_two, (last_dim,), (0,)).astype(jnp.bfloat16)
    branch, normed, inv_std = norm_forward(out_b, norm_gain, norm_bias)
    return branch, (pre_b, hidden_act, normed, inv_std)


def mlp_back(d_branch, saved, w_one, w_two, norm_gain):
    pre_b, hidden_act, normed, inv_std = saved
    last_dim = hidden_act.ndim - 1
    lead_dims = tuple(range(last_dim))
    d_gain = jnp.sum(d_branch * normed, axis=lead_dims)
    d_bias = jnp.sum(d_branch, axis=lead_dims)
    d_norm = d_branch * norm_gain
    d_out = (inv_std * (d_norm - jnp.mean(d_norm, axis=-1, keepdims=True) - normed * jnp.mean(d_norm * normed, axis=-1, keepdims=True))).astype(jnp.bfloat16)
    d_two = contract(hidden_act, d_out, lead_dims, lead_dims)
    d_act = contract(d_out, w_two, (last_dim,), (1,)).astype(jnp.bfloat16)
    pre_f = pre_b.astype(jnp.float32)
    gate_sig = jax.nn.sigmoid(pre_f)
    d_pre = (d_act.astype(jnp.float32) * gate_sig * (1.0 + pre_f * (1.0 - gate_sig))).astype(jnp.bfloat16)
    d_in = contract(d_pre, w_one, (last_dim,), (1,))
    return d_pre, d_in, d_two, d_gain, d_bias


def layer_forward(node_x, node_all, edge_x, senders, mask_b, layer_wts):
    w_e1, w_e2, w_n1, w_n2, norm_rows = layer_wts
    lat_width = node_x.shape[-1]
    sender_lat = jnp.take(node_all, senders, axis=1).reshape(edge_x.shape)
    pre_e = (contract(edge_x, w_e1[:lat_width], (3,), (0,))
             + contract(sender_lat, w_e1[lat_width:2 * lat_width], (3,), (0,))
             + contract(node_x, w_e1[2 * lat_width:], (2,), (0,))[:, :, None, :])
    branch_e, saved_e = mlp_tail(pre_e, w_e2, norm_rows[0], norm_rows[1])
    edge_new = (edge_x.astype(jnp.float32) + branch_e).astype(jnp.bfloat16)
    node_sum = jnp.einsum('bngd,ng->bnd', edge_new, mask_b, preferred_element_type=jnp.float32).astype(jnp.bfloat16)
    pre_n = contract(node_x, w_n1[:lat_width], (2,), (0,)) + contract(node_sum, w_n1[lat_width:], (2,), (0,))
    branch_n, saved_n = mlp_tail(pre_n, w_n2, norm_rows[2], norm_rows[3])
    node_new = (node_x.astype(jnp.float32) + branch_n).astype(jnp.bfloat16)
    return node_new, edge_new, (sender_lat, node_sum, saved_e, saved_n)


def layer_backward(d_node_new, d_edge_new, node_x, edge_x, senders, mask_f, saved, layer_wts, total_nodes):
    w_e1, w_e2, w_n1, w_n2, norm_rows = layer_wts
    sender_lat, node_sum, saved_e, saved_n = saved
    batch_size, tile_nodes, degree, lat_width = edge_x.shape
    d_res_n = d_node_new.astype(jnp.float32)
    d_pre_n, d_in_n, d_wn2, d_gain_n, d_bias_n = mlp_back(d_res_n, saved_n, w_n1, w_n2, norm_rows[2])
    d_wn1 = jnp.concatenate([contract(node_x, d_pre_n, (0, 1), (0, 1)), contract(node_sum, d_pre_n, (0, 1), (0, 1))], axis=0)
    d_sum = d_in_n[..., lat_width:].astype(jnp.bfloat16)
    d_res_e = (d_edge_new.astype(jnp.float32) + d_sum.astype(jnp.float32)[:, :, None, :] * mask_f[None, :, :, None]).astype(jnp.bfloat16).astype(jnp.float32)
    d_pre_e, d_in_e, d_we2, d_gain_e, d_bias_e = mlp_back(d_res_e, saved_e, w_e1, w_e2, norm_rows[0])
    recv_grad = contract(node_x, d_pre_e.reshape(batch_size, tile_nodes, -1), (0, 1), (0, 1))
    d_we1 = jnp.concatenate([contract(edge_x, d_pre_e, (0, 1, 2), (0, 1, 2)), contract(sender_lat, d_pre_e, (0, 1, 2), (0, 1, 2)), recv_grad.reshape(lat_width, degree, -1).sum(axis=1)], axis=0)
    d_edge_x = (d_res_e + d_in_e[..., :lat_width]).astype(jnp.bfloat16)
    d_sender = d_in_e[..., lat_width:2 * lat_width].reshape(batch_size, tile_nodes * degree, lat_width)
    scattered = jnp.zeros((batch_size, total_nodes, lat_width), jnp.float32).at[:, senders].add(d_sender)
    d_local = d_res_n + d_in_n[..., :lat_width] + d_in_e[..., 2 * lat_width:].sum(axis=2)
    grads = (d_we1, d_we2, d_wn1, d_wn2, jnp.stack([d_gain_e, d_bias_e, d_gain_n, d_bias_n]))
    return d_local, scattered, d_edge_x, grads


def adamw_update(master, grad_sum, moment_one, moment_two):
    corr_one = 1.0 - BETA_ONE ** STEP
    corr_two = 1.0 - BETA_TWO ** STEP
    one_new = BETA_ONE * moment_one + (1.0 - BETA_ONE) * grad_sum
    two_new = BETA_TWO * moment_two + (1.0 - BETA_TWO) * grad_sum * grad_sum
    direction = (one_new / corr_one) / (jnp.sqrt(two_new / corr_two) + ADAM_EPS)
    return master - LEARN_RATE * (direction + DECAY * master), one_new, two_new


def update_all(masters, moments_one, moments_two, layer_grads):
    new_master = []
    new_one = []
    new_two = []
    for slot in range(len(masters)):
        grad_sum = jnp.stack([per_layer[slot] for per_layer in layer_grads], axis=0)
        master_new, one_new, two_new = adamw_update(masters[slot], grad_sum, moments_one[slot], moments_two[slot])
        new_master.append(master_new)
        new_one.append(one_new)
        new_two.append(two_new)
    return tuple(new_master) + tuple(new_one) + tuple(new_two)


MESH_ID = pl.DeviceIdType.MESH
ORDERS = ((0, 1, 2), (1, 2, 0), (2, 0, 1))
RING = 4


class Place:
    def __init__(self):
        chip = lax.axis_index('dp')
        self.core = lax.axis_index('sp')
        self.at = (lax.rem(chip // 16, 4), lax.rem(chip // 4, 4), lax.rem(chip, 4))

    def step(self, dim, delta):
        return lax.rem(self.at[dim] + (delta + RING), RING)

    def chip(self, dim, delta):
        pos = list(self.at)
        pos[dim] = self.step(dim, delta)
        return {'dp': pos[0] * 16 + pos[1] * 4 + pos[2]}

    def partner(self):
        return {'sp': 1 - self.core}

    def barrier(self):
        sem = pltpu.get_barrier_semaphore()
        for dim in range(3):
            for delta in (1, -1):
                pl.semaphore_signal(sem, inc=1, device_id=self.chip(dim, delta), device_id_type=MESH_ID)
        pl.semaphore_signal(sem, inc=1, device_id=self.partner(), device_id_type=MESH_ID)
        pl.semaphore_wait(sem, 7)


def split_groups(count):
    base, extra = divmod(count, 3)
    sizes = [base + (1 if g < extra else 0) for g in range(3)]
    starts = [sum(sizes[:g]) for g in range(3)]
    return list(zip(starts, sizes))


def gather_kernel(tiles, src_ref, out_ref, send_sem, recv_sem):
    place = Place()
    half = tiles // 2
    first = place.core * half
    out_ref[place.at[0], place.at[1], place.at[2]] = src_ref[...]
    place.barrier()
    pending = []
    from_partner = []
    counter = [0]

    def send(src, dst, where):
        slot = counter[0]
        counter[0] += 1
        copy = pltpu.make_async_remote_copy(src_ref=src, dst_ref=dst, send_sem=send_sem.at[slot], recv_sem=recv_sem.at[slot], device_id=where, device_id_type=MESH_ID)
        copy.start()
        pending.append(copy)
        return copy

    groups = split_groups(half)

    def region(g, phase, j, side=None):
        order = ORDERS[g]
        start, size = groups[g]
        index = list(place.at)
        for q in range(phase):
            index[order[q]] = pl.ds(0, RING)
        index[order[phase]] = j
        lo, n = start, size
        if side is not None:
            if phase == 0:
                cut = (size + 1) // 2
                lo, n = (start, cut) if side == 0 else (start + cut, size - cut)
            else:
                index[order[0]] = pl.ds(2 * side, 2)
        return out_ref.at[index[0], index[1], index[2], pl.ds(first + lo, n)]

    def share(g, phase, j, side=None):
        piece = region(g, phase, j, side)
        from_partner.append(send(piece, piece, place.partner()))

    flight = {}
    for phase in range(3):
        for g in range(3):
            dim = ORDERS[g][phase]
            piece = region(g, phase, place.at[dim])
            origin = piece
            if phase == 0:
                origin = src_ref.at[pl.ds(first + groups[g][0], groups[g][1])]
            flight[g] = (send(origin, piece, place.chip(dim, 1)), send(origin, piece, place.chip(dim, -1)))
        for g in range(3):
            dim = ORDERS[g][phase]
            from_left, from_right = flight[g]
            from_left.wait_recv()
            piece = region(g, phase, place.step(dim, -1), 0)
            onward_right = send(piece, piece, place.chip(dim, 1))
            from_right.wait_recv()
            piece = region(g, phase, place.step(dim, 1), 1)
            onward_left = send(piece, piece, place.chip(dim, -1))
            flight[g] = (onward_right, onward_left)
            share(g, phase, place.step(dim, -1))
            share(g, phase, place.step(dim, 1))
        for g in range(3):
            dim = ORDERS[g][phase]
            far = place.step(dim, 2)
            flight[g][0].wait_recv()
            flight[g][1].wait_recv()
            share(g, phase, far)
    for copy in from_partner:
        copy.wait_recv()
    for copy in pending:
        copy.wait_send()


def gather_tiles(shard, collective_id):
    tiles = shard.shape[0]
    copies = 3 * 3 * (4 + 3)
    return pl.pallas_call(
        functools.partial(gather_kernel, tiles),
        out_shape=jax.ShapeDtypeStruct((RING, RING, RING) + shard.shape, shard.dtype),
        in_specs=[pl.BlockSpec(memory_space=pltpu.VMEM)],
        out_specs=pl.BlockSpec(memory_space=pltpu.VMEM),
        scratch_shapes=[pltpu.SemaphoreType.DMA((copies,)), pltpu.SemaphoreType.DMA((copies,))],
        compiler_params=pltpu.CompilerParams(collective_id=collective_id, has_side_effects=True, vmem_limit_bytes=40 * 2 ** 20),
        name='gather_tiles',
    )(shard)


def reduce_kernel(tiles, src_ref, out_ref, own, theirs, *rest):
    boxes = rest[:9]
    load_sem, send_sem, recv_sem = rest[9:]
    place = Place()
    half = tiles // 2
    first = place.core * half
    other = (1 - place.core) * half
    groups = split_groups(half)
    pending = []
    counter = [0]

    def send(src, dst, where):
        slot = counter[0]
        counter[0] += 1
        copy = pltpu.make_async_remote_copy(src_ref=src, dst_ref=dst, send_sem=send_sem.at[slot], recv_sem=recv_sem.at[slot], device_id=where, device_id_type=MESH_ID)
        copy.start()
        pending.append(copy)
        return copy

    def index_of(g, phase, j, side=None):
        order = ORDERS[g]
        start, size = groups[g]
        index = [pl.ds(0, RING)] * 3
        for q in range(phase):
            index[order[q]] = place.at[order[q]]
        index[order[phase]] = j
        lo, n = start, size
        if side is not None:
            if phase < 2:
                index[order[phase + 1]] = pl.ds(2 * side, 2)
            else:
                cut = (size + 1) // 2
                lo, n = (start, cut) if side == 0 else (start + cut, size - cut)
        return index, lo, n

    def in_own(ref, g, phase, j, side=None):
        index, lo, n = index_of(g, phase, j, side)
        return ref.at[index[0], index[1], index[2], pl.ds(lo, n)]

    loads = {}
    for turn, delta in enumerate((2, 1, -1, 0)):
        for g in range(3):
            j = place.step(ORDERS[g][0], delta)
            index, lo, n = index_of(g, 0, j)
            load = pltpu.make_async_copy(src_ref.at[index[0], index[1], index[2], pl.ds(first + lo, n)], in_own(own, g, 0, j), load_sem.at[turn * 3 + g])
            load.start()
            loads[turn, g] = load
    place.barrier()
    swaps = {}
    for turn, delta in enumerate((2, 1, -1, 0)):
        for g in range(3):
            j = place.step(ORDERS[g][0], delta)
            index, lo, n = index_of(g, 0, j)
            swaps[turn, g] = send(src_ref.at[index[0], index[1], index[2], pl.ds(other + lo, n)], in_own(theirs, g, 0, j), place.partner())

    def add_into(target, addend):
        target[...] = target[...] + addend[...]

    def ready(turn, g):
        delta = (2, 1, -1, 0)[turn]
        loads[turn, g].wait()
        swaps[turn, g].wait_recv()
        j = place.step(ORDERS[g][0], delta)
        add_into(in_own(own, g, 0, j), in_own(theirs, g, 0, j))

    def box(g, phase, slot, side):
        ref = boxes[g * 3 + phase]
        if phase < 2:
            return ref.at[slot]
        size = groups[g][1]
        cut = (size + 1) // 2
        return ref.at[slot, pl.ds(0, cut if side == 0 else size - cut)]

    for phase in range(3):
        flight = {}
        dims = [ORDERS[g][phase] for g in range(3)]

        def start(g, name, j_delta, side, slot, toward):
            j = place.step(dims[g], j_delta)
            flight[g, name] = send(in_own(own, g, phase, j, side), box(g, phase, slot, side), place.chip(dims[g], toward))

        for g in range(3):
            if phase == 0:
                ready(0, g)
            start(g, 'far_right', 2, 0, 0, 1)
            start(g, 'far_left', 2, 1, 2, -1)
        for g in range(3):
            if phase == 0:
                ready(1, g)
            start(g, 'near_right', 1, 1, 1, 1)
            if phase == 0:
                ready(2, g)
            start(g, 'near_left', -1, 0, 3, -1)
        for g in range(3):
            flight[g, 'far_right'].wait_recv()
            add_into(in_own(own, g, phase, place.step(dims[g], 1), 0), box(g, phase, 0, 0))
            start(g, 'sum_right', 1, 0, 4, 1)
            flight[g, 'far_left'].wait_recv()
            add_into(in_own(own, g, phase, place.step(dims[g], -1), 1), box(g, phase, 2, 1))
            start(g, 'sum_left', -1, 1, 5, -1)
        if phase == 0:
            for g in range(3):
                ready(3, g)
        for g in range(3):
            here = place.at[dims[g]]
            for name, slot, side in (('near_left', 3, 0), ('near_right', 1, 1)):
                flight[g, name].wait_recv()
                add_into(in_own(own, g, phase, here, side), box(g, phase, slot, side))
            for name, slot, side in (('sum_right', 4, 0), ('sum_left', 5, 1)):
                flight[g, name].wait_recv()
                add_into(in_own(own, g, phase, here, side), box(g, phase, slot, side))
    out_ref[pl.ds(first, half)] = own[place.at[0], place.at[1], place.at[2]]
    piece = out_ref.at[pl.ds(first, half)]
    send(piece, piece, place.partner()).wait_recv()
    for copy in pending:
        copy.wait_send()


def reduce_tiles(partials, collective_id):
    tiles = partials.shape[3]
    half = tiles // 2
    groups = split_groups(half)
    box_shapes = []
    for g in range(3):
        order = ORDERS[g]
        size = groups[g][1]
        dims = {dim: RING for dim in range(3) if dim != order[0]}
        dims[order[1]] = 2
        box_shapes.append((6,) + tuple(dims[dim] for dim in sorted(dims)) + (size, 8, 128))
        box_shapes.append((6, 2, size, 8, 128))
        box_shapes.append((6, (size + 1) // 2, 8, 128))
    copies = 12 + 3 * 3 * 6 + 1
    return pl.pallas_call(
        functools.partial(reduce_kernel, tiles),
        out_shape=jax.ShapeDtypeStruct((tiles, 8, 128), jnp.float32),
        in_specs=[pl.BlockSpec(memory_space=pl.ANY)],
        out_specs=pl.BlockSpec(memory_space=pltpu.VMEM),
        scratch_shapes=[pltpu.VMEM((RING, RING, RING, half, 8, 128), jnp.float32)] * 2 + [pltpu.VMEM(shape, jnp.float32) for shape in box_shapes] + [pltpu.SemaphoreType.DMA((12,)), pltpu.SemaphoreType.DMA((copies,)), pltpu.SemaphoreType.DMA((copies,))],
        compiler_params=pltpu.CompilerParams(collective_id=collective_id, has_side_effects=True, vmem_limit_bytes=56 * 2 ** 20),
        name='reduce_tiles',
    )(partials)


SHARD_ROWS = (24, 8, 16, 8)


def rows_to_tiles(values, sub):
    lead = values.shape[:-2]
    rows = values.shape[-2]
    cut = values.reshape(lead + (rows // sub, sub, 4, 128))
    n = len(lead)
    return jnp.moveaxis(cut, n + 2, n + 1).reshape(lead + (rows // sub * 4, sub, 128))


def tiles_to_rows(tiles):
    lead = tiles.shape[:-3]
    count, sub = tiles.shape[-3:-1]
    n = len(lead)
    cut = tiles.reshape(lead + (count // 4, 4, sub, 128))
    return jnp.moveaxis(cut, n + 1, n + 2).reshape(lead + (count // 4 * sub, 512))


def gather_weights(masters):
    rows = jnp.concatenate([masters[slot][layer] for layer in range(2) for slot in range(4)], axis=0).astype(jnp.bfloat16)
    norms = jnp.pad(masters[4].astype(jnp.bfloat16).reshape(1, 64), ((0, 15), (0, 64)))[None]
    shard = jnp.concatenate([rows_to_tiles(rows, 16), norms, jnp.zeros_like(norms)], axis=0)
    full = gather_tiles(shard, 1).reshape(64, 30, 16, 128)
    rows = tiles_to_rows(full[:, :28])
    norms = full[:, 28, 0, :64].reshape(64, 2, 4, 8).transpose(1, 2, 0, 3).reshape(2, 4, 512).astype(jnp.float32)
    layers = []
    first = 0
    for layer in range(2):
        mats = []
        for size in SHARD_ROWS:
            mats.append(rows[:, first:first + size].reshape(64 * size, 512))
            first += size
        layers.append(tuple(mats) + (norms[layer],))
    return layers


def reduce_grads(layer_grads):
    parts = []
    for grads in layer_grads:
        for slot, size in enumerate(SHARD_ROWS):
            parts.append(rows_to_tiles(grads[slot].reshape(64, size, 512), 8))
    norms = jnp.stack([grads[4] for grads in layer_grads]).reshape(8, 64, 8).transpose(1, 0, 2).reshape(64, 1, 64)
    norms = jnp.pad(norms, ((0, 0), (0, 7), (0, 64)))[:, None]
    parts += [norms, jnp.zeros_like(norms)]
    partials = jnp.concatenate(parts, axis=1).reshape(4, 4, 4, 58, 8, 128)
    total = reduce_tiles(partials, 2)
    rows = tiles_to_rows(total[:56])
    norms = total[56, 0, :64].reshape(2, 4, 8)
    out = []
    first = 0
    for layer in range(2):
        mats = []
        for size in SHARD_ROWS:
            mats.append(rows[first:first + size])
            first += size
        out.append(tuple(mats) + (norms[layer],))
    return out


def solution(mesh):
    lat_spec = P('dp', 'sp', None)
    edge_spec = P('sp')
    mat_spec = P(None, 'dp', None)
    norm_spec = P(None, None, 'dp')
    param_specs = (mat_spec, mat_spec, mat_spec, mat_spec, norm_spec)
    tile_count = mesh.shape['sp']

    def train_step(node_lat, edge_lat, senders, edge_mask, node_cot, edge_cot, w_edge1, w_edge2, w_node1, w_node2, norm_par, mom_edge1, mom_edge2, mom_node1, mom_node2, mom_norm, vel_edge1, vel_edge2, vel_node1, vel_node2, vel_norm):
        masters = (w_edge1, w_edge2, w_node1, w_node2, norm_par)
        moments_one = (mom_edge1, mom_edge2, mom_node1, mom_node2, mom_norm)
        moments_two = (vel_edge1, vel_edge2, vel_node1, vel_node2, vel_norm)
        batch_size, tile_nodes, lat_width = node_lat.shape
        degree = edge_lat.shape[1] // tile_nodes
        total_nodes = tile_nodes * tile_count
        layers = w_edge1.shape[0]
        mask_f = edge_mask.astype(jnp.float32).reshape(tile_nodes, degree)
        mask_b = mask_f.astype(jnp.bfloat16)
        node_x = node_lat
        edge_x = edge_lat.reshape(batch_size, tile_nodes, degree, lat_width)
        records = []
        weights = gather_weights(masters)
        for layer_idx in range(layers):
            layer_wts = weights[layer_idx]
            node_all = lax.all_gather(node_x, 'sp', axis=1, tiled=True)
            node_new, edge_new, saved = layer_forward(node_x, node_all, edge_x, senders, mask_b, layer_wts)
            records.append((node_x, edge_x, saved))
            node_x = node_new
            edge_x = edge_new
        d_node = node_cot
        d_edge = edge_cot.reshape(batch_size, tile_nodes, degree, lat_width)
        grads_rev = []
        for layer_idx in reversed(range(layers)):
            layer_wts = weights[layer_idx]
            node_in, edge_in, saved = records[layer_idx]
            d_local, scattered, d_edge, grads = layer_backward(d_node, d_edge, node_in, edge_in, senders, mask_f, saved, layer_wts, total_nodes)
            returned = lax.psum_scatter(scattered, 'sp', scatter_dimension=1, tiled=True)
            d_node = (d_local + returned).astype(jnp.bfloat16)
            grads_rev.append(grads)
        new_state = update_all(masters, moments_one, moments_two, reduce_grads(grads_rev[::-1]))
        return new_state + (d_node, d_edge.reshape(edge_lat.shape))

    return jax.shard_map(train_step, mesh=mesh, in_specs=(lat_spec, lat_spec, edge_spec, edge_spec, lat_spec, lat_spec) + param_specs + param_specs + param_specs, out_specs=param_specs + param_specs + param_specs + (lat_spec, lat_spec), check_vma=False)
```

```python
import functools

import jax
import jax.numpy as jnp
from jax import lax
from jax.experimental import pallas as pl
from jax.experimental.pallas import tpu as pltpu
from jax.sharding import PartitionSpec as P

NORM_EPS = 1e-5
LEARN_RATE = 1e-3
BETA_ONE = 0.9
BETA_TWO = 0.95
ADAM_EPS = 1e-8
DECAY = 0.1
STEP = 10
SHARD_ROWS = (24, 8, 16, 8)

MESH_ID = pl.DeviceIdType.MESH
ORDERS = ((0, 1, 2), (1, 2, 0), (2, 0, 1))
RING = 4


class Place:
    def __init__(self):
        chip = lax.axis_index('dp')
        self.core = lax.axis_index('sp')
        self.at = (lax.rem(chip // 16, 4), lax.rem(chip // 4, 4), lax.rem(chip, 4))

    def step(self, dim, delta):
        return lax.rem(self.at[dim] + (delta + RING), RING)

    def chip(self, dim, delta):
        pos = list(self.at)
        pos[dim] = self.step(dim, delta)
        return {'dp': pos[0] * 16 + pos[1] * 4 + pos[2]}

    def partner(self):
        return {'sp': 1 - self.core}

    def barrier(self):
        sem = pltpu.get_barrier_semaphore()
        for dim in range(3):
            for delta in (1, -1):
                pl.semaphore_signal(sem, inc=1, device_id=self.chip(dim, delta), device_id_type=MESH_ID)
        pl.semaphore_signal(sem, inc=1, device_id=self.partner(), device_id_type=MESH_ID)
        pl.semaphore_wait(sem, 7)


def split_groups(count):
    base, extra = divmod(count, 3)
    sizes = [base + (1 if g < extra else 0) for g in range(3)]
    starts = [sum(sizes[:g]) for g in range(3)]
    return list(zip(starts, sizes))


def gather_kernel(tiles, src_ref, out_ref, send_sem, recv_sem):
    place = Place()
    half = tiles // 2
    first = place.core * half
    out_ref[place.at[0], place.at[1], place.at[2]] = src_ref[...]
    place.barrier()
    pending = []
    from_partner = []
    counter = [0]

    def send(src, dst, where):
        slot = counter[0]
        counter[0] += 1
        copy = pltpu.make_async_remote_copy(src_ref=src, dst_ref=dst, send_sem=send_sem.at[slot], recv_sem=recv_sem.at[slot], device_id=where, device_id_type=MESH_ID)
        copy.start()
        pending.append(copy)
        return copy

    groups = split_groups(half)

    def region(g, phase, j, side=None):
        order = ORDERS[g]
        start, size = groups[g]
        index = list(place.at)
        for q in range(phase):
            index[order[q]] = pl.ds(0, RING)
        index[order[phase]] = j
        lo, n = start, size
        if side is not None:
            if phase == 0:
                cut = (size + 1) // 2
                lo, n = (start, cut) if side == 0 else (start + cut, size - cut)
            else:
                index[order[0]] = pl.ds(2 * side, 2)
        return out_ref.at[index[0], index[1], index[2], pl.ds(first + lo, n)]

    def share(g, phase, j, side=None):
        piece = region(g, phase, j, side)
        from_partner.append(send(piece, piece, place.partner()))

    flight = {}
    for phase in range(3):
        for g in range(3):
            dim = ORDERS[g][phase]
            piece = region(g, phase, place.at[dim])
            origin = piece
            if phase == 0:
                origin = src_ref.at[pl.ds(first + groups[g][0], groups[g][1])]
            flight[g] = (send(origin, piece, place.chip(dim, 1)), send(origin, piece, place.chip(dim, -1)))
        for g in range(3):
            dim = ORDERS[g][phase]
            from_left, from_right = flight[g]
            from_left.wait_recv()
            piece = region(g, phase, place.step(dim, -1), 0)
            onward_right = send(piece, piece, place.chip(dim, 1))
            from_right.wait_recv()
            piece = region(g, phase, place.step(dim, 1), 1)
            onward_left = send(piece, piece, place.chip(dim, -1))
            flight[g] = (onward_right, onward_left)
            share(g, phase, place.step(dim, -1))
            share(g, phase, place.step(dim, 1))
        for g in range(3):
            dim = ORDERS[g][phase]
            far = place.step(dim, 2)
            flight[g][0].wait_recv()
            flight[g][1].wait_recv()
            share(g, phase, far)
    for copy in from_partner:
        copy.wait_recv()
    for copy in pending:
        copy.wait_send()


def gather_tiles(shard, collective_id):
    tiles = shard.shape[0]
    copies = 3 * 3 * (4 + 3)
    return pl.pallas_call(
        functools.partial(gather_kernel, tiles),
        out_shape=jax.ShapeDtypeStruct((RING, RING, RING) + shard.shape, shard.dtype),
        in_specs=[pl.BlockSpec(memory_space=pltpu.VMEM)],
        out_specs=pl.BlockSpec(memory_space=pltpu.VMEM),
        scratch_shapes=[pltpu.SemaphoreType.DMA((copies,)), pltpu.SemaphoreType.DMA((copies,))],
        compiler_params=pltpu.CompilerParams(collective_id=collective_id, has_side_effects=True, vmem_limit_bytes=40 * 2 ** 20),
        name='gather_tiles',
    )(shard)


def reduce_kernel(low_ref, high_ref, norm_ref, out_ref, own, theirs, *rest):
    boxes = rest[:9]
    load_sem, send_sem, recv_sem = rest[9:]
    place = Place()
    half = 29
    groups = split_groups(half)
    pending = []
    loaded = []
    counter = [0]

    def send(src, dst, where):
        slot = counter[0]
        counter[0] += 1
        copy = pltpu.make_async_remote_copy(src_ref=src, dst_ref=dst, send_sem=send_sem.at[slot], recv_sem=recv_sem.at[slot], device_id=where, device_id_type=MESH_ID)
        copy.start()
        pending.append(copy)
        return copy

    def index_of(g, phase, j, side=None):
        order = ORDERS[g]
        start, size = groups[g]
        index = [pl.ds(0, RING)] * 3
        for q in range(phase):
            index[order[q]] = place.at[order[q]]
        index[order[phase]] = j
        lo, n = start, size
        if side is not None:
            if phase < 2:
                index[order[phase + 1]] = pl.ds(2 * side, 2)
            else:
                cut = (size + 1) // 2
                lo, n = (start, cut) if side == 0 else (start + cut, size - cut)
        return index, lo, n

    def in_own(ref, g, phase, j, side=None):
        index, lo, n = index_of(g, phase, j, side)
        return ref.at[index[0], index[1], index[2], pl.ds(lo, n)]

    def sources(g, index, core):
        lo, n = groups[g]
        pieces = []
        for ref, begin in ((low_ref, 0), (high_ref, 14)):
            start, stop = max(lo, begin), min(lo + n, begin + 14)
            if start < stop:
                pieces.append((ref.at[index[0], index[1], index[2], pl.ds(core * 14 + start - begin, stop - start)], start, stop - start))
        if lo + n == 29:
            pieces.append((norm_ref.at[index[0], index[1], index[2], pl.ds(core, 1)], 28, 1))
        return pieces

    loads = {}
    for turn, delta in enumerate((2, 1, -1, 0)):
        for g in range(3):
            j = place.step(ORDERS[g][0], delta)
            index, lo, n = index_of(g, 0, j)
            loads[turn, g] = []
            for ref, start, count in sources(g, index, place.core):
                load = pltpu.make_async_copy(ref, own.at[index[0], index[1], index[2], pl.ds(start, count)], load_sem.at[len(loaded)])
                load.start()
                loaded.append(load)
                loads[turn, g].append(load)
    place.barrier()
    swaps = {}
    for turn, delta in enumerate((2, 1, -1, 0)):
        for g in range(3):
            j = place.step(ORDERS[g][0], delta)
            index, lo, n = index_of(g, 0, j)
            swaps[turn, g] = [send(ref, theirs.at[index[0], index[1], index[2], pl.ds(start, count)], place.partner()) for ref, start, count in sources(g, index, 1 - place.core)]

    def add_into(target, addend):
        target[...] = target[...] + addend[...]

    def ready(turn, g):
        delta = (2, 1, -1, 0)[turn]
        for load in loads[turn, g]:
            load.wait()
        for swap in swaps[turn, g]:
            swap.wait_recv()
        j = place.step(ORDERS[g][0], delta)
        add_into(in_own(own, g, 0, j), in_own(theirs, g, 0, j))

    def box(g, phase, slot, side):
        ref = boxes[g * 3 + phase]
        if phase < 2:
            return ref.at[slot]
        size = groups[g][1]
        cut = (size + 1) // 2
        return ref.at[slot, pl.ds(0, cut if side == 0 else size - cut)]

    for phase in range(3):
        flight = {}
        dims = [ORDERS[g][phase] for g in range(3)]

        def start(g, name, j_delta, side, slot, toward):
            j = place.step(dims[g], j_delta)
            flight[g, name] = send(in_own(own, g, phase, j, side), box(g, phase, slot, side), place.chip(dims[g], toward))

        for g in range(3):
            if phase == 0:
                ready(0, g)
            start(g, 'far_right', 2, 0, 0, 1)
            start(g, 'far_left', 2, 1, 2, -1)
        for g in range(3):
            if phase == 0:
                ready(1, g)
            start(g, 'near_right', 1, 1, 1, 1)
            if phase == 0:
                ready(2, g)
            start(g, 'near_left', -1, 0, 3, -1)
        for g in range(3):
            flight[g, 'far_right'].wait_recv()
            add_into(in_own(own, g, phase, place.step(dims[g], 1), 0), box(g, phase, 0, 0))
            start(g, 'sum_right', 1, 0, 4, 1)
            flight[g, 'far_left'].wait_recv()
            add_into(in_own(own, g, phase, place.step(dims[g], -1), 1), box(g, phase, 2, 1))
            start(g, 'sum_left', -1, 1, 5, -1)
        if phase == 0:
            for g in range(3):
                ready(3, g)
        for g in range(3):
            here = place.at[dims[g]]
            for name, slot, side in (('near_left', 3, 0), ('near_right', 1, 1)):
                flight[g, name].wait_recv()
                add_into(in_own(own, g, phase, here, side), box(g, phase, slot, side))
            for name, slot, side in (('sum_right', 4, 0), ('sum_left', 5, 1)):
                flight[g, name].wait_recv()
                add_into(in_own(own, g, phase, here, side), box(g, phase, slot, side))
    out_ref[place.core] = own[place.at[0], place.at[1], place.at[2]]
    piece = out_ref.at[place.core]
    send(piece, piece, place.partner()).wait_recv()
    for copy in pending:
        copy.wait_send()


def reduce_tiles(grad_low, grad_high, norm_low, norm_high, collective_id):
    half = 29
    norms = jnp.stack([norm_low, norm_high], axis=1)
    grids = [array.reshape((RING, RING, RING) + array.shape[1:]) for array in (grad_low, grad_high, norms)]
    groups = split_groups(half)
    box_shapes = []
    for g in range(3):
        order = ORDERS[g]
        size = groups[g][1]
        dims = {dim: RING for dim in range(3) if dim != order[0]}
        dims[order[1]] = 2
        box_shapes.append((6,) + tuple(dims[dim] for dim in sorted(dims)) + (size, 8, 128))
        box_shapes.append((6, 2, size, 8, 128))
        box_shapes.append((6, (size + 1) // 2, 8, 128))
    copies = 20 + 3 * 3 * 6 + 1
    return pl.pallas_call(
        reduce_kernel,
        out_shape=jax.ShapeDtypeStruct((2, half, 8, 128), jnp.float32),
        in_specs=[pl.BlockSpec(memory_space=pl.ANY)] * 3,
        out_specs=pl.BlockSpec(memory_space=pltpu.VMEM),
        scratch_shapes=[pltpu.VMEM((RING, RING, RING, half, 8, 128), jnp.float32)] * 2 + [pltpu.VMEM(shape, jnp.float32) for shape in box_shapes] + [pltpu.SemaphoreType.DMA((20,)), pltpu.SemaphoreType.DMA((copies,)), pltpu.SemaphoreType.DMA((copies,))],
        compiler_params=pltpu.CompilerParams(collective_id=collective_id, has_side_effects=True, vmem_limit_bytes=56 * 2 ** 20),
        name='reduce_tiles',
    )(*grids)


TILE = 256
NODE_TILE = TILE // 8
BF16 = jnp.bfloat16
F32 = jnp.float32


def dot(left, right, left_dim=1, right_dim=0):
    return lax.dot_general(left, right, (((left_dim,), (right_dim,)), ((), ())), preferred_element_type=F32)


def split_three(values):
    high = values.astype(BF16)
    rest = values - high.astype(F32)
    mid = rest.astype(BF16)
    low = (rest - mid.astype(F32)).astype(BF16)
    return high, mid, low


def dot_wide(values, right, right_dim=0):
    high, mid, low = split_three(values)
    return dot(high, right, 1, right_dim) + dot(mid, right, 1, right_dim) + dot(low, right, 1, right_dim)


def dot_wide_rows(left, values):
    high, mid, low = split_three(values)
    return dot(left, high, 0, 0) + dot(left, mid, 0, 0) + dot(left, low, 0, 0)


def norm_stats(out_b):
    values = out_b.astype(F32)
    centered = values - jnp.mean(values, axis=-1, keepdims=True)
    inv_std = lax.rsqrt(jnp.mean(centered * centered, axis=-1, keepdims=True) + NORM_EPS)
    return centered * inv_std, inv_std


def mlp_forward(pre_act, w_two, gain, bias):
    pre_b = pre_act.astype(BF16)
    hidden = jax.nn.silu(pre_b.astype(F32)).astype(BF16)
    out_b = dot(hidden, w_two).astype(BF16)
    normed, _ = norm_stats(out_b)
    return normed * gain + bias, pre_b, out_b


def mlp_cotangents(d_branch, pre_b, out_b, w_two, gain):
    normed, inv_std = norm_stats(out_b)
    d_norm = d_branch * gain
    d_out = (inv_std * (d_norm - jnp.mean(d_norm, axis=-1, keepdims=True) - normed * jnp.mean(d_norm * normed, axis=-1, keepdims=True))).astype(BF16)
    d_act = dot(d_out, w_two, 1, 1).astype(BF16)
    pre_f = pre_b.astype(F32)
    gate = jax.nn.sigmoid(pre_f)
    hidden = (pre_f * gate).astype(BF16)
    d_pre = (d_act.astype(F32) * gate * (1.0 + pre_f * (1.0 - gate))).astype(BF16)
    d_gain = (d_branch * normed).reshape(-1, 8, d_branch.shape[-1]).sum(axis=0)
    d_bias = d_branch.reshape(-1, 8, d_branch.shape[-1]).sum(axis=0)
    return d_out, hidden, d_pre, d_gain, d_bias


def receiver_pick(copies):
    rows = lax.broadcasted_iota(jnp.int32, (TILE, copies * NODE_TILE), 0)
    cols = lax.broadcasted_iota(jnp.int32, (TILE, copies * NODE_TILE), 1)
    return lax.shift_right_logical(rows, 3) == lax.bitwise_and(cols, NODE_TILE - 1)


def as_bf16(flags):
    return jnp.where(flags, 1.0, 0.0).astype(BF16)


def unpack_weights(tiles_ref, layer, w_e1, w_e2, w_n1, w_n2, norms):
    def pair(p, carry):
        for k in range(4):
            lanes = pl.ds(128 * k, 128)
            w_e1[pl.ds(pl.multiple_of(48 * p, 16), 16), lanes] = tiles_ref[2 * p, 8 * layer + k]
            w_e1[pl.ds(pl.multiple_of(48 * p + 32, 16), 16), lanes] = tiles_ref[2 * p + 1, 8 * layer + k]
            w_n1[pl.ds(pl.multiple_of(32 * p, 16), 16), lanes] = tiles_ref[2 * p, 8 * layer + 4 + k]
            w_n1[pl.ds(pl.multiple_of(32 * p + 16, 16), 16), lanes] = tiles_ref[2 * p + 1, 8 * layer + 4 + k]
            for ref, first, tile in ((w_e1, 48 * p + 16, 16), (w_e2, 16 * p, 20), (w_n2, 16 * p, 24)):
                even = tiles_ref[2 * p, tile + k].astype(F32)[8 * layer:8 * layer + 8]
                odd = tiles_ref[2 * p + 1, tile + k].astype(F32)[8 * layer:8 * layer + 8]
                ref[pl.ds(pl.multiple_of(first, 16), 16), lanes] = jnp.concatenate([even, odd], axis=0).astype(BF16)
        return carry
    lax.fori_loop(0, 32, pair, 0)
    for k in range(4):
        total = tiles_ref[16 * k, 28].astype(F32)
        for d in range(1, 16):
            total = total + tiles_ref[16 * k + d, 28].astype(F32)
        norms[:, 128 * k:128 * k + 128] = total[8 * layer:8 * layer + 8]


def edge_forward(layer_io, edge_out, pre_out, out_out, sums_out, w_e1, w_e2, norms, recv_terms):
    node_all, node_own, edge_in, snd_col, mask_col = layer_io
    for part, term in enumerate(split_three(dot(node_own[...], w_e1[1024:1536]))):
        recv_terms[part] = term

    def tile(i, carry):
        rows = pl.ds(pl.multiple_of(i * TILE, TILE), TILE)
        nodes = pl.ds(pl.multiple_of(i * NODE_TILE, NODE_TILE), NODE_TILE)
        ids = lax.broadcasted_iota(jnp.int32, (TILE, 512), 1)
        sender = dot(as_bf16(snd_col[rows] == ids), node_all[...]).astype(BF16)
        recv = jnp.concatenate([recv_terms[0, nodes], recv_terms[1, nodes], recv_terms[2, nodes]], axis=0)
        edge = edge_in[rows]
        pre = dot(edge, w_e1[0:512]) + dot(sender, w_e1[512:1024]) + dot(as_bf16(receiver_pick(3)), recv)
        branch, pre_b, out_b = mlp_forward(pre, w_e2[...], norms[0:1], norms[1:2])
        edge_new = (edge.astype(F32) + branch).astype(BF16)
        pre_out[rows] = pre_b
        out_out[rows] = out_b
        if edge_out is not None:
            edge_out[rows] = edge_new
        picked = jnp.where(receiver_pick(1), mask_col[rows], 0.0).astype(BF16)
        sums_out[nodes] = dot(picked, edge_new, 0, 0).astype(BF16)
        return carry
    lax.fori_loop(0, edge_in.shape[0] // TILE, tile, 0)


def node_forward(node_own, sums, w_n1, w_n2, norms):
    pre = dot(node_own[...], w_n1[0:512]) + dot(sums[...], w_n1[512:1024])
    return mlp_forward(pre, w_n2[...], norms[2:3], norms[3:4])


def store_grad(grad_ref, values, first_row, shard_rows, first_tile):
    for q in range(values.shape[0] // 8):
        place = first_row // 8 + q
        per = shard_rows // 8
        for k in range(4):
            grad_ref[place // per, first_tile + place % per * 4 + k] = values[8 * q:8 * q + 8, 128 * k:128 * k + 128]


def layer_back(layer_io, d_node_new, d_edge_new, pre_e, out_e, sums, pre_n, out_n, mats, norms, snd_row, outs, scratch):
    node_all, node_own, edge_in, snd_col, mask_col = layer_io
    w_e1, w_e2, w_n1, w_n2 = mats
    grad_ref, norm_grad, d_edge, d_local, scattered = outs
    hidden_s, d_pre_s, d_out_s, d_sum_s, recv_s, gain_s = scratch
    d_out_n, hidden_n, d_pre_n, d_gain_n, d_bias_n = mlp_cotangents(d_node_new, pre_n, out_n, w_n2[...], norms[2:3])
    d_sum_s[...] = dot(d_pre_n, w_n1[512:1024], 1, 1).astype(BF16)
    d_local[...] = d_node_new + dot(d_pre_n, w_n1[0:512], 1, 1)
    store_grad(grad_ref, dot(hidden_n, d_out_n, 0, 0), 0, 8, 24)
    store_grad(grad_ref, dot(node_own[...], d_pre_n, 0, 0), 0, 16, 16)
    store_grad(grad_ref, dot(sums[...], d_pre_n, 0, 0), 512, 16, 16)
    gain_s[...] = jnp.zeros_like(gain_s)

    def tile(i, carry):
        rows = pl.ds(pl.multiple_of(i * TILE, TILE), TILE)
        nodes = pl.ds(pl.multiple_of(i * NODE_TILE, NODE_TILE), NODE_TILE)
        pick = receiver_pick(1)
        picked = jnp.where(pick, mask_col[rows], 0.0).astype(BF16)
        d_res = (d_edge_new[rows].astype(F32) + dot(picked, d_sum_s[nodes])).astype(BF16).astype(F32)
        d_out, hidden, d_pre, d_gain, d_bias = mlp_cotangents(d_res, pre_e[rows], out_e[rows], w_e2[...], norms[0:1])
        gain_s[0] = gain_s[0] + d_gain
        gain_s[1] = gain_s[1] + d_bias
        hidden_s[rows] = hidden
        d_out_s[rows] = d_out
        d_pre_s[rows] = d_pre
        d_edge[rows] = (d_res + dot(d_pre, w_e1[0:512], 1, 1)).astype(BF16)
        recv_s[nodes] = dot(as_bf16(pick), d_pre, 0, 0)
        return carry
    lax.fori_loop(0, edge_in.shape[0] // TILE, tile, 0)
    store_grad(grad_ref, dot(hidden_s[...], d_out_s[...], 0, 0), 0, 8, 12)
    store_grad(grad_ref, dot(edge_in[...], d_pre_s[...], 0, 0), 0, 24, 0)
    for block in range(4):
        ids = lax.broadcasted_iota(jnp.int32, (128, edge_in.shape[0]), 0) + 128 * block
        scattered[128 * block:128 * block + 128] = dot(as_bf16(snd_row[...] == ids), d_pre_s[...])
    store_grad(grad_ref, dot_wide_rows(node_all[...], scattered[...]), 512, 24, 0)
    store_grad(grad_ref, dot_wide_rows(node_own[...], recv_s[...]), 1024, 24, 0)
    d_local[...] = d_local[...] + dot_wide(recv_s[...], w_e1[1024:1536], 1)
    rows = [gain_s[0].sum(axis=0, keepdims=True), gain_s[1].sum(axis=0, keepdims=True), d_gain_n.sum(axis=0, keepdims=True), d_bias_n.sum(axis=0, keepdims=True)]
    full = jnp.concatenate(rows + [jnp.zeros((4, 512), F32)], axis=0)
    for d in range(64):
        k = d // 16
        norm_grad[d] = full[:, 128 * k:128 * k + 128]


def own_nodes(node_all):
    count = node_all.shape[0] // 2
    return node_all.at[pl.ds(pl.multiple_of(lax.axis_index('sp') * count, count), count)]


def forward_kernel(tiles_ref, node_all, edge_in, snd_col, mask_col, edge_out, pre_e, out_e, sums, pre_n, out_n, node_new, *rest):
    mats = (rest[0:4], rest[5:9])
    norms = (rest[4], rest[9])
    recv_terms = rest[10]
    for layer in range(2):
        unpack_weights(tiles_ref, layer, *mats[layer], norms[layer])
    node_own = own_nodes(node_all)
    w_e1, w_e2, w_n1, w_n2 = mats[0]
    edge_forward((node_all, node_own, edge_in, snd_col, mask_col), edge_out, pre_e, out_e, sums, w_e1, w_e2, norms[0], recv_terms)
    branch, pre_b, out_b = node_forward(node_own, sums, w_n1, w_n2, norms[0])
    pre_n[...] = pre_b
    out_n[...] = out_b
    node_new[...] = (node_own[...].astype(F32) + branch).astype(BF16)


def middle_kernel(node_all, edge_in, snd_col, snd_row, mask_col, node_cot, edge_cot, w_e1, w_e2, w_n1, w_n2, norms, grad_ref, norm_grad, d_edge, d_local, scattered, pre_e, out_e, sums, recv_terms, *scratch):
    node_own = own_nodes(node_all)
    layer_io = (node_all, node_own, edge_in, snd_col, mask_col)
    edge_forward(layer_io, None, pre_e, out_e, sums, w_e1, w_e2, norms, recv_terms)
    _, pre_n, out_n = node_forward(node_own, sums, w_n1, w_n2, norms)
    layer_back(layer_io, node_cot[...].astype(F32), edge_cot, pre_e, out_e, sums, pre_n, out_n, (w_e1, w_e2, w_n1, w_n2), norms, snd_row, (grad_ref, norm_grad, d_edge, d_local, scattered), scratch)


def node_cotangent(d_local, scattered, returned, w_above):
    count = d_local.shape[0]
    mine = scattered[pl.ds(pl.multiple_of(lax.axis_index('sp') * count, count), count)]
    return (d_local[...] + dot_wide(mine + returned[...], w_above[512:1024], 1)).astype(BF16)


def back_kernel(node_all, edge_in, snd_col, snd_row, mask_col, d_local_above, scattered_above, returned, w_above, d_edge_new, pre_e, out_e, sums, pre_n, out_n, w_e1, w_e2, w_n1, w_n2, norms, grad_ref, norm_grad, d_edge, d_local, scattered, *scratch):
    node_own = own_nodes(node_all)
    layer_io = (node_all, node_own, edge_in, snd_col, mask_col)
    d_node = node_cotangent(d_local_above, scattered_above, returned, w_above).astype(F32)
    layer_back(layer_io, d_node, d_edge_new, pre_e, out_e, sums, pre_n[...], out_n[...], (w_e1, w_e2, w_n1, w_n2), norms, snd_row, (grad_ref, norm_grad, d_edge, d_local, scattered), scratch)


def last_kernel(d_local, scattered, returned, w_e1, grad_node):
    grad_node[...] = node_cotangent(d_local, scattered, returned, w_e1)


def swap_kernel(src_ref, out_ref, send_sem, recv_sem):
    core = lax.axis_index('sp')
    sem = pltpu.get_barrier_semaphore()
    pl.semaphore_signal(sem, inc=1, device_id={'sp': 1 - core}, device_id_type=MESH_ID)
    pl.semaphore_wait(sem, 1)
    count = out_ref.shape[0]
    start = pl.multiple_of((1 - core) * count, count)
    copy = pltpu.make_async_remote_copy(src_ref=src_ref.at[pl.ds(start, count)], dst_ref=out_ref, send_sem=send_sem, recv_sem=recv_sem, device_id={'sp': 1 - core}, device_id_type=MESH_ID)
    copy.start()
    copy.wait()


def vmem_call(kernel, name, inputs, outputs, scratch, flops):
    spec = pl.BlockSpec(memory_space=pltpu.VMEM)
    return pl.pallas_call(
        kernel,
        out_shape=[jax.ShapeDtypeStruct(shape, dtype) for shape, dtype in outputs],
        in_specs=[spec] * len(inputs),
        out_specs=[spec] * len(outputs),
        scratch_shapes=[pltpu.VMEM(shape, dtype) for shape, dtype in scratch],
        compiler_params=pltpu.CompilerParams(vmem_limit_bytes=62 * 2 ** 20),
        cost_estimate=pl.CostEstimate(flops=flops, bytes_accessed=20 * 2 ** 20, transcendentals=0),
        name=name,
    )(*inputs)


def swap_halves(values, collective_id):
    return pl.pallas_call(
        swap_kernel,
        out_shape=jax.ShapeDtypeStruct((values.shape[0] // 2,) + values.shape[1:], values.dtype),
        in_specs=[pl.BlockSpec(memory_space=pltpu.VMEM)],
        out_specs=pl.BlockSpec(memory_space=pltpu.VMEM),
        scratch_shapes=[pltpu.SemaphoreType.DMA, pltpu.SemaphoreType.DMA],
        compiler_params=pltpu.CompilerParams(collective_id=collective_id, has_side_effects=True),
        name='swap_halves',
    )(values)


MAT_SHAPES = [((1536, 512), BF16), ((512, 512), BF16), ((1024, 512), BF16), ((512, 512), BF16), ((8, 512), F32)]
GRAD_SHAPES = [((64, 28, 8, 128), F32), ((64, 8, 128), F32), ((2048, 512), BF16), ((256, 512), F32), ((512, 512), F32)]
BACK_SCRATCH = [((2048, 512), BF16)] * 3 + [((256, 512), BF16), ((256, 512), F32), ((2, 8, 512), F32)]
EDGE = ((2048, 512), BF16)
NODE = ((256, 512), BF16)


def adamw_update(master, grad_sum, moment_one, moment_two):
    corr_one = 1.0 - BETA_ONE ** STEP
    corr_two = 1.0 - BETA_TWO ** STEP
    one_new = BETA_ONE * moment_one + (1.0 - BETA_ONE) * grad_sum
    two_new = BETA_TWO * moment_two + (1.0 - BETA_TWO) * grad_sum * grad_sum
    direction = (one_new / corr_one) / (jnp.sqrt(two_new / corr_two) + ADAM_EPS)
    return master - LEARN_RATE * (direction + DECAY * master), one_new, two_new


def update_all(masters, moments_one, moments_two, layer_grads):
    new_master = []
    new_one = []
    new_two = []
    for slot in range(len(masters)):
        grad_sum = jnp.stack([per_layer[slot] for per_layer in layer_grads], axis=0)
        master_new, one_new, two_new = adamw_update(masters[slot], grad_sum, moments_one[slot], moments_two[slot])
        new_master.append(master_new)
        new_one.append(one_new)
        new_two.append(two_new)
    return tuple(new_master) + tuple(new_one) + tuple(new_two)


def rows_to_tiles(values, sub):
    rows = values.shape[0]
    return values.reshape(rows // sub, sub, 4, 128).transpose(0, 2, 1, 3).reshape(rows // sub * 4, sub, 128)


def tiles_to_rows(tiles):
    count, sub = tiles.shape[:2]
    return tiles.reshape(count // 4, 4, sub, 128).transpose(0, 2, 1, 3).reshape(count // 4 * sub, 512)


def pack_shard(masters):
    chip = lax.axis_index('dp')
    odd = lax.rem(chip, 2) == 1
    edge_one, edge_two, node_one, node_two, norm = [master.astype(BF16) for master in masters]
    main = jnp.where(odd, edge_one[:, 8:24], edge_one[:, 0:16])
    tail = jnp.where(odd, edge_one[:, 0:8], edge_one[:, 16:24])
    rows = jnp.concatenate([main[0], node_one[0], main[1], node_one[1], tail[0], tail[1], edge_two[0], edge_two[1], node_two[0], node_two[1]], axis=0)
    wide = jnp.tile(norm, (1, 1, 16))
    lanes = lax.broadcasted_iota(jnp.int32, wide.shape, 2) // 8
    wide = jnp.where(lanes == lax.rem(chip, 16), wide, 0)
    norms = jnp.pad(wide, ((0, 0), (0, 4), (0, 0))).reshape(1, 16, 128)
    return jnp.concatenate([rows_to_tiles(rows, 16), norms, jnp.zeros_like(norms)], axis=0)


def unpack_grads(total):
    chip = lax.axis_index('dp')
    out = []
    for layer in range(2):
        tiles = jnp.concatenate([total[0, 14 * layer:14 * layer + 14], total[1, 14 * layer:14 * layer + 14]], axis=0)
        rows = tiles_to_rows(tiles)
        norm = lax.dynamic_slice(total[layer, 28], (0, lax.rem(chip, 16) * 8), (4, 8))
        mats = []
        first = 0
        for size in SHARD_ROWS:
            mats.append(rows[first:first + size])
            first += size
        out.append(tuple(mats) + (norm,))
    return out


def solution(mesh):
    lat_spec = P('dp', 'sp', None)
    edge_spec = P('sp')
    mat_spec = P(None, 'dp', None)
    norm_spec = P(None, None, 'dp')
    param_specs = (mat_spec, mat_spec, mat_spec, mat_spec, norm_spec)

    def train_step(node_lat, edge_lat, senders, edge_mask, node_cot, edge_cot, w_edge1, w_edge2, w_node1, w_node2, norm_par, mom_edge1, mom_edge2, mom_node1, mom_node2, mom_norm, vel_edge1, vel_edge2, vel_node1, vel_node2, vel_norm):
        masters = (w_edge1, w_edge2, w_node1, w_node2, norm_par)
        moments_one = (mom_edge1, mom_edge2, mom_node1, mom_node2, mom_norm)
        moments_two = (vel_edge1, vel_edge2, vel_node1, vel_node2, vel_norm)
        snd_col = senders.reshape(-1, 1)
        snd_row = senders.reshape(1, -1)
        mask_col = edge_mask.astype(F32).reshape(-1, 1)
        tiles = gather_tiles(pack_shard(masters), 1).reshape(64, 30, 16, 128)
        node_all = lax.all_gather(node_lat[0], 'sp', axis=0, tiled=True)
        outs = vmem_call(forward_kernel, 'forward_low', (tiles, node_all, edge_lat[0], snd_col, mask_col), [EDGE, EDGE, EDGE, NODE, NODE, NODE, NODE] + MAT_SHAPES + MAT_SHAPES, [((3, 256, 512), BF16)], 5 * 10 ** 9)
        edge_one, pre_e, out_e, sums, pre_n, out_n, node_one = outs[:7]
        mats_low = outs[7:12]
        mats_high = outs[12:17]
        node_all_one = lax.all_gather(node_one, 'sp', axis=0, tiled=True)
        grad_high, norm_high, d_edge_one, d_local_one, scattered_one = vmem_call(middle_kernel, 'forward_back_high', (node_all_one, edge_one, snd_col, snd_row, mask_col, node_cot[0], edge_cot[0]) + tuple(mats_high), GRAD_SHAPES, [EDGE, EDGE, NODE, ((3, 256, 512), BF16)] + BACK_SCRATCH, 13 * 10 ** 9)
        returned = swap_halves(scattered_one, 3)
        grad_low, norm_low, d_edge_zero, d_local_zero, scattered_zero = vmem_call(back_kernel, 'back_low', (node_all, edge_lat[0], snd_col, snd_row, mask_col, d_local_one, scattered_one, returned, mats_high[0], d_edge_one, pre_e, out_e, sums, pre_n, out_n) + tuple(mats_low), GRAD_SHAPES, BACK_SCRATCH, 8 * 10 ** 9)
        returned_zero = swap_halves(scattered_zero, 4)
        grad_node = vmem_call(last_kernel, 'node_grad', (d_local_zero, scattered_zero, returned_zero, mats_low[0]), [NODE], [], 4 * 10 ** 8)[0]
        total = reduce_tiles(grad_low, grad_high, norm_low, norm_high, 2)
        new_state = update_all(masters, moments_one, moments_two, unpack_grads(total))
        return new_state + (grad_node[None], d_edge_zero[None])

    return jax.shard_map(train_step, mesh=mesh, in_specs=(lat_spec, lat_spec, edge_spec, edge_spec, lat_spec, lat_spec) + param_specs + param_specs + param_specs, out_specs=param_specs + param_specs + param_specs + (lat_spec, lat_spec), check_vma=False)
```

```python
import functools

import jax
import jax.numpy as jnp
from jax import lax
from jax.experimental import pallas as pl
from jax.experimental.pallas import tpu as pltpu
from jax.sharding import PartitionSpec as P

NORM_EPS = 1e-5
LEARN_RATE = 1e-3
BETA_ONE = 0.9
BETA_TWO = 0.95
ADAM_EPS = 1e-8
DECAY = 0.1
STEP = 10

MESH_ID = pl.DeviceIdType.MESH
ORDERS = ((0, 1, 2), (1, 2, 0), (2, 0, 1))
RING = 4
HOPS = (1, -1, 2)


class Place:
    def __init__(self):
        chip = lax.axis_index('dp')
        self.core = lax.axis_index('sp')
        self.at = (lax.rem(chip // 16, 4), lax.rem(chip // 4, 4), lax.rem(chip, 4))

    def step(self, dim, delta):
        return lax.rem(self.at[dim] + (delta + RING), RING)

    def chip(self, dim, delta):
        pos = list(self.at)
        pos[dim] = self.step(dim, delta)
        return {'dp': pos[0] * 16 + pos[1] * 4 + pos[2]}

    def partner(self):
        return {'sp': 1 - self.core}

    def barrier(self, ring=True):
        sem = pltpu.get_barrier_semaphore()
        peers = [self.partner()]
        if ring:
            peers += [self.chip(dim, delta) for dim in range(3) for delta in HOPS]
        for peer in peers:
            pl.semaphore_signal(sem, inc=1, device_id=peer, device_id_type=MESH_ID)
        pl.semaphore_wait(sem, len(peers))


class Wire:
    def __init__(self, send_sem, recv_sem):
        self.sems = (send_sem, recv_sem)
        self.slots = {}
        self.parts = {}

    def describe(self, key):
        source, target, where = self.parts[key]
        slot = self.slots.setdefault(key, len(self.slots))
        return pltpu.make_async_remote_copy(src_ref=source(), dst_ref=target(), send_sem=self.sems[0].at[slot], recv_sem=self.sems[1].at[slot], device_id=where(), device_id_type=MESH_ID)

    def start(self, key, source, target, where):
        self.parts[key] = (source, target, where)
        self.describe(key).start()

    def wait_recv(self, key):
        self.describe(key).wait_recv()

    def finish(self):
        for key in list(self.parts):
            self.describe(key).wait_send()


def split_groups(count):
    base, extra = divmod(count, 3)
    sizes = [base + (1 if g < extra else 0) for g in range(3)]
    starts = [sum(sizes[:g]) for g in range(3)]
    return list(zip(starts, sizes))


class Gather:
    def __init__(self, name, place, wire, src_ref, grid_ref):
        self.name, self.place, self.wire = name, place, wire
        self.src, self.grid = src_ref, grid_ref
        self.half = src_ref.shape[0] // 2
        self.first = place.core * self.half
        self.groups = split_groups(self.half)
        self.shared = []

    def region(self, g, phase, delta, side=None):
        order = ORDERS[g]
        start, size = self.groups[g]
        index = list(self.place.at)
        for q in range(phase):
            index[order[q]] = pl.ds(0, RING)
        index[order[phase]] = self.place.step(order[phase], delta)
        if side is not None:
            index[order[0]] = pl.ds(2 * side, 2)
        return self.grid.at[index[0], index[1], index[2], pl.ds(self.first + start, size)]

    def send(self, g, phase, delta, toward, tag, side=None):
        dim = ORDERS[g][phase]
        piece = functools.partial(self.region, g, phase, delta, side)
        origin = piece
        if phase == 0:
            start, size = self.groups[g]
            origin = lambda: self.src.at[pl.ds(self.first + start, size)]
        self.wire.start((self.name, g, phase, tag), origin, piece, lambda: self.place.chip(dim, toward))

    def share(self, g, phase, delta):
        key = (self.name, g, phase, 'share', delta)
        self.shared.append(key)
        piece = functools.partial(self.region, g, phase, delta)
        self.wire.start(key, piece, piece, self.place.partner)

    def begin(self, phase):
        for g in range(3):
            for toward in (HOPS if phase < 2 else (1, -1)):
                self.send(g, phase, 0, toward, toward)

    def arrived(self, g, phase, tag):
        self.wire.wait_recv((self.name, g, phase, tag))

    def stage(self, number):
        if number == 0:
            self.begin(0)
        elif number in (1, 2):
            for g in range(3):
                for toward in HOPS:
                    self.arrived(g, number - 1, toward)
            self.begin(number)
            for g in range(3):
                for toward in HOPS:
                    self.share(g, number - 1, -toward)
        elif number == 3:
            for g in range(3):
                self.arrived(g, 2, 1)
                self.send(g, 2, -1, 1, 'on_right', 0)
                self.arrived(g, 2, -1)
                self.send(g, 2, 1, -1, 'on_left', 1)
            for g in range(3):
                self.share(g, 2, -1)
                self.share(g, 2, 1)
        elif number == 4:
            for g in range(3):
                self.arrived(g, 2, 'on_right')
                self.arrived(g, 2, 'on_left')
                self.share(g, 2, 2)
        else:
            for key in self.shared:
                self.wire.wait_recv(key)


GATHER_COPIES = 3 * (3 + 3 + 4 + 3 + 3 + 3)


class Reduce:
    def __init__(self, name, place, wire, sources, own, theirs, boxes, out_ref, out_first, load_sem=None):
        self.name, self.place, self.wire = name, place, wire
        self.sources, self.own, self.theirs, self.boxes = sources, own, theirs, boxes
        self.out, self.out_first, self.load_sem = out_ref, out_first, load_sem
        self.count = own.shape[3]
        self.groups = split_groups(self.count)
        self.turns = (2, 1, -1, 0)

    def index_of(self, g, phase, delta, side=None):
        order = ORDERS[g]
        index = [pl.ds(0, RING)] * 3
        for q in range(phase):
            index[order[q]] = self.place.at[order[q]]
        index[order[phase]] = self.place.step(order[phase], delta)
        if side is not None:
            index[order[phase + 1]] = pl.ds(2 * side, 2)
        return index

    def kept(self, ref, g, phase, delta, side=None):
        index = self.index_of(g, phase, delta, side)
        return ref.at[index[0], index[1], index[2], pl.ds(*self.groups[g])]

    def pieces(self, g, delta, core):
        index = self.index_of(g, 0, delta)
        lo, n = self.groups[g]
        begin = 0
        out = []
        for ref, first, count in self.sources:
            part = count // 2
            start, stop = max(lo, begin), min(lo + n, begin + part)
            if start < stop:
                out.append((ref.at[index[0], index[1], index[2], pl.ds(first + core * part + start - begin, stop - start)], start, stop - start))
            begin += part
        return out

    def slot(self, ref, g, delta, start, count):
        index = self.index_of(g, 0, delta)
        return ref.at[index[0], index[1], index[2], pl.ds(start, count)]

    def loads(self):
        out = []
        for delta in self.turns:
            for g in range(3):
                for ref, start, count in self.pieces(g, delta, self.place.core):
                    out.append((delta, g, functools.partial(pltpu.make_async_copy, ref, self.slot(self.own, g, delta, start, count), self.load_sem.at[len(out)])))
        return out

    def ready(self, g, delta):
        here = self.pieces(g, delta, self.place.core)
        if self.load_sem is not None:
            for turn, group, load in self.loads():
                if turn == delta and group == g:
                    load().wait()
        for n, (ref, start, count) in enumerate(here):
            self.wire.wait_recv((self.name, 'swap', g, delta, n))
            target = self.slot(self.own, g, delta, start, count)
            mine = target if self.load_sem is not None else ref
            target[...] = mine[...] + self.slot(self.theirs, g, delta, start, count)[...]

    def box(self, g, phase, number):
        return self.boxes[g * 3 + phase].at[number]

    def send(self, g, phase, tag, delta, side, number, toward):
        dim = ORDERS[g][phase]
        self.wire.start((self.name, g, phase, tag), functools.partial(self.kept, self.own, g, phase, delta, side), functools.partial(self.box, g, phase, number), lambda: self.place.chip(dim, toward))

    def absorb(self, g, phase, tag, delta, side, number):
        self.wire.wait_recv((self.name, g, phase, tag))
        target = self.kept(self.own, g, phase, delta, side)
        target[...] = target[...] + self.box(g, phase, number)[...]

    def far(self, g, phase):
        self.send(g, phase, 'far_right', 2, 0, 0, 1)
        self.send(g, phase, 'far_left', 2, 1, 2, -1)

    def near(self, g, phase):
        self.send(g, phase, 'near_right', 1, 1, 1, 1)
        self.send(g, phase, 'near_left', -1, 0, 3, -1)

    def onward(self, g, phase):
        self.absorb(g, phase, 'far_right', 1, 0, 0)
        self.send(g, phase, 'sum_right', 1, 0, 4, 1)
        self.absorb(g, phase, 'far_left', -1, 1, 2)
        self.send(g, phase, 'sum_left', -1, 1, 5, -1)

    def settle(self, g, phase):
        for tag, number, side in (('near_left', 3, 0), ('near_right', 1, 1), ('sum_right', 4, 0), ('sum_left', 5, 1)):
            self.absorb(g, phase, tag, 0, side, number)

    def stage(self, number):
        if number == 0:
            if self.load_sem is not None:
                for _, _, load in self.loads():
                    load().start()
            for delta in self.turns:
                for g in range(3):
                    for n, (_, start, count) in enumerate(self.pieces(g, delta, 1 - self.place.core)):
                        self.wire.start((self.name, 'swap', g, delta, n), lambda g=g, delta=delta, n=n: self.pieces(g, delta, 1 - self.place.core)[n][0], functools.partial(self.slot, self.theirs, g, delta, start, count), self.place.partner)
        elif number == 1:
            for g in range(3):
                self.ready(g, 2)
                self.far(g, 0)
            for g in range(3):
                self.ready(g, 1)
                self.ready(g, -1)
                self.near(g, 0)
        elif number == 2:
            for g in range(3):
                self.onward(g, 0)
            for g in range(3):
                self.ready(g, 0)
        elif number == 3:
            for g in range(3):
                self.settle(g, 0)
                self.far(g, 1)
                self.near(g, 1)
        elif number == 4:
            for g in range(3):
                self.onward(g, 1)
        elif number == 5:
            for g in range(3):
                self.settle(g, 1)
                for n, toward in enumerate(HOPS):
                    self.send(g, 2, toward, toward, None, n, toward)
        elif number == 6:
            for g in range(3):
                for n, toward in enumerate(HOPS):
                    self.absorb(g, 2, toward, 0, None, n)
            span = lambda: self.out.at[self.place.core, pl.ds(self.out_first, self.count)]
            span()[...] = self.own[self.place.at[0], self.place.at[1], self.place.at[2]]
            self.wire.start((self.name, 'result'), span, span, self.place.partner)
        else:
            self.wire.wait_recv((self.name, 'result'))


def box_shapes(count):
    out = []
    for g, (_, size) in enumerate(split_groups(count)):
        order = ORDERS[g]
        dims = {dim: RING for dim in range(3) if dim != order[0]}
        dims[order[1]] = 2
        out.append((6,) + tuple(dims[dim] for dim in sorted(dims)) + (size, 8, 128))
        out.append((6, 2, size, 8, 128))
        out.append((3, size, 8, 128))
    return out


def reduce_scratch(count):
    grid = pltpu.VMEM((RING, RING, RING, count, 8, 128), jnp.float32)
    return [grid, grid] + [pltpu.VMEM(shape, jnp.float32) for shape in box_shapes(count)]


TILE = 256
NODE_TILE = TILE // 8
BF16 = jnp.bfloat16
F32 = jnp.float32


def dot(left, right, left_dim=1, right_dim=0):
    return lax.dot_general(left, right, (((left_dim,), (right_dim,)), ((), ())), preferred_element_type=F32)


def split_three(values):
    high = values.astype(BF16)
    rest = values - high.astype(F32)
    mid = rest.astype(BF16)
    low = (rest - mid.astype(F32)).astype(BF16)
    return high, mid, low


def dot_wide(values, right, right_dim=0):
    high, mid, low = split_three(values)
    return dot(high, right, 1, right_dim) + dot(mid, right, 1, right_dim) + dot(low, right, 1, right_dim)


def dot_wide_rows(left, values):
    high, mid, low = split_three(values)
    return dot(left, high, 0, 0) + dot(left, mid, 0, 0) + dot(left, low, 0, 0)


def norm_stats(out_b):
    values = out_b.astype(F32)
    centered = values - jnp.mean(values, axis=-1, keepdims=True)
    inv_std = lax.rsqrt(jnp.mean(centered * centered, axis=-1, keepdims=True) + NORM_EPS)
    return centered * inv_std, inv_std


def mlp_forward(pre_act, w_two, gain, bias):
    pre_b = pre_act.astype(BF16)
    hidden = jax.nn.silu(pre_b.astype(F32)).astype(BF16)
    out_b = dot(hidden, w_two).astype(BF16)
    normed, _ = norm_stats(out_b)
    return normed * gain + bias, pre_b, out_b


def mlp_cotangents(d_branch, pre_b, out_b, w_two, gain):
    normed, inv_std = norm_stats(out_b)
    d_norm = d_branch * gain
    d_out = (inv_std * (d_norm - jnp.mean(d_norm, axis=-1, keepdims=True) - normed * jnp.mean(d_norm * normed, axis=-1, keepdims=True))).astype(BF16)
    d_act = dot(d_out, w_two, 1, 1).astype(BF16)
    pre_f = pre_b.astype(F32)
    gate = jax.nn.sigmoid(pre_f)
    hidden = (pre_f * gate).astype(BF16)
    d_pre = (d_act.astype(F32) * gate * (1.0 + pre_f * (1.0 - gate))).astype(BF16)
    d_gain = (d_branch * normed).reshape(-1, 8, d_branch.shape[-1]).sum(axis=0)
    d_bias = d_branch.reshape(-1, 8, d_branch.shape[-1]).sum(axis=0)
    return d_out, hidden, d_pre, d_gain, d_bias


def receiver_pick(copies):
    rows = lax.broadcasted_iota(jnp.int32, (TILE, copies * NODE_TILE), 0)
    cols = lax.broadcasted_iota(jnp.int32, (TILE, copies * NODE_TILE), 1)
    return lax.shift_right_logical(rows, 3) == lax.bitwise_and(cols, NODE_TILE - 1)


def as_bf16(flags):
    return jnp.where(flags, 1.0, 0.0).astype(BF16)


def unpack_weights(grid, w_e1, w_e2, w_n1, w_n2, norms):
    def pair(p, carry):
        at = (p // 8, lax.rem(p // 2, 4))
        x = lax.rem(p, 2) * 2
        for k in range(4):
            lanes = pl.ds(128 * k, 128)
            for dev in range(2):
                w_e1[pl.ds(pl.multiple_of(48 * p + 32 * dev, 16), 16), lanes] = grid[at[0], at[1], x + dev, k]
                w_n1[pl.ds(pl.multiple_of(32 * p + 16 * dev, 16), 16), lanes] = grid[at[0], at[1], x + dev, 4 + k]
            for ref, first, tile, top in ((w_e1, 48 * p + 16, 8, 0), (w_e2, 16 * p, 8, 8), (w_n2, 16 * p, 12, 0)):
                even = grid[at[0], at[1], x, tile + k].astype(F32)[top:top + 8]
                odd = grid[at[0], at[1], x + 1, tile + k].astype(F32)[top:top + 8]
                ref[pl.ds(pl.multiple_of(first, 16), 16), lanes] = jnp.concatenate([even, odd], axis=0).astype(BF16)
        return carry
    lax.fori_loop(0, 32, pair, 0)
    for k in range(4):
        total = grid[k, 0, 0, 12].astype(F32)
        for d in range(1, 16):
            total = total + grid[k, d // 4, d % 4, 12].astype(F32)
        norms[:, 128 * k:128 * k + 128] = total[8:16]


def fill_columns(snd_rows, mask_rows, snd_col, mask_col):
    for rows, col in ((snd_rows, snd_col), (mask_rows, mask_col)):
        turned = rows[...].astype(F32).T
        for n in range(rows.shape[0]):
            col[128 * n:128 * n + 128, :] = turned[:, n:n + 1]


def edge_forward(layer_io, hook, edge_out, pre_out, out_out, sums_out, w_e1, w_e2, norms, recv_terms):
    node_all, node_own, edge_in, snd_col, mask_col = layer_io
    for part, term in enumerate(split_three(dot(node_own[...], w_e1[1024:1536]))):
        recv_terms[part] = term

    def tile(i, carry):
        rows = pl.ds(pl.multiple_of(i * TILE, TILE), TILE)
        nodes = pl.ds(pl.multiple_of(i * NODE_TILE, NODE_TILE), NODE_TILE)
        ids = lax.broadcasted_iota(jnp.int32, (TILE, 512), 1)
        sender = dot(as_bf16(snd_col[rows].astype(jnp.int32) == ids), node_all[...]).astype(BF16)
        recv = jnp.concatenate([recv_terms[0, nodes], recv_terms[1, nodes], recv_terms[2, nodes]], axis=0)
        edge = edge_in[rows]
        pre = dot(edge, w_e1[0:512]) + dot(sender, w_e1[512:1024]) + dot(as_bf16(receiver_pick(3)), recv)
        branch, pre_b, out_b = mlp_forward(pre, w_e2[...], norms[0:1], norms[1:2])
        edge_new = (edge.astype(F32) + branch).astype(BF16)
        pre_out[rows] = pre_b
        out_out[rows] = out_b
        if edge_out is not None:
            edge_out[rows] = edge_new
        picked = jnp.where(receiver_pick(1), mask_col[rows], 0.0).astype(BF16)
        sums_out[nodes] = dot(picked, edge_new, 0, 0).astype(BF16)
        hook(i)
        return carry
    lax.fori_loop(0, edge_in.shape[0] // TILE, tile, 0)


def node_forward(node_own, sums, w_n1, w_n2, norms):
    pre = dot(node_own[...], w_n1[0:512]) + dot(sums[...], w_n1[512:1024])
    return mlp_forward(pre, w_n2[...], norms[2:3], norms[3:4])


def store_grad(grad_ref, values, first_row, shard_rows, first_tile):
    for q in range(values.shape[0] // 8):
        place = first_row // 8 + q
        per = shard_rows // 8
        for k in range(4):
            dev = place // per
            grad_ref[dev // 16, dev // 4 % 4, dev % 4, first_tile + place % per * 4 + k] = values[8 * q:8 * q + 8, 128 * k:128 * k + 128]


def layer_back(layer_io, d_node_new, d_edge_new, pre_e, out_e, sums, pre_n, out_n, mats, norms, snd_rows, outs, scratch, after_nodes, hook, pass_on):
    node_all, node_own, edge_in, snd_col, mask_col = layer_io
    w_e1, w_e2, w_n1, w_n2 = mats
    grad_ref, norm_grad, d_edge, d_local, scattered = outs
    hidden_s, d_pre_s, d_out_s, d_sum_s, recv_s, gain_s = scratch
    d_out_n, hidden_n, d_pre_n, d_gain_n, d_bias_n = mlp_cotangents(d_node_new, pre_n, out_n, w_n2[...], norms[2:3])
    d_sum_s[...] = dot(d_pre_n, w_n1[512:1024], 1, 1).astype(BF16)
    d_local[...] = d_node_new + dot(d_pre_n, w_n1[0:512], 1, 1)
    store_grad(grad_ref, dot(hidden_n, d_out_n, 0, 0), 0, 8, 24)
    store_grad(grad_ref, dot(node_own[...], d_pre_n, 0, 0), 0, 16, 16)
    store_grad(grad_ref, dot(sums[...], d_pre_n, 0, 0), 512, 16, 16)
    after_nodes()
    gain_s[...] = jnp.zeros_like(gain_s)

    def tile(i, carry):
        rows = pl.ds(pl.multiple_of(i * TILE, TILE), TILE)
        nodes = pl.ds(pl.multiple_of(i * NODE_TILE, NODE_TILE), NODE_TILE)
        pick = receiver_pick(1)
        picked = jnp.where(pick, mask_col[rows], 0.0).astype(BF16)
        d_res = (d_edge_new[rows].astype(F32) + dot(picked, d_sum_s[nodes])).astype(BF16).astype(F32)
        d_out, hidden, d_pre, d_gain, d_bias = mlp_cotangents(d_res, pre_e[rows], out_e[rows], w_e2[...], norms[0:1])
        gain_s[0] = gain_s[0] + d_gain
        gain_s[1] = gain_s[1] + d_bias
        hidden_s[rows] = hidden
        d_out_s[rows] = d_out
        d_pre_s[rows] = d_pre
        d_edge[rows] = (d_res + dot(d_pre, w_e1[0:512], 1, 1)).astype(BF16)
        recv_s[nodes] = dot(as_bf16(pick), d_pre, 0, 0)
        hook(i)
        return carry
    lax.fori_loop(0, edge_in.shape[0] // TILE, tile, 0)
    store_grad(grad_ref, dot(hidden_s[...], d_out_s[...], 0, 0), 0, 8, 12)
    store_grad(grad_ref, dot(edge_in[...], d_pre_s[...], 0, 0), 0, 24, 0)
    snd_row = jnp.concatenate([snd_rows[n:n + 1] for n in range(snd_rows.shape[0])], axis=1)
    for block in range(4):
        ids = lax.broadcasted_iota(jnp.int32, (128, edge_in.shape[0]), 0) + 128 * block
        scattered[128 * block:128 * block + 128] = dot(as_bf16(snd_row == ids), d_pre_s[...])
    pass_on()
    store_grad(grad_ref, dot_wide_rows(node_all[...], scattered[...]), 512, 24, 0)
    store_grad(grad_ref, dot_wide_rows(node_own[...], recv_s[...]), 1024, 24, 0)
    d_local[...] = d_local[...] + dot_wide(recv_s[...], w_e1[1024:1536], 1)
    for part, (gain, bias) in enumerate(((gain_s[0], gain_s[1]), (d_gain_n, d_bias_n))):
        full = jnp.concatenate([gain.sum(axis=0, keepdims=True), bias.sum(axis=0, keepdims=True), jnp.zeros((6, 512), F32)], axis=0)
        for d in range(64):
            k = d // 16
            norm_grad[k, d // 4 % 4, d % 4, part] = full[:, 128 * k:128 * k + 128]


def half_of(ref, core):
    count = ref.shape[0] // 2
    return ref.at[pl.ds(pl.multiple_of(core * count, count), count)]


def no_hook(i):
    return None


def at_tile(plan):
    def hook(i):
        for tile, stages in plan.items():
            @pl.when(i == tile)
            def _():
                for plan_of, number in stages:
                    plan_of.stage(number)
    return hook


def forward_kernel(shard_low, shard_high, node_in, edge_in, snd_rows, mask_rows, node_all, node_all_one, edge_out, pre_e, out_e, sums, pre_n, out_n, *rest):
    mats = (rest[0:4], rest[5:9])
    norms = (rest[4], rest[9])
    recv_terms, grid_low, grid_high, snd_col, mask_col, send_sem, recv_sem = rest[10:]
    place = Place()
    wire = Wire(send_sem, recv_sem)
    low = Gather('low', place, wire, shard_low, grid_low)
    high = Gather('high', place, wire, shard_high, grid_high)
    node_own = half_of(node_all, place.core)
    grid_low[place.at[0], place.at[1], place.at[2]] = shard_low[...]
    grid_high[place.at[0], place.at[1], place.at[2]] = shard_high[...]
    node_own[...] = node_in[...]
    place.barrier()
    low.stage(0)
    high.stage(0)
    wire.start('node', lambda: node_in, lambda: half_of(node_all, place.core), place.partner)
    fill_columns(snd_rows, mask_rows, snd_col, mask_col)
    low.stage(1)
    high.stage(1)
    low.stage(2)
    low.stage(3)
    high.stage(2)
    low.stage(4)
    low.stage(5)
    unpack_weights(grid_low, *mats[0], norms[0])
    wire.wait_recv('node')
    w_e1, w_e2, w_n1, w_n2 = mats[0]
    hook = at_tile({1: [(high, 3)], 4: [(high, 4)]})
    edge_forward((node_all, node_own, edge_in, snd_col, mask_col), hook, edge_out, pre_e, out_e, sums, w_e1, w_e2, norms[0], recv_terms)
    branch, pre_b, out_b = node_forward(node_own, sums, w_n1, w_n2, norms[0])
    pre_n[...] = pre_b
    out_n[...] = out_b
    half_of(node_all_one, place.core)[...] = (node_own[...].astype(F32) + branch).astype(BF16)
    piece = lambda: half_of(node_all_one, place.core)
    wire.start('node_one', piece, piece, place.partner)
    high.stage(5)
    unpack_weights(grid_high, *mats[1], norms[1])
    wire.wait_recv('node_one')
    wire.finish()


def middle_kernel(node_all, edge_in, snd_rows, mask_rows, node_cot, edge_cot, w_e1, w_e2, w_n1, w_n2, norms, grad_ref, norm_grad, d_edge, d_local, scattered, returned, pre_e, out_e, sums, recv_terms, snd_col, mask_col, *rest):
    scratch = rest[:-2]
    place = Place()
    wire = Wire(*rest[-2:])
    place.barrier(ring=False)
    node_own = half_of(node_all, place.core)
    fill_columns(snd_rows, mask_rows, snd_col, mask_col)
    layer_io = (node_all, node_own, edge_in, snd_col, mask_col)
    edge_forward(layer_io, no_hook, None, pre_e, out_e, sums, w_e1, w_e2, norms, recv_terms)
    _, pre_n, out_n = node_forward(node_own, sums, w_n1, w_n2, norms)

    def pass_on():
        wire.start('scattered', lambda: half_of(scattered, 1 - place.core), lambda: returned, place.partner)
    layer_back(layer_io, node_cot[...].astype(F32), edge_cot, pre_e, out_e, sums, pre_n, out_n, (w_e1, w_e2, w_n1, w_n2), norms, snd_rows, (grad_ref, norm_grad, d_edge, d_local, scattered), scratch, lambda: None, no_hook, pass_on)
    wire.wait_recv('scattered')
    wire.finish()


def node_cotangent(d_local, scattered, returned, w_above, core):
    return (d_local[...] + dot_wide(half_of(scattered, core)[...] + returned[...], w_above[512:1024], 1)).astype(BF16)


def back_kernel(node_all, edge_in, snd_rows, mask_rows, d_local_above, scattered_above, returned_above, w_above, d_edge_new, pre_e, out_e, sums, pre_n, out_n, w_e1, w_e2, w_n1, w_n2, norms, grad_high, norm_high, grad_node, d_edge, total, grad_ref, norm_grad, d_local, scattered, returned, mask_col, snd_col, *rest):
    scratch, rest = rest[:6], rest[6:]
    load_sem, send_sem, recv_sem = rest[-3:]
    place = Place()
    wire = Wire(send_sem, recv_sem)
    plans = []
    for n, (name, sources, count, first, sem) in enumerate((
            ('high', [(grad_high, 0, 28), (norm_high, 0, 2)], 15, 0, load_sem),
            ('node', [(grad_ref, 16, 12)], 6, 15, None),
            ('edge', [(grad_ref, 0, 16), (norm_grad, 0, 2)], 9, 21, None))):
        own, theirs = rest[11 * n:11 * n + 2]
        plans.append(Reduce(name, place, wire, sources, own, theirs, rest[11 * n + 2:11 * n + 11], total, first, sem))
    high, node, edge = plans
    place.barrier()
    high.stage(0)
    node_own = half_of(node_all, place.core)
    fill_columns(snd_rows, mask_rows, snd_col, mask_col)
    layer_io = (node_all, node_own, edge_in, snd_col, mask_col)
    d_node = node_cotangent(d_local_above, scattered_above, returned_above, w_above, place.core).astype(F32)

    def after_nodes():
        node.stage(0)
        high.stage(1)

    def pass_on():
        wire.start('scattered', lambda: half_of(scattered, 1 - place.core), lambda: returned, place.partner)
    hook = at_tile({0: [(node, 1)], 3: [(high, 2)], 4: [(node, 2)], 6: [(high, 3)]})
    layer_back(layer_io, d_node, d_edge_new, pre_e, out_e, sums, pre_n[...], out_n[...], (w_e1, w_e2, w_n1, w_n2), norms, snd_rows, (grad_ref, norm_grad, d_edge, d_local, scattered), scratch, after_nodes, hook, pass_on)
    edge.stage(0)
    node.stage(3)
    edge.stage(1)
    high.stage(4)
    node.stage(4)
    wire.wait_recv('scattered')
    grad_node[...] = node_cotangent(d_local, scattered, returned, w_e1, place.core)
    high.stage(5)
    node.stage(5)
    edge.stage(2)
    edge.stage(3)
    high.stage(6)
    node.stage(6)
    for number in (4, 5, 6):
        edge.stage(number)
    for plan in (high, node, edge):
        plan.stage(7)
    wire.finish()


def vmem_call(kernel, name, inputs, outputs, scratch, flops, collective_id, copies, in_hbm=()):
    spec = pl.BlockSpec(memory_space=pltpu.VMEM)
    anywhere = pl.BlockSpec(memory_space=pl.ANY)
    return pl.pallas_call(
        kernel,
        out_shape=[jax.ShapeDtypeStruct(shape, dtype) for shape, dtype in outputs],
        in_specs=[spec] * len(inputs) + [anywhere] * len(in_hbm),
        out_specs=[spec] * len(outputs),
        scratch_shapes=[pltpu.VMEM(*entry) if isinstance(entry, tuple) else entry for entry in scratch] + [pltpu.SemaphoreType.DMA((copies,))] * 2,
        compiler_params=pltpu.CompilerParams(collective_id=collective_id, has_side_effects=True, vmem_limit_bytes=63 * 2 ** 20),
        cost_estimate=pl.CostEstimate(flops=flops, bytes_accessed=20 * 2 ** 20, transcendentals=0),
        name=name,
    )(*inputs, *in_hbm)


MAT_SHAPES = [((1536, 512), BF16), ((512, 512), BF16), ((1024, 512), BF16), ((512, 512), BF16), ((8, 512), F32)]
GRADS = [((4, 4, 4, 28, 8, 128), F32), ((4, 4, 4, 2, 8, 128), F32)]
BACK_SCRATCH = [((2048, 512), BF16)] * 3 + [((256, 512), BF16), ((256, 512), F32), ((2, 8, 512), F32)]
EDGE = ((2048, 512), BF16)
NODE = ((256, 512), BF16)
NODES = ((512, 512), BF16)
NODE_F32 = ((256, 512), F32)
NODES_F32 = ((512, 512), F32)
COLUMN = ((2048, 1), F32)
RECV_TERMS = ((3, 256, 512), BF16)


def adamw_update(master, grad_sum, moment_one, moment_two):
    corr_one = 1.0 - BETA_ONE ** STEP
    corr_two = 1.0 - BETA_TWO ** STEP
    one_new = BETA_ONE * moment_one + (1.0 - BETA_ONE) * grad_sum
    two_new = BETA_TWO * moment_two + (1.0 - BETA_TWO) * grad_sum * grad_sum
    direction = (one_new / corr_one) / (jnp.sqrt(two_new / corr_two) + ADAM_EPS)
    return master - LEARN_RATE * (direction + DECAY * master), one_new, two_new


def update_all(masters, moments_one, moments_two, layer_grads):
    new_master = []
    new_one = []
    new_two = []
    for slot in range(len(masters)):
        grad_sum = jnp.stack([per_layer[slot] for per_layer in layer_grads], axis=0)
        master_new, one_new, two_new = adamw_update(masters[slot], grad_sum, moments_one[slot], moments_two[slot])
        new_master.append(master_new)
        new_one.append(one_new)
        new_two.append(two_new)
    return tuple(new_master) + tuple(new_one) + tuple(new_two)


def rows_to_tiles(values, sub):
    rows = values.shape[0]
    return values.reshape(rows // sub, sub, 4, 128).transpose(0, 2, 1, 3).reshape(rows // sub * 4, sub, 128)


def tiles_to_rows(tiles):
    count, sub = tiles.shape[:2]
    return tiles.reshape(count // 4, 4, sub, 128).transpose(0, 2, 1, 3).reshape(count // 4 * sub, 512)


def pack_shards(masters):
    chip = lax.axis_index('dp')
    odd = lax.rem(chip, 2) == 1
    edge_one, edge_two, node_one, node_two, norm = [master.astype(BF16) for master in masters]
    main = jnp.where(odd, edge_one[:, 8:24], edge_one[:, 0:16])
    tail = jnp.where(odd, edge_one[:, 0:8], edge_one[:, 16:24])
    wide = jnp.tile(norm, (1, 1, 16))
    lanes = lax.broadcasted_iota(jnp.int32, wide.shape, 2) // 8
    norms = jnp.pad(jnp.where(lanes == lax.rem(chip, 16), wide, 0), ((0, 0), (0, 4), (0, 384)))
    return [rows_to_tiles(jnp.concatenate([main[n], node_one[n], tail[n], edge_two[n], node_two[n], norms[n]], axis=0), 16) for n in range(2)]


def unpack_grads(total):
    chip = lax.axis_index('dp')
    tiles_high = jnp.concatenate([total[0, 0:14], total[1, 0:14]], axis=0)
    tiles_low = jnp.concatenate([total[0, 21:29], total[1, 21:29], total[0, 15:21], total[1, 15:21]], axis=0)
    out = []
    for tiles, norm_at in ((tiles_low, 29), (tiles_high, 14)):
        rows = tiles_to_rows(tiles)
        norm = lax.dynamic_slice(total[:, norm_at, 0:2], (0, 0, lax.rem(chip, 16) * 8), (2, 2, 8)).reshape(4, 8)
        mats = []
        first = 0
        for size in (24, 8, 16, 8):
            mats.append(rows[first:first + size])
            first += size
        out.append(tuple(mats) + (norm,))
    return out


def solution(mesh):
    lat_spec = P('dp', 'sp', None)
    edge_spec = P('sp')
    mat_spec = P(None, 'dp', None)
    norm_spec = P(None, None, 'dp')
    param_specs = (mat_spec, mat_spec, mat_spec, mat_spec, norm_spec)

    def train_step(node_lat, edge_lat, senders, edge_mask, node_cot, edge_cot, w_edge1, w_edge2, w_node1, w_node2, norm_par, mom_edge1, mom_edge2, mom_node1, mom_node2, mom_norm, vel_edge1, vel_edge2, vel_node1, vel_node2, vel_norm):
        masters = (w_edge1, w_edge2, w_node1, w_node2, norm_par)
        moments_one = (mom_edge1, mom_edge2, mom_node1, mom_node2, mom_norm)
        moments_two = (vel_edge1, vel_edge2, vel_node1, vel_node2, vel_norm)
        snd_rows = senders.reshape(-1, 128)
        mask_rows = edge_mask.reshape(-1, 128)
        shard_low, shard_high = pack_shards(masters)
        grid = pltpu.VMEM((RING, RING, RING) + shard_low.shape, BF16)
        outs = vmem_call(forward_kernel, 'gather_forward', (shard_low, shard_high, node_lat[0], edge_lat[0], snd_rows, mask_rows), [NODES, NODES, EDGE, EDGE, EDGE, NODE, NODE, NODE] + MAT_SHAPES + MAT_SHAPES, [RECV_TERMS, grid, grid, COLUMN, COLUMN], 5 * 10 ** 9, 1, 2 * GATHER_COPIES + 2)
        node_all, node_all_one, edge_one, pre_e, out_e, sums, pre_n, out_n = outs[:8]
        mats_low = outs[8:13]
        mats_high = outs[13:18]
        grad_high, norm_high, d_edge_one, d_local_one, scattered_one, returned_one = vmem_call(middle_kernel, 'forward_back_high', (node_all_one, edge_one, snd_rows, mask_rows, node_cot[0], edge_cot[0]) + tuple(mats_high), GRADS + [EDGE, NODE_F32, NODES_F32, NODE_F32], [EDGE, EDGE, NODE, RECV_TERMS, COLUMN, COLUMN] + BACK_SCRATCH, 13 * 10 ** 9, 2, 1)
        reduce_bufs = reduce_scratch(15) + reduce_scratch(6) + reduce_scratch(9)
        inputs = (node_all, edge_lat[0], snd_rows, mask_rows, d_local_one, scattered_one, returned_one, mats_high[0], d_edge_one, pre_e, out_e, sums, pre_n, out_n) + tuple(mats_low)
        grad_node, d_edge_zero, total = vmem_call(back_kernel, 'back_low_reduce', inputs, [NODE, EDGE, ((2, 30, 8, 128), F32)], GRADS + [NODE_F32, NODES_F32, NODE_F32, COLUMN, COLUMN] + BACK_SCRATCH + reduce_bufs + [pltpu.SemaphoreType.DMA((16,))], 8 * 10 ** 9, 3, 200, (grad_high, norm_high))
        new_state = update_all(masters, moments_one, moments_two, unpack_grads(total))
        return new_state + (grad_node[None], d_edge_zero[None])

    return jax.shard_map(train_step, mesh=mesh, in_specs=(lat_spec, lat_spec, edge_spec, edge_spec, lat_spec, lat_spec) + param_specs + param_specs + param_specs, out_specs=param_specs + param_specs + param_specs + (lat_spec, lat_spec), check_vma=False)
```

```python
import functools

import jax
import jax.numpy as jnp
from jax import lax
from jax.experimental import pallas as pl
from jax.experimental.pallas import tpu as pltpu
from jax.sharding import PartitionSpec as P

NORM_EPS = 1e-5
LEARN_RATE = 1e-3
BETA_ONE = 0.9
BETA_TWO = 0.95
ADAM_EPS = 1e-8
DECAY = 0.1
STEP = 10

MESH_ID = pl.DeviceIdType.MESH
ORDERS = ((0, 1, 2), (1, 2, 0), (2, 0, 1))
RING = 4
HOPS = (1, -1, 2)


class Place:
    def __init__(self):
        chip = lax.axis_index('dp')
        self.core = lax.axis_index('sp')
        self.at = (lax.rem(chip // 16, 4), lax.rem(chip // 4, 4), lax.rem(chip, 4))

    def step(self, dim, delta):
        return lax.rem(self.at[dim] + (delta + RING), RING)

    def chip(self, dim, delta):
        pos = list(self.at)
        pos[dim] = self.step(dim, delta)
        return {'dp': pos[0] * 16 + pos[1] * 4 + pos[2]}

    def partner(self):
        return {'sp': 1 - self.core}

    def peers(self):
        return [self.partner()] + [self.chip(dim, delta) for dim in range(3) for delta in HOPS]

    def barrier(self):
        sem = pltpu.get_barrier_semaphore()
        peers = self.peers()
        for peer in peers:
            pl.semaphore_signal(sem, inc=1, device_id=peer, device_id_type=MESH_ID)
        pl.semaphore_wait(sem, len(peers))


class Wire:
    def __init__(self, send_sem, recv_sem):
        self.sems = (send_sem, recv_sem)
        self.slots = {}
        self.parts = {}

    def describe(self, key):
        source, target, where = self.parts[key]
        slot = self.slots.setdefault(key, len(self.slots))
        return pltpu.make_async_remote_copy(src_ref=source(), dst_ref=target(), send_sem=self.sems[0].at[slot], recv_sem=self.sems[1].at[slot], device_id=where(), device_id_type=MESH_ID)

    def start(self, key, source, target, where):
        self.parts[key] = (source, target, where)
        self.describe(key).start()

    def wait_recv(self, key):
        self.describe(key).wait_recv()

    def finish(self):
        for key in list(self.parts):
            self.describe(key).wait_send()


class Credit:
    def __init__(self, place, sem):
        self.place, self.sem = place, sem

    def stage(self, number):
        pl.semaphore_signal(self.sem, inc=1, device_id=self.place.partner(), device_id_type=MESH_ID)


def split_groups(count):
    base, extra = divmod(count, 3)
    sizes = [base + (1 if g < extra else 0) for g in range(3)]
    starts = [sum(sizes[:g]) for g in range(3)]
    return list(zip(starts, sizes))


class Gather:
    def __init__(self, name, place, wire, src_ref, grid_ref):
        self.name, self.place, self.wire = name, place, wire
        self.src, self.grid = src_ref, grid_ref
        self.half = src_ref.shape[0] // 2
        self.first = place.core * self.half
        self.groups = split_groups(self.half)
        self.shared = []

    def region(self, g, phase, delta, side=None):
        order = ORDERS[g]
        start, size = self.groups[g]
        index = list(self.place.at)
        for q in range(phase):
            index[order[q]] = pl.ds(0, RING)
        index[order[phase]] = self.place.step(order[phase], delta)
        if side is not None:
            index[order[0]] = pl.ds(2 * side, 2)
        return self.grid.at[index[0], index[1], index[2], pl.ds(self.first + start, size)]

    def send(self, g, phase, delta, toward, tag, side=None):
        dim = ORDERS[g][phase]
        piece = functools.partial(self.region, g, phase, delta, side)
        origin = piece
        if phase == 0:
            start, size = self.groups[g]
            origin = lambda: self.src.at[pl.ds(self.first + start, size)]
        self.wire.start((self.name, g, phase, tag), origin, piece, lambda: self.place.chip(dim, toward))

    def share(self, g, phase, delta):
        key = (self.name, g, phase, 'share', delta)
        self.shared.append(key)
        piece = functools.partial(self.region, g, phase, delta)
        self.wire.start(key, piece, piece, self.place.partner)

    def begin(self, phase):
        for g in range(3):
            for toward in (HOPS if phase < 2 else (1, -1)):
                self.send(g, phase, 0, toward, toward)

    def arrived(self, g, phase, tag):
        self.wire.wait_recv((self.name, g, phase, tag))

    def stage(self, number):
        if number == 0:
            self.begin(0)
        elif number in (1, 2):
            for g in range(3):
                for toward in HOPS:
                    self.arrived(g, number - 1, toward)
            self.begin(number)
            for g in range(3):
                for toward in HOPS:
                    self.share(g, number - 1, -toward)
        elif number == 3:
            for g in range(3):
                self.arrived(g, 2, 1)
                self.send(g, 2, -1, 1, 'on_right', 0)
                self.arrived(g, 2, -1)
                self.send(g, 2, 1, -1, 'on_left', 1)
            for g in range(3):
                self.share(g, 2, -1)
                self.share(g, 2, 1)
        elif number == 4:
            for g in range(3):
                self.arrived(g, 2, 'on_right')
                self.arrived(g, 2, 'on_left')
                self.share(g, 2, 2)
        else:
            for key in self.shared:
                self.wire.wait_recv(key)


GATHER_COPIES = 3 * (3 + 3 + 4 + 3 + 3 + 3)


class Reduce:
    def __init__(self, name, place, wire, source, first, count, bufs, out_ref, out_first, own=None, load_sem=None):
        self.name, self.place, self.wire = name, place, wire
        self.source, self.first, self.count = source, first, count // 2
        self.theirs, self.boxes = bufs[0], bufs[1:10]
        self.out, self.out_first, self.load_sem = out_ref, out_first, load_sem
        self.own, self.base = (source, first + place.core * self.count) if own is None else (own, 0)
        self.groups = split_groups(self.count)
        self.turns = (2, 1, -1, 0)

    def index_of(self, g, phase, delta, side=None):
        order = ORDERS[g]
        index = [pl.ds(0, RING)] * 3
        for q in range(phase):
            index[order[q]] = self.place.at[order[q]]
        index[order[phase]] = self.place.step(order[phase], delta)
        if side is not None:
            index[order[phase + 1]] = pl.ds(2 * side, 2)
        return index

    def kept(self, g, phase, delta, side=None):
        index = self.index_of(g, phase, delta, side)
        start, size = self.groups[g]
        return self.own.at[index[0], index[1], index[2], pl.ds(self.base + start, size)]

    def piece(self, g, delta, core):
        index = self.index_of(g, 0, delta)
        start, size = self.groups[g]
        return self.source.at[index[0], index[1], index[2], pl.ds(self.first + core * self.count + start, size)]

    def slot(self, g, delta):
        index = self.index_of(g, 0, delta)
        return self.theirs.at[index[0], index[1], index[2], pl.ds(*self.groups[g])]

    def load(self, g, delta):
        return pltpu.make_async_copy(self.piece(g, delta, self.place.core), self.kept(g, 0, delta), self.load_sem.at[self.turns.index(delta) * 3 + g])

    def ready(self, g, delta):
        if self.load_sem is not None:
            self.load(g, delta).wait()
        self.wire.wait_recv((self.name, 'swap', g, delta))
        target = self.kept(g, 0, delta)
        target[...] = target[...] + self.slot(g, delta)[...]

    def box(self, g, phase, number):
        return self.boxes[g * 3 + phase].at[number]

    def send(self, g, phase, tag, delta, side, number, toward):
        dim = ORDERS[g][phase]
        self.wire.start((self.name, g, phase, tag), functools.partial(self.kept, g, phase, delta, side), functools.partial(self.box, g, phase, number), lambda: self.place.chip(dim, toward))

    def absorb(self, g, phase, tag, delta, side, number):
        self.wire.wait_recv((self.name, g, phase, tag))
        target = self.kept(g, phase, delta, side)
        target[...] = target[...] + self.box(g, phase, number)[...]

    def far(self, g, phase):
        self.send(g, phase, 'far_right', 2, 0, 0, 1)
        self.send(g, phase, 'far_left', 2, 1, 2, -1)

    def near(self, g, phase):
        self.send(g, phase, 'near_right', 1, 1, 1, 1)
        self.send(g, phase, 'near_left', -1, 0, 3, -1)

    def onward(self, g, phase):
        self.absorb(g, phase, 'far_right', 1, 0, 0)
        self.send(g, phase, 'sum_right', 1, 0, 4, 1)
        self.absorb(g, phase, 'far_left', -1, 1, 2)
        self.send(g, phase, 'sum_left', -1, 1, 5, -1)

    def settle(self, g, phase):
        for tag, number, side in (('near_left', 3, 0), ('near_right', 1, 1), ('sum_right', 4, 0), ('sum_left', 5, 1)):
            self.absorb(g, phase, tag, 0, side, number)

    def stage(self, number):
        if number == 0:
            for delta in self.turns:
                for g in range(3):
                    if self.load_sem is not None:
                        self.load(g, delta).start()
                    self.wire.start((self.name, 'swap', g, delta), functools.partial(self.piece, g, delta, 1 - self.place.core), functools.partial(self.slot, g, delta), self.place.partner)
        elif number == 1:
            for g in range(3):
                self.ready(g, 2)
                self.far(g, 0)
            for g in range(3):
                self.ready(g, 1)
                self.ready(g, -1)
                self.near(g, 0)
        elif number == 2:
            for g in range(3):
                self.onward(g, 0)
            for g in range(3):
                self.ready(g, 0)
        elif number == 3:
            for g in range(3):
                self.settle(g, 0)
                self.far(g, 1)
                self.near(g, 1)
        elif number == 4:
            for g in range(3):
                self.onward(g, 1)
        elif number == 5:
            for g in range(3):
                self.settle(g, 1)
                for n, toward in enumerate(HOPS):
                    self.send(g, 2, toward, toward, None, n, toward)
        elif number == 6:
            for g in range(3):
                for n, toward in enumerate(HOPS):
                    self.absorb(g, 2, toward, 0, None, n)
            span = lambda: self.out.at[self.place.core, pl.ds(self.out_first, self.count)]
            span()[...] = self.own[self.place.at[0], self.place.at[1], self.place.at[2], pl.ds(self.base, self.count)]
            self.wire.start((self.name, 'result'), span, span, self.place.partner)
        else:
            self.wire.wait_recv((self.name, 'result'))


def box_shapes(count):
    out = []
    for g, (_, size) in enumerate(split_groups(count)):
        order = ORDERS[g]
        dims = {dim: RING for dim in range(3) if dim != order[0]}
        dims[order[1]] = 2
        out.append((6,) + tuple(dims[dim] for dim in sorted(dims)) + (size, 8, 128))
        out.append((6, 2, size, 8, 128))
        out.append((3, size, 8, 128))
    return out


def reduce_scratch(count):
    grid = pltpu.VMEM((RING, RING, RING, count, 8, 128), jnp.float32)
    return [grid] + [pltpu.VMEM(shape, jnp.float32) for shape in box_shapes(count)]


REDUCE_COPIES = 12 + 3 * 15 + 1


TILE = 256
NODE_TILE = TILE // 8
BF16 = jnp.bfloat16
F32 = jnp.float32


def dot(left, right, left_dim=1, right_dim=0):
    return lax.dot_general(left, right, (((left_dim,), (right_dim,)), ((), ())), preferred_element_type=F32)


def split_three(values):
    high = values.astype(BF16)
    rest = values - high.astype(F32)
    mid = rest.astype(BF16)
    low = (rest - mid.astype(F32)).astype(BF16)
    return high, mid, low


def dot_wide(values, right, right_dim=0):
    high, mid, low = split_three(values)
    return dot(high, right, 1, right_dim) + dot(mid, right, 1, right_dim) + dot(low, right, 1, right_dim)


def dot_wide_rows(left, values):
    high, mid, low = split_three(values)
    return dot(left, high, 0, 0) + dot(left, mid, 0, 0) + dot(left, low, 0, 0)


def norm_stats(out_b):
    values = out_b.astype(F32)
    centered = values - jnp.mean(values, axis=-1, keepdims=True)
    inv_std = lax.rsqrt(jnp.mean(centered * centered, axis=-1, keepdims=True) + NORM_EPS)
    return centered * inv_std, inv_std


def mlp_forward(pre_act, w_two, gain, bias):
    pre_b = pre_act.astype(BF16)
    hidden = jax.nn.silu(pre_b.astype(F32)).astype(BF16)
    out_b = dot(hidden, w_two).astype(BF16)
    normed, _ = norm_stats(out_b)
    return normed * gain + bias, pre_b, out_b


def mlp_cotangents(d_branch, pre_b, out_b, w_two, gain):
    normed, inv_std = norm_stats(out_b)
    d_norm = d_branch * gain
    d_out = (inv_std * (d_norm - jnp.mean(d_norm, axis=-1, keepdims=True) - normed * jnp.mean(d_norm * normed, axis=-1, keepdims=True))).astype(BF16)
    d_act = dot(d_out, w_two, 1, 1).astype(BF16)
    pre_f = pre_b.astype(F32)
    gate = jax.nn.sigmoid(pre_f)
    hidden = (pre_f * gate).astype(BF16)
    d_pre = (d_act.astype(F32) * gate * (1.0 + pre_f * (1.0 - gate))).astype(BF16)
    d_gain = (d_branch * normed).reshape(-1, 8, d_branch.shape[-1]).sum(axis=0)
    d_bias = d_branch.reshape(-1, 8, d_branch.shape[-1]).sum(axis=0)
    return d_out, hidden, d_pre, d_gain, d_bias


def receiver_pick(copies):
    rows = lax.broadcasted_iota(jnp.int32, (TILE, copies * NODE_TILE), 0)
    cols = lax.broadcasted_iota(jnp.int32, (TILE, copies * NODE_TILE), 1)
    return lax.shift_right_logical(rows, 3) == lax.bitwise_and(cols, NODE_TILE - 1)


def as_bf16(flags):
    return jnp.where(flags, 1.0, 0.0).astype(BF16)


def unpack_weights(grid, w_e1, w_e2, w_n1, w_n2, norms):
    def pair(p, carry):
        at = (p // 8, lax.rem(p // 2, 4))
        x = lax.rem(p, 2) * 2
        for k in range(4):
            lanes = pl.ds(128 * k, 128)
            for dev in range(2):
                w_e1[pl.ds(pl.multiple_of(48 * p + 32 * dev, 16), 16), lanes] = grid[at[0], at[1], x + dev, k]
                w_n1[pl.ds(pl.multiple_of(32 * p + 16 * dev, 16), 16), lanes] = grid[at[0], at[1], x + dev, 4 + k]
            for ref, first, tile, top in ((w_e1, 48 * p + 16, 8, 0), (w_e2, 16 * p, 8, 8), (w_n2, 16 * p, 12, 0)):
                even = grid[at[0], at[1], x, tile + k].astype(F32)[top:top + 8]
                odd = grid[at[0], at[1], x + 1, tile + k].astype(F32)[top:top + 8]
                ref[pl.ds(pl.multiple_of(first, 16), 16), lanes] = jnp.concatenate([even, odd], axis=0).astype(BF16)
        return carry
    lax.fori_loop(0, 32, pair, 0)
    for k in range(4):
        total = grid[k, 0, 0, 12].astype(F32)
        for d in range(1, 16):
            total = total + grid[k, d // 4, d % 4, 12].astype(F32)
        norms[:, 128 * k:128 * k + 128] = total[8:16]


def fill_columns(snd_rows, mask_rows, snd_col, mask_col):
    for rows, col in ((snd_rows, snd_col), (mask_rows, mask_col)):
        turned = rows[...].astype(F32).T
        for n in range(rows.shape[0]):
            col[128 * n:128 * n + 128, :] = turned[:, n:n + 1]


def edge_forward(layer_io, hook, edge_out, pre_out, out_out, sums_out, w_e1, w_e2, norms, recv_terms):
    node_all, node_own, edge_in, snd_col, mask_col = layer_io
    for part, term in enumerate(split_three(dot(node_own[...], w_e1[1024:1536]))):
        recv_terms[part] = term

    def tile(i, carry):
        rows = pl.ds(pl.multiple_of(i * TILE, TILE), TILE)
        nodes = pl.ds(pl.multiple_of(i * NODE_TILE, NODE_TILE), NODE_TILE)
        ids = lax.broadcasted_iota(jnp.int32, (TILE, 512), 1)
        sender = dot(as_bf16(snd_col[rows].astype(jnp.int32) == ids), node_all[...]).astype(BF16)
        recv = jnp.concatenate([recv_terms[0, nodes], recv_terms[1, nodes], recv_terms[2, nodes]], axis=0)
        edge = edge_in[rows]
        pre = dot(edge, w_e1[0:512]) + dot(sender, w_e1[512:1024]) + dot(as_bf16(receiver_pick(3)), recv)
        branch, pre_b, out_b = mlp_forward(pre, w_e2[...], norms[0:1], norms[1:2])
        edge_new = (edge.astype(F32) + branch).astype(BF16)
        pre_out[rows] = pre_b
        out_out[rows] = out_b
        if edge_out is not None:
            edge_out[rows] = edge_new
        picked = jnp.where(receiver_pick(1), mask_col[rows], 0.0).astype(BF16)
        sums_out[nodes] = dot(picked, edge_new, 0, 0).astype(BF16)
        hook(i)
        return carry
    lax.fori_loop(0, edge_in.shape[0] // TILE, tile, 0)


def node_forward(node_own, sums, w_n1, w_n2, norms):
    pre = dot(node_own[...], w_n1[0:512]) + dot(sums[...], w_n1[512:1024])
    return mlp_forward(pre, w_n2[...], norms[2:3], norms[3:4])


def lane_tiles(values):
    return [values[:, 128 * k:128 * k + 128].reshape(-1, 8, 128) for k in range(4)]


def tile_at(tile):
    return tile + tile // 8 if tile < 16 else tile + 2


def store_square(grad_ref, values, first_tile):
    for k, tiles in enumerate(lane_tiles(values)):
        grad_ref[:, :, :, tile_at(first_tile + k)] = tiles.reshape(4, 4, 4, 8, 128)


def store_double(grad_ref, values, first_tile, part):
    for k, tiles in enumerate(lane_tiles(values)):
        tiles = tiles.reshape(2, 4, 4, 2, 8, 128)
        for r in range(2):
            grad_ref[2 * part:2 * part + 2, :, :, tile_at(first_tile + 4 * r + k)] = tiles[:, :, :, r]


def store_triple(grad_ref, values, first_pair):
    for n in range(values.shape[0] // 96):
        pair = first_pair + n
        for k, tiles in enumerate(lane_tiles(values[96 * n:96 * n + 96])):
            tiles = tiles.reshape(4, 3, 8, 128)
            for r in range(3):
                grad_ref[pair // 4, pair % 4, :, tile_at(4 * r + k)] = tiles[:, r]


def layer_back(layer_io, d_node_new, d_edge_new, pre_e, out_e, sums, pre_n, out_n, mats, norms, snd_rows, outs, scratch, after_nodes, hook, pass_on):
    node_all, node_own, edge_in, snd_col, mask_col = layer_io
    w_e1, w_e2, w_n1, w_n2 = mats
    grad_ref, d_edge, d_local, scattered = outs
    hidden_s, d_pre_s, d_out_s, d_sum_s, recv_s, gain_s = scratch
    d_out_n, hidden_n, d_pre_n, d_gain_n, d_bias_n = mlp_cotangents(d_node_new, pre_n, out_n, w_n2[...], norms[2:3])
    d_sum_s[...] = dot(d_pre_n, w_n1[512:1024], 1, 1).astype(BF16)
    d_local[...] = d_node_new + dot(d_pre_n, w_n1[0:512], 1, 1)
    store_square(grad_ref, dot(hidden_n, d_out_n, 0, 0), 24)
    store_double(grad_ref, dot(node_own[...], d_pre_n, 0, 0), 16, 0)
    store_double(grad_ref, dot(sums[...], d_pre_n, 0, 0), 16, 1)
    after_nodes()
    gain_s[...] = jnp.zeros_like(gain_s)

    def tile(i, carry):
        rows = pl.ds(pl.multiple_of(i * TILE, TILE), TILE)
        nodes = pl.ds(pl.multiple_of(i * NODE_TILE, NODE_TILE), NODE_TILE)
        pick = receiver_pick(1)
        picked = jnp.where(pick, mask_col[rows], 0.0).astype(BF16)
        d_res = (d_edge_new[rows].astype(F32) + dot(picked, d_sum_s[nodes])).astype(BF16).astype(F32)
        d_out, hidden, d_pre, d_gain, d_bias = mlp_cotangents(d_res, pre_e[rows], out_e[rows], w_e2[...], norms[0:1])
        gain_s[0] = gain_s[0] + d_gain
        gain_s[1] = gain_s[1] + d_bias
        hidden_s[rows] = hidden
        d_out_s[rows] = d_out
        d_pre_s[rows] = d_pre
        d_edge[rows] = d_res.astype(BF16)
        recv_s[nodes] = dot(as_bf16(pick), d_pre, 0, 0)
        hook(i)
        return carry
    lax.fori_loop(0, edge_in.shape[0] // TILE, tile, 0)
    store_square(grad_ref, dot(hidden_s[...], d_out_s[...], 0, 0), 12)
    upper = dot(edge_in[...], d_pre_s[...], 0, 0)
    store_triple(grad_ref, upper[0:480], 0)
    snd_row = jnp.concatenate([snd_rows[n:n + 1] for n in range(snd_rows.shape[0])], axis=1)
    for block in range(4):
        ids = lax.broadcasted_iota(jnp.int32, (128, edge_in.shape[0]), 0) + 128 * block
        scattered[128 * block:128 * block + 128] = dot(as_bf16(snd_row == ids), d_pre_s[...])
    pass_on()
    middle = dot_wide_rows(node_all[...], scattered[...])
    store_triple(grad_ref, jnp.concatenate([upper[480:512], middle[0:448]], axis=0), 5)
    lower = dot_wide_rows(node_own[...], recv_s[...])
    store_triple(grad_ref, jnp.concatenate([middle[448:512], lower], axis=0), 10)
    for part, (gain, bias) in enumerate(((gain_s[0], gain_s[1]), (d_gain_n, d_bias_n))):
        full = jnp.concatenate([gain.sum(axis=0, keepdims=True), bias.sum(axis=0, keepdims=True), jnp.zeros((6, 512), F32)], axis=0)
        for k in range(4):
            grad_ref[k, :, :, 8 + 9 * part] = jnp.broadcast_to(full[:, 128 * k:128 * k + 128], (4, 4, 8, 128))


def layer_back_late(w_e1, d_edge, d_local, scratch):
    d_pre_s, recv_s = scratch[1], scratch[4]

    def tile(i, carry):
        rows = pl.ds(pl.multiple_of(i * TILE, TILE), TILE)
        d_edge[rows] = (d_edge[rows].astype(F32) + dot(d_pre_s[rows], w_e1[0:512], 1, 1)).astype(BF16)
        return carry
    lax.fori_loop(0, d_edge.shape[0] // TILE, tile, 0)
    d_local[...] = d_local[...] + dot_wide(recv_s[...], w_e1[1024:1536], 1)


def half_of(ref, core):
    count = ref.shape[0] // 2
    return ref.at[pl.ds(pl.multiple_of(core * count, count), count)]


def no_hook(i):
    return None


def at_tile(plan):
    def hook(i):
        for tile, stages in plan.items():
            @pl.when(i == tile)
            def _():
                for plan_of, number in stages:
                    plan_of.stage(number)
    return hook


def pack_shard(layer, masters, shard, norm_pad):
    edge_one, edge_two, node_one, node_two, norm_rows = masters
    chip = lax.axis_index('dp')
    odd = lax.rem(chip, 2) == 1
    norm_pad[...] = jnp.zeros_like(norm_pad)
    norm_pad[0:4, 0:8] = norm_rows[layer]
    placed = pltpu.roll(norm_pad[...], lax.rem(chip, 16) * 8, 1)
    for k in range(4):
        lanes = slice(128 * k, 128 * k + 128)
        first, mid, last = edge_one[layer, 0:8, lanes], edge_one[layer, 8:16, lanes], edge_one[layer, 16:24, lanes]
        shard[k] = jnp.concatenate([jnp.where(odd, mid, first), jnp.where(odd, last, mid)], axis=0).astype(BF16)
        shard[4 + k] = node_one[layer, :, lanes].astype(BF16)
        shard[8 + k] = jnp.concatenate([jnp.where(odd, first, last), edge_two[layer, :, lanes]], axis=0).astype(BF16)
        shard[12 + k] = jnp.concatenate([node_two[layer, :, lanes], placed if k == 0 else jnp.zeros_like(placed)], axis=0).astype(BF16)


def node_cotangent(d_local, scattered, returned, w_above, core):
    return (d_local[...] + dot_wide(half_of(scattered, core)[...] + returned[...], w_above[512:1024], 1)).astype(BF16)


def pack_kernel(edge_one, edge_two, node_one, node_two, norm_rows, shard_low, shard_high, norm_pad):
    for layer, shard in enumerate((shard_low, shard_high)):
        pack_shard(layer, (edge_one, edge_two, node_one, node_two, norm_rows), shard, norm_pad)


def pack_call(masters):
    spec = pl.BlockSpec(memory_space=pltpu.VMEM)
    shard = jax.ShapeDtypeStruct((16, 16, 128), BF16)
    return pl.pallas_call(pack_kernel, out_shape=[shard, shard], in_specs=[spec] * 5, out_specs=[spec] * 2, scratch_shapes=[pltpu.VMEM((8, 128), F32)], compiler_params=pltpu.CompilerParams(vmem_limit_bytes=67043328), name='pack')(*masters)


def step_kernel(shard_low, shard_high, node_in, snd_rows, mask_rows, node_cot, edge_lat, edge_cot, grad_node, d_edge, total, node_all, node_all_one, edge_in, pre_low, out_low, pre_high, out_high, d_pre, snd_col, mask_col, sums_low, sums_high, pre_node, out_node, recv_terms, d_sum, recv_sum, gain_sum, d_local, scattered_high, scattered_low, returned_high, returned_low, *rest):
    mats_low, norms_low, mats_high, norms_high = rest[0:4], rest[4], rest[5:9], rest[9]
    load_sem, credit_sem, peer_sem, send_sem, recv_sem = rest[10:]
    wire = Wire(send_sem, recv_sem)
    load_edge = lambda n: pltpu.make_async_copy(edge_lat, edge_in, load_sem.at[n])
    load_cot = lambda: pltpu.make_async_copy(edge_cot, d_edge, load_sem.at[1])
    load_edge(0).start()
    load_cot().start()

    def begin():
        place = Place()
        node_own = half_of(node_all, place.core)
        node_own_one = half_of(node_all_one, place.core)
        return place, (node_all, node_own, edge_in, snd_col, mask_col), (node_all_one, node_own_one, edge_in, snd_col, mask_col)

    def gather_and_first(grid_low, grid_high):
        place, low_io, high_io = begin()
        node_own, node_own_one = low_io[1], high_io[1]
        for shard, grid in ((shard_low, grid_low), (shard_high, grid_high)):
            grid[place.at[0], place.at[1], place.at[2]] = shard[...]
        node_own[...] = node_in[...]
        place.barrier()
        low = Gather('low', place, wire, shard_low, grid_low)
        high = Gather('high', place, wire, shard_high, grid_high)
        low.stage(0)
        high.stage(0)
        wire.start('node', lambda: node_in, lambda: half_of(node_all, place.core), place.partner)
        fill_columns(snd_rows, mask_rows, snd_col, mask_col)
        low.stage(1)
        high.stage(1)
        low.stage(2)
        low.stage(3)
        high.stage(2)
        low.stage(4)
        low.stage(5)
        unpack_weights(grid_low, *mats_low, norms_low)
        wire.wait_recv('node')
        load_edge(0).wait()
        hook = at_tile({1: [(high, 3)], 4: [(high, 4)]})
        edge_forward(low_io, hook, edge_in, pre_low, out_low, sums_low, mats_low[0], mats_low[1], norms_low, recv_terms)
        branch, pre_b, out_b = node_forward(node_own, sums_low, mats_low[2], mats_low[3], norms_low)
        pre_node[...] = pre_b
        out_node[...] = out_b
        node_own_one[...] = (node_own[...].astype(F32) + branch).astype(BF16)
        piece = lambda: half_of(node_all_one, place.core)
        wire.start('node_one', piece, piece, place.partner)
        high.stage(5)
        unpack_weights(grid_high, *mats_high, norms_high)
        wire.wait_recv('node_one')
        wire.finish()
        wire.parts.clear()

    def second_and_back(grad_high, grad_low, theirs_edge, theirs_node, *boxes):
        place, low_io, high_io = begin()
        node_own_one = high_io[1]
        peers = place.peers()
        for peer in peers:
            pl.semaphore_signal(peer_sem, inc=1, device_id=peer, device_id_type=MESH_ID)
        high_node = Reduce('high_node', place, wire, grad_high, 18, 12, (theirs_node,) + boxes[0:9], total, 24)
        high_edge = Reduce('high_edge', place, wire, grad_high, 0, 18, (theirs_edge,) + boxes[9:18], total, 0)
        low_node = Reduce('low_node', place, wire, grad_low, 18, 12, (theirs_node,) + boxes[18:27], total, 9)
        low_edge = Reduce('low_edge', place, wire, grad_low, 0, 18, (theirs_edge,) + boxes[27:36], total, 15)
        edge_forward(high_io, no_hook, None, pre_high, out_high, sums_high, mats_high[0], mats_high[1], norms_high, recv_terms)
        _, pre_n, out_n = node_forward(node_own_one, sums_high, mats_high[2], mats_high[3], norms_high)
        load_cot().wait()

        def pass_on_high():
            wire.start('scattered_high', lambda: half_of(scattered_high, 1 - place.core), lambda: returned_high, place.partner)

        def after_nodes_high():
            pl.semaphore_wait(peer_sem, len(peers))
            high_node.stage(0)
        hook = at_tile({1: [(high_node, 1)], 3: [(high_node, 2), (Credit(place, credit_sem.at[0]), 0)], 5: [(high_node, 3)], 7: [(high_node, 4)]})
        scratch = (pre_high, d_pre, out_high, d_sum, recv_sum, gain_sum)
        layer_back(high_io, node_cot[...].astype(F32), d_edge, pre_high, out_high, sums_high, pre_n, out_n, mats_high, norms_high, snd_rows, (grad_high, d_edge, d_local, scattered_high), scratch, after_nodes_high, hook, pass_on_high)
        load_edge(2).start()
        high_edge.stage(0)
        high_node.stage(5)
        layer_back_late(mats_high[0], d_edge, d_local, scratch)
        wire.wait_recv('scattered_high')
        d_node = node_cotangent(d_local, scattered_high, returned_high, mats_high[0], place.core).astype(F32)
        load_edge(2).wait()

        def pass_on_low():
            wire.start('scattered_low', lambda: half_of(scattered_low, 1 - place.core), lambda: returned_low, place.partner)

        def after_nodes_low():
            high_edge.stage(1)
            pl.semaphore_wait(credit_sem.at[0], 1)
            low_node.stage(0)
        hook = at_tile({0: [(high_node, 6)], 1: [(low_node, 1)], 2: [(high_edge, 2), (Credit(place, credit_sem.at[1]), 0)], 3: [(low_node, 2)], 4: [(high_edge, 3)], 5: [(low_node, 3)], 6: [(high_edge, 4)], 7: [(low_node, 4)]})
        scratch = (pre_low, d_pre, out_low, d_sum, recv_sum, gain_sum)
        layer_back(low_io, d_node, d_edge, pre_low, out_low, sums_low, pre_node[...], out_node[...], mats_low, norms_low, snd_rows, (grad_low, d_edge, d_local, scattered_low), scratch, after_nodes_low, hook, pass_on_low)
        pl.semaphore_wait(credit_sem.at[1], 1)
        low_edge.stage(0)
        high_edge.stage(5)
        low_node.stage(5)
        low_edge.stage(1)
        layer_back_late(mats_low[0], d_edge, d_local, scratch)
        high_edge.stage(6)
        low_node.stage(6)
        low_edge.stage(2)
        wire.wait_recv('scattered_low')
        grad_node[...] = node_cotangent(d_local, scattered_low, returned_low, mats_low[0], place.core)
        for number in (3, 4, 5, 6):
            low_edge.stage(number)
        for plan in (high_node, high_edge, low_node, low_edge):
            plan.stage(7)
        wire.finish()

    grid = pltpu.VMEM((RING, RING, RING, 16, 16, 128), BF16)
    pl.run_scoped(gather_and_first, grid, grid)
    grad = pltpu.VMEM((RING, RING, RING, 30, 8, 128), F32)
    theirs = [pltpu.VMEM((RING, RING, RING, count, 8, 128), F32) for count in (9, 6)]
    boxes = [pltpu.VMEM(shape, F32) for count in (6, 9, 6, 9) for shape in box_shapes(count)]
    pl.run_scoped(second_and_back, grad, grad, *theirs, *boxes)


def step_call(vmem_inputs, hbm_inputs):
    spec = pl.BlockSpec(memory_space=pltpu.VMEM)
    anywhere = pl.BlockSpec(memory_space=pl.ANY)
    edge = ((2048, 512), BF16)
    node = ((256, 512), BF16)
    nodes = ((512, 512), BF16)
    column = ((2048, 1), F32)
    node_wide = ((256, 512), F32)
    nodes_wide = ((512, 512), F32)
    mats = [((1536, 512), BF16), ((512, 512), BF16), ((1024, 512), BF16), ((512, 512), BF16), ((8, 512), F32)]
    scratch = [nodes, nodes, edge, edge, edge, edge, edge, edge, column, column, node, node, node, node, ((3, 256, 512), BF16), node, node_wide, ((2, 8, 512), F32), node_wide, nodes_wide, nodes_wide, node_wide, node_wide] + mats + mats
    copies = 2 * GATHER_COPIES + 4 * REDUCE_COPIES + 4
    return pl.pallas_call(
        step_kernel,
        out_shape=[jax.ShapeDtypeStruct(*node), jax.ShapeDtypeStruct(*edge), jax.ShapeDtypeStruct((2, 30, 8, 128), F32)],
        in_specs=[spec] * len(vmem_inputs) + [anywhere] * len(hbm_inputs),
        out_specs=[spec] * 3,
        scratch_shapes=[pltpu.VMEM(*entry) for entry in scratch] + [pltpu.SemaphoreType.DMA((3,)), pltpu.SemaphoreType.REGULAR((2,)), pltpu.SemaphoreType.REGULAR, pltpu.SemaphoreType.DMA((copies,)), pltpu.SemaphoreType.DMA((copies,))],
        compiler_params=pltpu.CompilerParams(collective_id=1, has_side_effects=True, vmem_limit_bytes=67043328),
        cost_estimate=pl.CostEstimate(flops=27 * 10 ** 9, bytes_accessed=20 * 2 ** 20, transcendentals=0),
        name='train_step',
    )(*vmem_inputs, *hbm_inputs)


def update_kernel(total, node_in, edge_in, *refs):
    refs[-2][...] = node_in[...]
    refs[-1][...] = edge_in[...]
    masters, ones, twos, new_masters, new_ones, new_twos = [refs[5 * n:5 * n + 5] for n in range(6)]

    def apply(slot, index, grad):
        master, one, two = adamw_update(masters[slot][index], grad, ones[slot][index], twos[slot][index])
        new_masters[slot][index] = master
        new_ones[slot][index] = one
        new_twos[slot][index] = two

    shift = lax.rem(16 - lax.rem(lax.axis_index('dp'), 16), 16) * 8
    for layer in range(2):
        edge_first = 15 if layer == 0 else 0
        for slot, (first, rows) in enumerate(((0, 3), (12, 1), (16, 2), (24, 1))):
            for r in range(rows):
                for k in range(4):
                    tile = first + 4 * r + k
                    if tile < 16:
                        grad = total[tile // 8, edge_first + tile % 8]
                    else:
                        grad = total[(tile - 16) // 6, 9 + 15 * layer + (tile - 16) % 6]
                    apply(slot, (layer, slice(8 * r, 8 * r + 8), slice(128 * k, 128 * k + 128)), grad)
        for part in range(2):
            turned = pltpu.roll(total[part, edge_first + 8], shift, 1)
            apply(4, (layer, slice(2 * part, 2 * part + 2), slice(0, 8)), turned[0:2, 0:8])


def update_call(total, grad_node, grad_edge, masters, ones, twos):
    spec = pl.BlockSpec(memory_space=pltpu.VMEM)
    shapes = [jax.ShapeDtypeStruct(array.shape, array.dtype) for array in masters + ones + twos + (grad_node, grad_edge)]
    return tuple(pl.pallas_call(update_kernel, out_shape=shapes, in_specs=[spec] * 18, out_specs=[spec] * 17, compiler_params=pltpu.CompilerParams(vmem_limit_bytes=67043328), name='update')(total, grad_node, grad_edge, *masters, *ones, *twos))


def adamw_update(master, grad_sum, moment_one, moment_two):
    corr_one = 1.0 - BETA_ONE ** STEP
    corr_two = 1.0 - BETA_TWO ** STEP
    one_new = BETA_ONE * moment_one + (1.0 - BETA_ONE) * grad_sum
    two_new = BETA_TWO * moment_two + (1.0 - BETA_TWO) * grad_sum * grad_sum
    direction = (one_new / corr_one) / (jnp.sqrt(two_new / corr_two) + ADAM_EPS)
    return master - LEARN_RATE * (direction + DECAY * master), one_new, two_new


def solution(mesh):
    lat_spec = P('dp', 'sp', None)
    edge_spec = P('sp')
    mat_spec = P(None, 'dp', None)
    norm_spec = P(None, None, 'dp')
    param_specs = (mat_spec, mat_spec, mat_spec, mat_spec, norm_spec)

    def train_step(node_lat, edge_lat, senders, edge_mask, node_cot, edge_cot, *params):
        masters, ones, twos = params[0:5], params[5:10], params[10:15]
        snd_rows = senders.reshape(-1, 128)
        mask_rows = edge_mask.reshape(-1, 128)
        grad_node, grad_edge, total = step_call(tuple(pack_call(masters)) + (node_lat[0], snd_rows, mask_rows, node_cot[0]), (edge_lat[0], edge_cot[0]))
        outs = update_call(total, grad_node, grad_edge, masters, ones, twos)
        return outs[:15] + (outs[15][None], outs[16][None])

    return jax.shard_map(train_step, mesh=mesh, in_specs=(lat_spec, lat_spec, edge_spec, edge_spec, lat_spec, lat_spec) + param_specs + param_specs + param_specs, out_specs=param_specs + param_specs + param_specs + (lat_spec, lat_spec), check_vma=False)
```

```python
import functools

import jax
import jax.numpy as jnp
from jax import lax
from jax.experimental import pallas as pl
from jax.experimental.pallas import tpu as pltpu
from jax.sharding import PartitionSpec as P

NORM_EPS = 1e-5
LEARN_RATE = 1e-3
BETA_ONE = 0.9
BETA_TWO = 0.95
ADAM_EPS = 1e-8
DECAY = 0.1
STEP = 10

MESH_ID = pl.DeviceIdType.MESH
ORDERS = ((0, 1, 2), (1, 2, 0), (2, 0, 1))
RING = 4
HOPS = (1, -1, 2)


class Place:
    def __init__(self):
        chip = lax.axis_index('dp')
        self.core = lax.axis_index('sp')
        self.at = (lax.rem(chip // 16, 4), lax.rem(chip // 4, 4), lax.rem(chip, 4))

    def step(self, dim, delta):
        return lax.rem(self.at[dim] + (delta + RING), RING)

    def chip(self, dim, delta):
        pos = list(self.at)
        pos[dim] = self.step(dim, delta)
        return {'dp': pos[0] * 16 + pos[1] * 4 + pos[2]}

    def partner(self):
        return {'sp': 1 - self.core}

    def peers(self):
        return [self.partner()] + [self.chip(dim, delta) for dim in range(3) for delta in HOPS]

    def barrier(self):
        sem = pltpu.get_barrier_semaphore()
        peers = self.peers()
        for peer in peers:
            pl.semaphore_signal(sem, inc=1, device_id=peer, device_id_type=MESH_ID)
        pl.semaphore_wait(sem, len(peers))


class Wire:
    def __init__(self, send_sem, recv_sem):
        self.sems = (send_sem, recv_sem)
        self.slots = {}
        self.parts = {}

    def describe(self, key):
        source, target, where = self.parts[key]
        slot = self.slots.setdefault(key, len(self.slots))
        return pltpu.make_async_remote_copy(src_ref=source(), dst_ref=target(), send_sem=self.sems[0].at[slot], recv_sem=self.sems[1].at[slot], device_id=where(), device_id_type=MESH_ID)

    def start(self, key, source, target, where):
        self.parts[key] = (source, target, where)
        self.describe(key).start()

    def wait_recv(self, key):
        self.describe(key).wait_recv()

    def finish(self):
        for key in list(self.parts):
            self.describe(key).wait_send()


class Credit:
    def __init__(self, place, sem):
        self.place, self.sem = place, sem

    def stage(self, number):
        pl.semaphore_signal(self.sem, inc=1, device_id=self.place.partner(), device_id_type=MESH_ID)


def split_groups(count):
    base, extra = divmod(count, 3)
    sizes = [base + (1 if g < extra else 0) for g in range(3)]
    starts = [sum(sizes[:g]) for g in range(3)]
    return list(zip(starts, sizes))


class Gather:
    def __init__(self, name, place, wire, src_ref, grid_ref):
        self.name, self.place, self.wire = name, place, wire
        self.src, self.grid = src_ref, grid_ref
        self.half = src_ref.shape[0] // 2
        self.first = place.core * self.half
        self.groups = split_groups(self.half)
        self.shared = []

    def region(self, g, phase, delta, side=None):
        order = ORDERS[g]
        start, size = self.groups[g]
        index = list(self.place.at)
        for q in range(phase):
            index[order[q]] = pl.ds(0, RING)
        index[order[phase]] = self.place.step(order[phase], delta)
        if side is not None:
            index[order[0]] = pl.ds(2 * side, 2)
        return self.grid.at[index[0], index[1], index[2], pl.ds(self.first + start, size)]

    def send(self, g, phase, delta, toward, tag, side=None):
        dim = ORDERS[g][phase]
        piece = functools.partial(self.region, g, phase, delta, side)
        origin = piece
        if phase == 0:
            start, size = self.groups[g]
            origin = lambda: self.src.at[pl.ds(self.first + start, size)]
        self.wire.start((self.name, g, phase, tag), origin, piece, lambda: self.place.chip(dim, toward))

    def share(self, g, phase, delta):
        key = (self.name, g, phase, 'share', delta)
        self.shared.append(key)
        piece = functools.partial(self.region, g, phase, delta)
        self.wire.start(key, piece, piece, self.place.partner)

    def begin(self, phase):
        for g in range(3):
            for toward in (HOPS if phase < 2 else (1, -1)):
                self.send(g, phase, 0, toward, toward)

    def arrived(self, g, phase, tag):
        self.wire.wait_recv((self.name, g, phase, tag))

    def stage(self, number):
        if number == 0:
            self.begin(0)
        elif number in (1, 2):
            for g in range(3):
                for toward in HOPS:
                    self.arrived(g, number - 1, toward)
            self.begin(number)
            for g in range(3):
                for toward in HOPS:
                    self.share(g, number - 1, -toward)
        elif number == 3:
            for g in range(3):
                self.arrived(g, 2, 1)
                self.send(g, 2, -1, 1, 'on_right', 0)
                self.arrived(g, 2, -1)
                self.send(g, 2, 1, -1, 'on_left', 1)
            for g in range(3):
                self.share(g, 2, -1)
                self.share(g, 2, 1)
        elif number == 4:
            for g in range(3):
                self.arrived(g, 2, 'on_right')
                self.arrived(g, 2, 'on_left')
                self.share(g, 2, 2)
        else:
            for key in self.shared:
                self.wire.wait_recv(key)


GATHER_COPIES = 3 * (3 + 3 + 4 + 3 + 3 + 3)


class Reduce:
    def __init__(self, name, place, wire, source, first, count, bufs, out_ref, out_first, own=None, load_sem=None):
        self.name, self.place, self.wire = name, place, wire
        self.source, self.first, self.count = source, first, count // 2
        self.theirs, self.boxes = bufs[0], bufs[1:10]
        self.out, self.out_first, self.load_sem = out_ref, out_first, load_sem
        self.own, self.base = (source, first + place.core * self.count) if own is None else (own, 0)
        self.groups = split_groups(self.count)
        self.turns = (2, 1, -1, 0)

    def index_of(self, g, phase, delta, side=None):
        order = ORDERS[g]
        index = [pl.ds(0, RING)] * 3
        for q in range(phase):
            index[order[q]] = self.place.at[order[q]]
        index[order[phase]] = self.place.step(order[phase], delta)
        if side is not None:
            index[order[phase + 1]] = pl.ds(2 * side, 2)
        return index

    def kept(self, g, phase, delta, side=None):
        index = self.index_of(g, phase, delta, side)
        start, size = self.groups[g]
        return self.own.at[index[0], index[1], index[2], pl.ds(self.base + start, size)]

    def piece(self, g, delta, core):
        index = self.index_of(g, 0, delta)
        start, size = self.groups[g]
        return self.source.at[index[0], index[1], index[2], pl.ds(self.first + core * self.count + start, size)]

    def slot(self, g, delta):
        index = self.index_of(g, 0, delta)
        return self.theirs.at[index[0], index[1], index[2], pl.ds(*self.groups[g])]

    def load(self, g, delta):
        return pltpu.make_async_copy(self.piece(g, delta, self.place.core), self.kept(g, 0, delta), self.load_sem.at[self.turns.index(delta) * 3 + g])

    def ready(self, g, delta):
        if self.load_sem is not None:
            self.load(g, delta).wait()
        self.wire.wait_recv((self.name, 'swap', g, delta))
        target = self.kept(g, 0, delta)
        target[...] = target[...] + self.slot(g, delta)[...]

    def box(self, g, phase, number):
        return self.boxes[g * 3 + phase].at[number]

    def send(self, g, phase, tag, delta, side, number, toward):
        dim = ORDERS[g][phase]
        self.wire.start((self.name, g, phase, tag), functools.partial(self.kept, g, phase, delta, side), functools.partial(self.box, g, phase, number), lambda: self.place.chip(dim, toward))

    def absorb(self, g, phase, tag, delta, side, number):
        self.wire.wait_recv((self.name, g, phase, tag))
        target = self.kept(g, phase, delta, side)
        target[...] = target[...] + self.box(g, phase, number)[...]

    def far(self, g, phase):
        self.send(g, phase, 'far_right', 2, 0, 0, 1)
        self.send(g, phase, 'far_left', 2, 1, 2, -1)

    def near(self, g, phase):
        self.send(g, phase, 'near_right', 1, 1, 1, 1)
        self.send(g, phase, 'near_left', -1, 0, 3, -1)

    def onward(self, g, phase):
        self.absorb(g, phase, 'far_right', 1, 0, 0)
        self.send(g, phase, 'sum_right', 1, 0, 4, 1)
        self.absorb(g, phase, 'far_left', -1, 1, 2)
        self.send(g, phase, 'sum_left', -1, 1, 5, -1)

    def direct(self, g, phase):
        for n, toward in enumerate(HOPS):
            self.send(g, phase, toward, toward, None, n, toward)

    def collect(self, g, phase):
        for n, toward in enumerate(HOPS):
            self.absorb(g, phase, toward, 0, None, n)

    def settle(self, g, phase):
        for tag, number, side in (('near_left', 3, 0), ('near_right', 1, 1), ('sum_right', 4, 0), ('sum_left', 5, 1)):
            self.absorb(g, phase, tag, 0, side, number)

    def stage(self, number):
        if number == 0:
            for delta in self.turns:
                for g in range(3):
                    if self.load_sem is not None:
                        self.load(g, delta).start()
                    self.wire.start((self.name, 'swap', g, delta), functools.partial(self.piece, g, delta, 1 - self.place.core), functools.partial(self.slot, g, delta), self.place.partner)
        elif number == 1:
            for g in range(3):
                self.ready(g, 2)
                self.far(g, 0)
            for g in range(3):
                self.ready(g, 1)
                self.ready(g, -1)
                self.near(g, 0)
        elif number == 2:
            for g in range(3):
                self.onward(g, 0)
            for g in range(3):
                self.ready(g, 0)
        elif number == 3:
            for g in range(3):
                self.settle(g, 0)
                self.direct(g, 1)
        elif number == 4:
            return
        elif number == 5:
            for g in range(3):
                self.collect(g, 1)
                self.direct(g, 2)
        elif number == 6:
            for g in range(3):
                self.collect(g, 2)
            span = lambda: self.out.at[self.place.core, pl.ds(self.out_first, self.count)]
            span()[...] = self.own[self.place.at[0], self.place.at[1], self.place.at[2], pl.ds(self.base, self.count)]
            self.wire.start((self.name, 'result'), span, span, self.place.partner)
        else:
            self.wire.wait_recv((self.name, 'result'))


def box_shapes(count):
    out = []
    for g, (_, size) in enumerate(split_groups(count)):
        order = ORDERS[g]
        dims = {dim: RING for dim in range(3) if dim != order[0]}
        dims[order[1]] = 2
        out.append((6,) + tuple(dims[dim] for dim in sorted(dims)) + (size, 8, 128))
        out.append((3, RING, size, 8, 128))
        out.append((3, size, 8, 128))
    return out


def reduce_scratch(count):
    grid = pltpu.VMEM((RING, RING, RING, count, 8, 128), jnp.float32)
    return [grid] + [pltpu.VMEM(shape, jnp.float32) for shape in box_shapes(count)]


REDUCE_COPIES = 12 + 3 * 12 + 1


TILE = 512
NODE_TILE = TILE // 8
BF16 = jnp.bfloat16
F32 = jnp.float32


def dot(left, right, left_dim=1, right_dim=0):
    return lax.dot_general(left, right, (((left_dim,), (right_dim,)), ((), ())), preferred_element_type=F32)


def split_three(values):
    high = values.astype(BF16)
    rest = values - high.astype(F32)
    mid = rest.astype(BF16)
    low = (rest - mid.astype(F32)).astype(BF16)
    return high, mid, low


def dot_wide(values, right, right_dim=0):
    high, mid, low = split_three(values)
    return dot(high, right, 1, right_dim) + dot(mid, right, 1, right_dim) + dot(low, right, 1, right_dim)


def dot_wide_rows(left, values):
    high, mid, low = split_three(values)
    return dot(left, high, 0, 0) + dot(left, mid, 0, 0) + dot(left, low, 0, 0)


def norm_stats(out_b):
    values = out_b.astype(F32)
    centered = values - jnp.mean(values, axis=-1, keepdims=True)
    inv_std = lax.rsqrt(jnp.mean(centered * centered, axis=-1, keepdims=True) + NORM_EPS)
    return centered * inv_std, inv_std


def mlp_forward(pre_act, w_two, gain, bias):
    pre_b = pre_act.astype(BF16)
    hidden = jax.nn.silu(pre_b.astype(F32)).astype(BF16)
    out_b = dot(hidden, w_two).astype(BF16)
    normed, _ = norm_stats(out_b)
    return normed * gain + bias, pre_b, out_b


def mlp_cotangents(d_branch, pre_b, out_b, w_two, gain):
    normed, inv_std = norm_stats(out_b)
    d_norm = d_branch * gain
    d_out = (inv_std * (d_norm - jnp.mean(d_norm, axis=-1, keepdims=True) - normed * jnp.mean(d_norm * normed, axis=-1, keepdims=True))).astype(BF16)
    d_act = dot(d_out, w_two, 1, 1).astype(BF16)
    pre_f = pre_b.astype(F32)
    gate = jax.nn.sigmoid(pre_f)
    hidden = (pre_f * gate).astype(BF16)
    d_pre = (d_act.astype(F32) * gate * (1.0 + pre_f * (1.0 - gate))).astype(BF16)
    d_gain = (d_branch * normed).reshape(-1, 8, d_branch.shape[-1]).sum(axis=0)
    d_bias = d_branch.reshape(-1, 8, d_branch.shape[-1]).sum(axis=0)
    return d_out, hidden, d_pre, d_gain, d_bias


def receiver_pick(copies):
    rows = lax.broadcasted_iota(jnp.int32, (TILE, copies * NODE_TILE), 0)
    cols = lax.broadcasted_iota(jnp.int32, (TILE, copies * NODE_TILE), 1)
    return lax.shift_right_logical(rows, 3) == lax.bitwise_and(cols, NODE_TILE - 1)


def as_bf16(flags):
    return jnp.where(flags, 1.0, 0.0).astype(BF16)


def unpack_weights(grid, w_e1, w_e2, w_n1, w_n2, norms):
    def row(p, carry):
        at = (p // 4, lax.rem(p, 4))
        for x in range(0, 4, 2):
            for k in range(4):
                lanes = pl.ds(128 * k, 128)
                for dev in range(2):
                    w_e1[pl.ds(pl.multiple_of(96 * p, 32) + (24 * x + 32 * dev), 16), lanes] = grid[at[0], at[1], x + dev, k]
                    w_n1[pl.ds(pl.multiple_of(64 * p, 64) + 16 * (x + dev), 16), lanes] = grid[at[0], at[1], x + dev, 4 + k]
                for ref, first, tile, top in ((w_e1, pl.multiple_of(96 * p, 32) + (24 * x + 16), 8, 0), (w_e2, pl.multiple_of(32 * p, 32) + 8 * x, 8, 8), (w_n2, pl.multiple_of(32 * p, 32) + 8 * x, 12, 0)):
                    even = grid[at[0], at[1], x, tile + k].astype(F32)[top:top + 8]
                    odd = grid[at[0], at[1], x + 1, tile + k].astype(F32)[top:top + 8]
                    ref[pl.ds(first, 16), lanes] = jnp.concatenate([even, odd], axis=0).astype(BF16)
        return carry
    lax.fori_loop(0, 16, row, 0)
    for k in range(4):
        total = grid[k, 0, 0, 12].astype(F32)
        for d in range(1, 16):
            total = total + grid[k, d // 4, d % 4, 12].astype(F32)
        norms[:, 128 * k:128 * k + 128] = total[8:16]


def fill_columns(snd_rows, mask_rows, snd_col, mask_col):
    for rows, col in ((snd_rows, snd_col), (mask_rows, mask_col)):
        turned = rows[...].astype(F32).T
        for n in range(rows.shape[0]):
            col[128 * n:128 * n + 128, :] = turned[:, n:n + 1]


def pick_senders(snd_col, node_all, rows):
    ids = lax.broadcasted_iota(jnp.int32, (TILE, 512), 1)
    return dot(as_bf16(snd_col[rows].astype(jnp.int32) == ids), node_all[...]).astype(BF16)


def all_senders(snd_col, node_all, out):
    def tile(i, carry):
        rows = pl.ds(pl.multiple_of(i * TILE, TILE), TILE)
        out[rows] = pick_senders(snd_col, node_all, rows)
        return carry
    lax.fori_loop(0, out.shape[0] // TILE, tile, 0)


def edge_forward(layer_io, senders, hook, edge_out, pre_out, out_out, sums_out, w_e1, w_e2, norms, recv_terms):
    node_all, node_own, edge_in, snd_col, mask_col = layer_io
    for part, term in enumerate(split_three(dot(node_own[...], w_e1[1024:1536]))):
        recv_terms[part] = term

    def tile(i, carry):
        rows = pl.ds(pl.multiple_of(i * TILE, TILE), TILE)
        nodes = pl.ds(pl.multiple_of(i * NODE_TILE, NODE_TILE), NODE_TILE)
        sender = pick_senders(snd_col, node_all, rows) if senders is None else senders[rows]
        recv = jnp.concatenate([recv_terms[0, nodes], recv_terms[1, nodes], recv_terms[2, nodes]], axis=0)
        edge = edge_in[rows]
        pre = dot(edge, w_e1[0:512]) + dot(sender, w_e1[512:1024]) + dot(as_bf16(receiver_pick(3)), recv)
        branch, pre_b, out_b = mlp_forward(pre, w_e2[...], norms[0:1], norms[1:2])
        edge_new = (edge.astype(F32) + branch).astype(BF16)
        pre_out[rows] = pre_b
        out_out[rows] = out_b
        if edge_out is not None:
            edge_out[rows] = edge_new
        picked = jnp.where(receiver_pick(1), mask_col[rows], 0.0).astype(BF16)
        sums_out[nodes] = dot(picked, edge_new, 0, 0).astype(BF16)
        hook(i)
        return carry
    lax.fori_loop(0, edge_in.shape[0] // TILE, tile, 0)


def node_forward(node_own, sums, w_n1, w_n2, norms):
    pre = dot(node_own[...], w_n1[0:512]) + dot(sums[...], w_n1[512:1024])
    return mlp_forward(pre, w_n2[...], norms[2:3], norms[3:4])


def lane_tiles(values):
    return [values[:, 128 * k:128 * k + 128].reshape(-1, 8, 128) for k in range(4)]


def tile_at(tile):
    return tile + tile // 8 if tile < 16 else tile + 2


def store_square(grad_ref, values, first_tile):
    for k, tiles in enumerate(lane_tiles(values)):
        grad_ref[:, :, :, tile_at(first_tile + k)] = tiles.reshape(4, 4, 4, 8, 128)


def store_double(grad_ref, values, first_tile, part):
    for k, tiles in enumerate(lane_tiles(values)):
        tiles = tiles.reshape(2, 4, 4, 2, 8, 128)
        for r in range(2):
            grad_ref[2 * part:2 * part + 2, :, :, tile_at(first_tile + 4 * r + k)] = tiles[:, :, :, r]


def store_triple(grad_ref, values, first_pair):
    for n in range(values.shape[0] // 96):
        pair = first_pair + n
        for k, tiles in enumerate(lane_tiles(values[96 * n:96 * n + 96])):
            tiles = tiles.reshape(4, 3, 8, 128)
            for r in range(3):
                grad_ref[pair // 4, pair % 4, :, tile_at(4 * r + k)] = tiles[:, r]


def layer_back(layer_io, d_node_new, d_edge_new, pre_e, out_e, sums, pre_n, out_n, mats, norms, snd_rows, outs, scratch, after_nodes, hook, pass_on):
    node_all, node_own, edge_in, snd_col, mask_col = layer_io
    w_e1, w_e2, w_n1, w_n2 = mats
    grad_ref, d_edge, d_local, scattered = outs
    hidden_s, d_pre_s, d_out_s, d_sum_s, recv_s, gain_s = scratch
    d_out_n, hidden_n, d_pre_n, d_gain_n, d_bias_n = mlp_cotangents(d_node_new, pre_n, out_n, w_n2[...], norms[2:3])
    d_sum_s[...] = dot(d_pre_n, w_n1[512:1024], 1, 1).astype(BF16)
    d_local[...] = d_node_new + dot(d_pre_n, w_n1[0:512], 1, 1)
    store_square(grad_ref, dot(hidden_n, d_out_n, 0, 0), 24)
    store_double(grad_ref, dot(node_own[...], d_pre_n, 0, 0), 16, 0)
    store_double(grad_ref, dot(sums[...], d_pre_n, 0, 0), 16, 1)
    after_nodes()
    gain_s[...] = jnp.zeros_like(gain_s)

    def tile(i, carry):
        rows = pl.ds(pl.multiple_of(i * TILE, TILE), TILE)
        nodes = pl.ds(pl.multiple_of(i * NODE_TILE, NODE_TILE), NODE_TILE)
        pick = receiver_pick(1)
        picked = jnp.where(pick, mask_col[rows], 0.0).astype(BF16)
        d_res = (d_edge_new[rows].astype(F32) + dot(picked, d_sum_s[nodes])).astype(BF16).astype(F32)
        d_out, hidden, d_pre, d_gain, d_bias = mlp_cotangents(d_res, pre_e[rows], out_e[rows], w_e2[...], norms[0:1])
        gain_s[0] = gain_s[0] + d_gain
        gain_s[1] = gain_s[1] + d_bias
        hidden_s[rows] = hidden
        d_out_s[rows] = d_out
        d_pre_s[rows] = d_pre
        d_edge[rows] = d_res.astype(BF16)
        recv_s[nodes] = dot(as_bf16(pick), d_pre, 0, 0)
        hook(i)
        return carry
    lax.fori_loop(0, edge_in.shape[0] // TILE, tile, 0)
    store_square(grad_ref, dot(hidden_s[...], d_out_s[...], 0, 0), 12)
    upper = dot(edge_in[...], d_pre_s[...], 0, 0)
    store_triple(grad_ref, upper[0:480], 0)
    snd_row = jnp.concatenate([snd_rows[n:n + 1] for n in range(snd_rows.shape[0])], axis=1)
    for block in range(4):
        ids = lax.broadcasted_iota(jnp.int32, (128, edge_in.shape[0]), 0) + 128 * block
        scattered[128 * block:128 * block + 128] = dot(as_bf16(snd_row == ids), d_pre_s[...])
    pass_on()
    middle = dot_wide_rows(node_all[...], scattered[...])
    store_triple(grad_ref, jnp.concatenate([upper[480:512], middle[0:448]], axis=0), 5)
    lower = dot_wide_rows(node_own[...], recv_s[...])
    store_triple(grad_ref, jnp.concatenate([middle[448:512], lower], axis=0), 10)
    for part, (gain, bias) in enumerate(((gain_s[0], gain_s[1]), (d_gain_n, d_bias_n))):
        full = jnp.concatenate([gain.sum(axis=0, keepdims=True), bias.sum(axis=0, keepdims=True), jnp.zeros((6, 512), F32)], axis=0)
        for k in range(4):
            grad_ref[k, :, :, 8 + 9 * part] = jnp.broadcast_to(full[:, 128 * k:128 * k + 128], (4, 4, 8, 128))


def layer_back_late(w_e1, d_edge, d_local, scratch):
    d_pre_s, recv_s = scratch[1], scratch[4]

    def tile(i, carry):
        rows = pl.ds(pl.multiple_of(i * TILE, TILE), TILE)
        d_edge[rows] = (d_edge[rows].astype(F32) + dot(d_pre_s[rows], w_e1[0:512], 1, 1)).astype(BF16)
        return carry
    lax.fori_loop(0, d_edge.shape[0] // TILE, tile, 0)
    d_local[...] = d_local[...] + dot_wide(recv_s[...], w_e1[1024:1536], 1)


def half_of(ref, core):
    count = ref.shape[0] // 2
    return ref.at[pl.ds(pl.multiple_of(core * count, count), count)]


def no_hook(i):
    return None


def at_tile(plan):
    def hook(i):
        for tile, stages in plan.items():
            @pl.when(i == tile)
            def _():
                for plan_of, number in stages:
                    plan_of.stage(number)
    return hook


def pack_shard(layer, masters, shard, norm_pad):
    edge_one, edge_two, node_one, node_two, norm_rows = masters
    chip = lax.axis_index('dp')
    odd = lax.rem(chip, 2) == 1
    norm_pad[...] = jnp.zeros_like(norm_pad)
    norm_pad[0:4, 0:8] = norm_rows[layer]
    placed = pltpu.roll(norm_pad[...], lax.rem(chip, 16) * 8, 1)
    for k in range(4):
        lanes = slice(128 * k, 128 * k + 128)
        first, mid, last = edge_one[layer, 0:8, lanes], edge_one[layer, 8:16, lanes], edge_one[layer, 16:24, lanes]
        shard[k] = jnp.concatenate([jnp.where(odd, mid, first), jnp.where(odd, last, mid)], axis=0).astype(BF16)
        shard[4 + k] = node_one[layer, :, lanes].astype(BF16)
        shard[8 + k] = jnp.concatenate([jnp.where(odd, first, last), edge_two[layer, :, lanes]], axis=0).astype(BF16)
        shard[12 + k] = jnp.concatenate([node_two[layer, :, lanes], placed if k == 0 else jnp.zeros_like(placed)], axis=0).astype(BF16)


def node_cotangent(d_local, scattered, returned, w_above, core):
    return (d_local[...] + dot_wide(half_of(scattered, core)[...] + returned[...], w_above[512:1024], 1)).astype(BF16)


def pack_kernel(edge_one, edge_two, node_one, node_two, norm_rows, shard_low, shard_high, norm_pad):
    for layer, shard in enumerate((shard_low, shard_high)):
        pack_shard(layer, (edge_one, edge_two, node_one, node_two, norm_rows), shard, norm_pad)


def pack_call(masters):
    spec = pl.BlockSpec(memory_space=pltpu.VMEM)
    shard = jax.ShapeDtypeStruct((16, 16, 128), BF16)
    return pl.pallas_call(pack_kernel, out_shape=[shard, shard], in_specs=[spec] * 5, out_specs=[spec] * 2, scratch_shapes=[pltpu.VMEM((8, 128), F32)], compiler_params=pltpu.CompilerParams(vmem_limit_bytes=67043328), name='pack')(*masters)


def step_kernel(shard_low, shard_high, node_in, snd_rows, mask_rows, node_cot, edge_lat, edge_cot, grad_node, d_edge, total, node_all, node_all_one, edge_in, pre_low, out_low, pre_high, out_high, d_pre, snd_col, mask_col, sums_low, sums_high, pre_node, out_node, recv_terms, d_sum, recv_sum, gain_sum, d_local, scattered_high, scattered_low, returned_high, returned_low, *rest):
    mats_low, norms_low, mats_high, norms_high = rest[0:4], rest[4], rest[5:9], rest[9]
    load_sem, credit_sem, peer_sem, send_sem, recv_sem = rest[10:]
    wire = Wire(send_sem, recv_sem)
    load_edge = lambda n: pltpu.make_async_copy(edge_lat, edge_in, load_sem.at[n])
    load_cot = lambda: pltpu.make_async_copy(edge_cot, d_edge, load_sem.at[1])
    load_edge(0).start()
    load_cot().start()

    def begin():
        place = Place()
        node_own = half_of(node_all, place.core)
        node_own_one = half_of(node_all_one, place.core)
        return place, (node_all, node_own, edge_in, snd_col, mask_col), (node_all_one, node_own_one, edge_in, snd_col, mask_col)

    def gather_and_first(grid_low, grid_high):
        place, low_io, high_io = begin()
        node_own, node_own_one = low_io[1], high_io[1]
        for shard, grid in ((shard_low, grid_low), (shard_high, grid_high)):
            grid[place.at[0], place.at[1], place.at[2]] = shard[...]
        node_own[...] = node_in[...]
        place.barrier()
        low = Gather('low', place, wire, shard_low, grid_low)
        high = Gather('high', place, wire, shard_high, grid_high)
        low.stage(0)
        high.stage(0)
        wire.start('node', lambda: node_in, lambda: half_of(node_all, place.core), place.partner)
        fill_columns(snd_rows, mask_rows, snd_col, mask_col)
        low.stage(1)
        high.stage(1)
        low.stage(2)
        wire.wait_recv('node')
        all_senders(snd_col, node_all, d_pre)
        low.stage(3)
        high.stage(2)
        low.stage(4)
        low.stage(5)
        unpack_weights(grid_low, *mats_low, norms_low)
        load_edge(0).wait()
        hook = at_tile({0: [(high, 3)], 2: [(high, 4)]})
        edge_forward(low_io, d_pre, hook, edge_in, pre_low, out_low, sums_low, mats_low[0], mats_low[1], norms_low, recv_terms)
        branch, pre_b, out_b = node_forward(node_own, sums_low, mats_low[2], mats_low[3], norms_low)
        pre_node[...] = pre_b
        out_node[...] = out_b
        node_own_one[...] = (node_own[...].astype(F32) + branch).astype(BF16)
        piece = lambda: half_of(node_all_one, place.core)
        wire.start('node_one', piece, piece, place.partner)
        high.stage(5)
        unpack_weights(grid_high, *mats_high, norms_high)
        wire.wait_recv('node_one')
        wire.finish()
        wire.parts.clear()

    def second_and_back(grad_high, grad_low, theirs_edge, theirs_node, *boxes):
        place, low_io, high_io = begin()
        node_own_one = high_io[1]
        peers = place.peers()
        for peer in peers:
            pl.semaphore_signal(peer_sem, inc=1, device_id=peer, device_id_type=MESH_ID)
        high_node = Reduce('high_node', place, wire, grad_high, 18, 12, (theirs_node,) + boxes[0:9], total, 24)
        high_edge = Reduce('high_edge', place, wire, grad_high, 0, 18, (theirs_edge,) + boxes[9:18], total, 0)
        low_node = Reduce('low_node', place, wire, grad_low, 18, 12, (theirs_node,) + boxes[18:27], total, 9)
        low_edge = Reduce('low_edge', place, wire, grad_low, 0, 18, (theirs_edge,) + boxes[27:36], total, 15)
        edge_forward(high_io, None, no_hook, None, pre_high, out_high, sums_high, mats_high[0], mats_high[1], norms_high, recv_terms)
        _, pre_n, out_n = node_forward(node_own_one, sums_high, mats_high[2], mats_high[3], norms_high)
        load_cot().wait()

        def pass_on_high():
            wire.start('scattered_high', lambda: half_of(scattered_high, 1 - place.core), lambda: returned_high, place.partner)

        def after_nodes_high():
            pl.semaphore_wait(peer_sem, len(peers))
            high_node.stage(0)
        hook = at_tile({1: [(high_node, 1)], 2: [(high_node, 2), (Credit(place, credit_sem.at[0]), 0)], 3: [(high_node, 3)]})
        scratch = (pre_high, d_pre, out_high, d_sum, recv_sum, gain_sum)
        layer_back(high_io, node_cot[...].astype(F32), d_edge, pre_high, out_high, sums_high, pre_n, out_n, mats_high, norms_high, snd_rows, (grad_high, d_edge, d_local, scattered_high), scratch, after_nodes_high, hook, pass_on_high)
        load_edge(2).start()
        high_edge.stage(0)
        high_node.stage(4)
        layer_back_late(mats_high[0], d_edge, d_local, scratch)
        high_node.stage(5)
        wire.wait_recv('scattered_high')
        d_node = node_cotangent(d_local, scattered_high, returned_high, mats_high[0], place.core).astype(F32)
        load_edge(2).wait()

        def pass_on_low():
            wire.start('scattered_low', lambda: half_of(scattered_low, 1 - place.core), lambda: returned_low, place.partner)

        def after_nodes_low():
            high_edge.stage(1)
            pl.semaphore_wait(credit_sem.at[0], 1)
            low_node.stage(0)
        hook = at_tile({0: [(high_node, 6)], 1: [(low_node, 1)], 2: [(high_edge, 2), (Credit(place, credit_sem.at[1]), 0)]})
        scratch = (pre_low, d_pre, out_low, d_sum, recv_sum, gain_sum)
        layer_back(low_io, d_node, d_edge, pre_low, out_low, sums_low, pre_node[...], out_node[...], mats_low, norms_low, snd_rows, (grad_low, d_edge, d_local, scattered_low), scratch, after_nodes_low, hook, pass_on_low)
        pl.semaphore_wait(credit_sem.at[1], 1)
        low_edge.stage(0)
        high_edge.stage(3)
        low_node.stage(2)
        low_edge.stage(1)
        layer_back_late(mats_low[0], d_edge, d_local, scratch)
        high_edge.stage(4)
        low_node.stage(3)
        wire.wait_recv('scattered_low')
        grad_node[...] = node_cotangent(d_local, scattered_low, returned_low, mats_low[0], place.core)
        low_edge.stage(2)
        high_edge.stage(5)
        low_node.stage(4)
        low_edge.stage(3)
        low_node.stage(5)
        high_edge.stage(6)
        low_edge.stage(4)
        low_node.stage(6)
        low_edge.stage(5)
        low_edge.stage(6)
        for plan in (high_node, high_edge, low_node, low_edge):
            plan.stage(7)
        wire.finish()

    grid = pltpu.VMEM((RING, RING, RING, 16, 16, 128), BF16)
    pl.run_scoped(gather_and_first, grid, grid)
    grad = pltpu.VMEM((RING, RING, RING, 30, 8, 128), F32)
    theirs = [pltpu.VMEM((RING, RING, RING, count, 8, 128), F32) for count in (9, 6)]
    boxes = [pltpu.VMEM(shape, F32) for count in (6, 9, 6, 9) for shape in box_shapes(count)]
    pl.run_scoped(second_and_back, grad, grad, *theirs, *boxes)


def step_call(vmem_inputs, hbm_inputs):
    spec = pl.BlockSpec(memory_space=pltpu.VMEM)
    anywhere = pl.BlockSpec(memory_space=pl.ANY)
    edge = ((2048, 512), BF16)
    node = ((256, 512), BF16)
    nodes = ((512, 512), BF16)
    column = ((2048, 1), F32)
    node_wide = ((256, 512), F32)
    nodes_wide = ((512, 512), F32)
    mats = [((1536, 512), BF16), ((512, 512), BF16), ((1024, 512), BF16), ((512, 512), BF16), ((8, 512), F32)]
    scratch = [nodes, nodes, edge, edge, edge, edge, edge, edge, column, column, node, node, node, node, ((3, 256, 512), BF16), node, node_wide, ((2, 8, 512), F32), node_wide, nodes_wide, nodes_wide, node_wide, node_wide] + mats + mats
    copies = 2 * GATHER_COPIES + 4 * REDUCE_COPIES + 4
    return pl.pallas_call(
        step_kernel,
        out_shape=[jax.ShapeDtypeStruct(*node), jax.ShapeDtypeStruct(*edge), jax.ShapeDtypeStruct((2, 30, 8, 128), F32)],
        in_specs=[spec] * len(vmem_inputs) + [anywhere] * len(hbm_inputs),
        out_specs=[spec] * 3,
        scratch_shapes=[pltpu.VMEM(*entry) for entry in scratch] + [pltpu.SemaphoreType.DMA((3,)), pltpu.SemaphoreType.REGULAR((2,)), pltpu.SemaphoreType.REGULAR, pltpu.SemaphoreType.DMA((copies,)), pltpu.SemaphoreType.DMA((copies,))],
        compiler_params=pltpu.CompilerParams(collective_id=1, has_side_effects=True, vmem_limit_bytes=67043328),
        cost_estimate=pl.CostEstimate(flops=27 * 10 ** 9, bytes_accessed=20 * 2 ** 20, transcendentals=0),
        name='train_step',
    )(*vmem_inputs, *hbm_inputs)


def update_kernel(total, node_in, edge_in, *refs):
    refs[-2][...] = node_in[...]
    refs[-1][...] = edge_in[...]
    masters, ones, twos, new_masters, new_ones, new_twos = [refs[5 * n:5 * n + 5] for n in range(6)]

    def apply(slot, index, grad):
        master, one, two = adamw_update(masters[slot][index], grad, ones[slot][index], twos[slot][index])
        new_masters[slot][index] = master
        new_ones[slot][index] = one
        new_twos[slot][index] = two

    shift = lax.rem(16 - lax.rem(lax.axis_index('dp'), 16), 16) * 8
    for layer in range(2):
        edge_first = 15 if layer == 0 else 0
        for slot, (first, rows) in enumerate(((0, 3), (12, 1), (16, 2), (24, 1))):
            for r in range(rows):
                for k in range(4):
                    tile = first + 4 * r + k
                    if tile < 16:
                        grad = total[tile // 8, edge_first + tile % 8]
                    else:
                        grad = total[(tile - 16) // 6, 9 + 15 * layer + (tile - 16) % 6]
                    apply(slot, (layer, slice(8 * r, 8 * r + 8), slice(128 * k, 128 * k + 128)), grad)
        for part in range(2):
            turned = pltpu.roll(total[part, edge_first + 8], shift, 1)
            apply(4, (layer, slice(2 * part, 2 * part + 2), slice(0, 8)), turned[0:2, 0:8])


def update_call(total, grad_node, grad_edge, masters, ones, twos):
    spec = pl.BlockSpec(memory_space=pltpu.VMEM)
    shapes = [jax.ShapeDtypeStruct(array.shape, array.dtype) for array in masters + ones + twos + (grad_node, grad_edge)]
    return tuple(pl.pallas_call(update_kernel, out_shape=shapes, in_specs=[spec] * 18, out_specs=[spec] * 17, compiler_params=pltpu.CompilerParams(vmem_limit_bytes=67043328), name='update')(total, grad_node, grad_edge, *masters, *ones, *twos))


def adamw_update(master, grad_sum, moment_one, moment_two):
    corr_one = 1.0 - BETA_ONE ** STEP
    corr_two = 1.0 - BETA_TWO ** STEP
    one_new = BETA_ONE * moment_one + (1.0 - BETA_ONE) * grad_sum
    two_new = BETA_TWO * moment_two + (1.0 - BETA_TWO) * grad_sum * grad_sum
    direction = (one_new / corr_one) / (jnp.sqrt(two_new / corr_two) + ADAM_EPS)
    return master - LEARN_RATE * (direction + DECAY * master), one_new, two_new


def solution(mesh):
    lat_spec = P('dp', 'sp', None)
    edge_spec = P('sp')
    mat_spec = P(None, 'dp', None)
    norm_spec = P(None, None, 'dp')
    param_specs = (mat_spec, mat_spec, mat_spec, mat_spec, norm_spec)

    def train_step(node_lat, edge_lat, senders, edge_mask, node_cot, edge_cot, *params):
        masters, ones, twos = params[0:5], params[5:10], params[10:15]
        snd_rows = senders.reshape(-1, 128)
        mask_rows = edge_mask.reshape(-1, 128)
        grad_node, grad_edge, total = step_call(tuple(pack_call(masters)) + (node_lat[0], snd_rows, mask_rows, node_cot[0]), (edge_lat[0], edge_cot[0]))
        outs = update_call(total, grad_node, grad_edge, masters, ones, twos)
        return outs[:15] + (outs[15][None], outs[16][None])

    return jax.shard_map(train_step, mesh=mesh, in_specs=(lat_spec, lat_spec, edge_spec, edge_spec, lat_spec, lat_spec) + param_specs + param_specs + param_specs, out_specs=param_specs + param_specs + param_specs + (lat_spec, lat_spec), check_vma=False)
```

```python
import functools

import jax
import jax.numpy as jnp
from jax import lax
from jax.experimental import pallas as pl
from jax.experimental.pallas import tpu as pltpu
from jax.sharding import PartitionSpec as P

NORM_EPS = 1e-5
LEARN_RATE = 1e-3
BETA_ONE = 0.9
BETA_TWO = 0.95
ADAM_EPS = 1e-8
DECAY = 0.1
STEP = 10

MESH_ID = pl.DeviceIdType.MESH
ORDERS = ((0, 1, 2), (1, 2, 0), (2, 0, 1))
RING = 4
HOPS = (1, -1, 2)


class Place:
    def __init__(self):
        chip = lax.axis_index('dp')
        self.core = lax.axis_index('sp')
        self.at = (lax.rem(chip // 16, 4), lax.rem(chip // 4, 4), lax.rem(chip, 4))

    def step(self, dim, delta):
        return lax.rem(self.at[dim] + (delta + RING), RING)

    def chip(self, dim, delta):
        pos = list(self.at)
        pos[dim] = self.step(dim, delta)
        return {'dp': pos[0] * 16 + pos[1] * 4 + pos[2]}

    def partner(self):
        return {'sp': 1 - self.core}

    def peers(self):
        return [self.partner()] + [self.chip(dim, delta) for dim in range(3) for delta in HOPS]

    def barrier(self):
        sem = pltpu.get_barrier_semaphore()
        peers = self.peers()
        for peer in peers:
            pl.semaphore_signal(sem, inc=1, device_id=peer, device_id_type=MESH_ID)
        pl.semaphore_wait(sem, len(peers))


class Wire:
    def __init__(self, send_sem, recv_sem):
        self.sems = (send_sem, recv_sem)
        self.slots = {}
        self.parts = {}

    def describe(self, key):
        source, target, where = self.parts[key]
        slot = self.slots.setdefault(key, len(self.slots))
        return pltpu.make_async_remote_copy(src_ref=source(), dst_ref=target(), send_sem=self.sems[0].at[slot], recv_sem=self.sems[1].at[slot], device_id=where(), device_id_type=MESH_ID)

    def start(self, key, source, target, where):
        self.parts[key] = (source, target, where)
        self.describe(key).start()

    def wait_recv(self, key):
        self.describe(key).wait_recv()

    def finish(self):
        for key in list(self.parts):
            self.describe(key).wait_send()


class Credit:
    def __init__(self, place, sem):
        self.place, self.sem = place, sem

    def stage(self, number):
        pl.semaphore_signal(self.sem, inc=1, device_id=self.place.partner(), device_id_type=MESH_ID)


def split_groups(count):
    base, extra = divmod(count, 3)
    sizes = [base + (1 if g < extra else 0) for g in range(3)]
    starts = [sum(sizes[:g]) for g in range(3)]
    return list(zip(starts, sizes))


class Gather:
    def __init__(self, name, place, wire, src_ref, grid_ref):
        self.name, self.place, self.wire = name, place, wire
        self.src, self.grid = src_ref, grid_ref
        self.half = src_ref.shape[0] // 2
        self.first = place.core * self.half
        self.groups = split_groups(self.half)
        self.shared = []

    def region(self, g, phase, delta, side=None):
        order = ORDERS[g]
        start, size = self.groups[g]
        index = list(self.place.at)
        for q in range(phase):
            index[order[q]] = pl.ds(0, RING)
        index[order[phase]] = self.place.step(order[phase], delta)
        if side is not None:
            index[order[0]] = pl.ds(2 * side, 2)
        return self.grid.at[index[0], index[1], index[2], pl.ds(self.first + start, size)]

    def send(self, g, phase, delta, toward, tag, side=None):
        dim = ORDERS[g][phase]
        piece = functools.partial(self.region, g, phase, delta, side)
        origin = piece
        if phase == 0:
            start, size = self.groups[g]
            origin = lambda: self.src.at[pl.ds(self.first + start, size)]
        self.wire.start((self.name, g, phase, tag), origin, piece, lambda: self.place.chip(dim, toward))

    def share(self, g, phase, delta):
        key = (self.name, g, phase, 'share', delta)
        self.shared.append(key)
        piece = functools.partial(self.region, g, phase, delta)
        self.wire.start(key, piece, piece, self.place.partner)

    def begin(self, phase):
        for g in range(3):
            for toward in (HOPS if phase < 2 else (1, -1)):
                self.send(g, phase, 0, toward, toward)

    def arrived(self, g, phase, tag):
        self.wire.wait_recv((self.name, g, phase, tag))

    def stage(self, number):
        if number == 0:
            self.begin(0)
        elif number in (1, 2):
            for g in range(3):
                for toward in HOPS:
                    self.arrived(g, number - 1, toward)
            self.begin(number)
            for g in range(3):
                for toward in HOPS:
                    self.share(g, number - 1, -toward)
        elif number == 3:
            for g in range(3):
                self.arrived(g, 2, 1)
                self.send(g, 2, -1, 1, 'on_right', 0)
                self.arrived(g, 2, -1)
                self.send(g, 2, 1, -1, 'on_left', 1)
            for g in range(3):
                self.share(g, 2, -1)
                self.share(g, 2, 1)
        elif number == 4:
            for g in range(3):
                self.arrived(g, 2, 'on_right')
                self.arrived(g, 2, 'on_left')
                self.share(g, 2, 2)
        else:
            for key in self.shared:
                self.wire.wait_recv(key)


GATHER_COPIES = 3 * (3 + 3 + 4 + 3 + 3 + 3)


class Reduce:
    def __init__(self, name, place, wire, source, first, count, bufs, out_ref, out_first, own=None, load_sem=None):
        self.name, self.place, self.wire = name, place, wire
        self.source, self.first, self.count = source, first, count // 2
        self.theirs, self.boxes = bufs[0], bufs[1:10]
        self.out, self.out_first, self.load_sem = out_ref, out_first, load_sem
        self.own, self.base = (source, first + place.core * self.count) if own is None else (own, 0)
        self.groups = split_groups(self.count)
        self.turns = (2, 1, -1, 0)

    def index_of(self, g, phase, delta, side=None):
        order = ORDERS[g]
        index = [pl.ds(0, RING)] * 3
        for q in range(phase):
            index[order[q]] = self.place.at[order[q]]
        index[order[phase]] = self.place.step(order[phase], delta)
        if side is not None:
            index[order[phase + 1]] = pl.ds(2 * side, 2)
        return index

    def kept(self, g, phase, delta, side=None):
        index = self.index_of(g, phase, delta, side)
        start, size = self.groups[g]
        return self.own.at[index[0], index[1], index[2], pl.ds(self.base + start, size)]

    def piece(self, g, delta, core):
        index = self.index_of(g, 0, delta)
        start, size = self.groups[g]
        return self.source.at[index[0], index[1], index[2], pl.ds(self.first + core * self.count + start, size)]

    def slot(self, g, delta):
        index = self.index_of(g, 0, delta)
        return self.theirs.at[index[0], index[1], index[2], pl.ds(*self.groups[g])]

    def load(self, g, delta):
        return pltpu.make_async_copy(self.piece(g, delta, self.place.core), self.kept(g, 0, delta), self.load_sem.at[self.turns.index(delta) * 3 + g])

    def ready(self, g, delta):
        if self.load_sem is not None:
            self.load(g, delta).wait()
        self.wire.wait_recv((self.name, 'swap', g, delta))
        target = self.kept(g, 0, delta)
        target[...] = target[...] + self.slot(g, delta)[...]

    def box(self, g, phase, number):
        return self.boxes[g * 3 + phase].at[number]

    def send(self, g, phase, tag, delta, side, number, toward):
        dim = ORDERS[g][phase]
        self.wire.start((self.name, g, phase, tag), functools.partial(self.kept, g, phase, delta, side), functools.partial(self.box, g, phase, number), lambda: self.place.chip(dim, toward))

    def absorb(self, g, phase, tag, delta, side, number):
        self.wire.wait_recv((self.name, g, phase, tag))
        target = self.kept(g, phase, delta, side)
        target[...] = target[...] + self.box(g, phase, number)[...]

    def far(self, g, phase):
        self.send(g, phase, 'far_right', 2, 0, 0, 1)
        self.send(g, phase, 'far_left', 2, 1, 2, -1)

    def near(self, g, phase):
        self.send(g, phase, 'near_right', 1, 1, 1, 1)
        self.send(g, phase, 'near_left', -1, 0, 3, -1)

    def onward(self, g, phase):
        self.absorb(g, phase, 'far_right', 1, 0, 0)
        self.send(g, phase, 'sum_right', 1, 0, 4, 1)
        self.absorb(g, phase, 'far_left', -1, 1, 2)
        self.send(g, phase, 'sum_left', -1, 1, 5, -1)

    def direct(self, g, phase):
        for n, toward in enumerate(HOPS):
            self.send(g, phase, toward, toward, None, n, toward)

    def collect(self, g, phase):
        for n, toward in enumerate(HOPS):
            self.absorb(g, phase, toward, 0, None, n)

    def settle(self, g, phase):
        for tag, number, side in (('near_left', 3, 0), ('near_right', 1, 1), ('sum_right', 4, 0), ('sum_left', 5, 1)):
            self.absorb(g, phase, tag, 0, side, number)

    def stage(self, number):
        if number == 0:
            for delta in self.turns:
                for g in range(3):
                    if self.load_sem is not None:
                        self.load(g, delta).start()
                    self.wire.start((self.name, 'swap', g, delta), functools.partial(self.piece, g, delta, 1 - self.place.core), functools.partial(self.slot, g, delta), self.place.partner)
        elif number == 1:
            for g in range(3):
                self.ready(g, 2)
                self.far(g, 0)
            for g in range(3):
                self.ready(g, 1)
                self.ready(g, -1)
                self.near(g, 0)
        elif number == 2:
            for g in range(3):
                self.onward(g, 0)
            for g in range(3):
                self.ready(g, 0)
        elif number == 3:
            for g in range(3):
                self.settle(g, 0)
                self.direct(g, 1)
        elif number == 4:
            return
        elif number == 5:
            for g in range(3):
                self.collect(g, 1)
                self.direct(g, 2)
        elif number == 6:
            for g in range(3):
                self.collect(g, 2)
            span = lambda: self.out.at[self.place.core, pl.ds(self.out_first, self.count)]
            span()[...] = self.own[self.place.at[0], self.place.at[1], self.place.at[2], pl.ds(self.base, self.count)]
            self.wire.start((self.name, 'result'), span, span, self.place.partner)
        else:
            self.wire.wait_recv((self.name, 'result'))


def box_shapes(count):
    out = []
    for g, (_, size) in enumerate(split_groups(count)):
        order = ORDERS[g]
        dims = {dim: RING for dim in range(3) if dim != order[0]}
        dims[order[1]] = 2
        out.append((6,) + tuple(dims[dim] for dim in sorted(dims)) + (size, 8, 128))
        out.append((3, RING, size, 8, 128))
        out.append((3, size, 8, 128))
    return out


def reduce_scratch(count):
    grid = pltpu.VMEM((RING, RING, RING, count, 8, 128), jnp.float32)
    return [grid] + [pltpu.VMEM(shape, jnp.float32) for shape in box_shapes(count)]


REDUCE_COPIES = 12 + 3 * 12 + 1


TILE = 512
NODE_TILE = TILE // 8
BF16 = jnp.bfloat16
F32 = jnp.float32


def dot(left, right, left_dim=1, right_dim=0):
    return lax.dot_general(left, right, (((left_dim,), (right_dim,)), ((), ())), preferred_element_type=F32)


def split_three(values):
    high = values.astype(BF16)
    rest = values - high.astype(F32)
    mid = rest.astype(BF16)
    low = (rest - mid.astype(F32)).astype(BF16)
    return high, mid, low


def dot_wide(values, right, right_dim=0):
    high, mid, low = split_three(values)
    return dot(high, right, 1, right_dim) + dot(mid, right, 1, right_dim) + dot(low, right, 1, right_dim)


def dot_wide_rows(left, values):
    high, mid, low = split_three(values)
    return dot(left, high, 0, 0) + dot(left, mid, 0, 0) + dot(left, low, 0, 0)


def norm_stats(out_b):
    values = out_b.astype(F32)
    centered = values - jnp.mean(values, axis=-1, keepdims=True)
    inv_std = lax.rsqrt(jnp.mean(centered * centered, axis=-1, keepdims=True) + NORM_EPS)
    return centered * inv_std, inv_std


def mlp_forward(pre_act, w_two, gain, bias):
    pre_b = pre_act.astype(BF16)
    hidden = jax.nn.silu(pre_b.astype(F32)).astype(BF16)
    out_b = dot(hidden, w_two).astype(BF16)
    normed, _ = norm_stats(out_b)
    return normed * gain + bias, pre_b, out_b


def mlp_cotangents(d_branch, pre_b, out_b, w_two, gain):
    normed, inv_std = norm_stats(out_b)
    d_norm = d_branch * gain
    d_out = (inv_std * (d_norm - jnp.mean(d_norm, axis=-1, keepdims=True) - normed * jnp.mean(d_norm * normed, axis=-1, keepdims=True))).astype(BF16)
    d_act = dot(d_out, w_two, 1, 1).astype(BF16)
    pre_f = pre_b.astype(F32)
    gate = jax.nn.sigmoid(pre_f)
    hidden = (pre_f * gate).astype(BF16)
    d_pre = (d_act.astype(F32) * gate * (1.0 + pre_f * (1.0 - gate))).astype(BF16)
    d_gain = (d_branch * normed).reshape(-1, 8, d_branch.shape[-1]).sum(axis=0)
    d_bias = d_branch.reshape(-1, 8, d_branch.shape[-1]).sum(axis=0)
    return d_out, hidden, d_pre, d_gain, d_bias


def receiver_pick(copies):
    rows = lax.broadcasted_iota(jnp.int32, (TILE, copies * NODE_TILE), 0)
    cols = lax.broadcasted_iota(jnp.int32, (TILE, copies * NODE_TILE), 1)
    return lax.shift_right_logical(rows, 3) == lax.bitwise_and(cols, NODE_TILE - 1)


def as_bf16(flags):
    return jnp.where(flags, 1.0, 0.0).astype(BF16)


def unpack_weights(grid, w_e1, w_e2, w_n1, w_n2, norms):
    def row(p, carry):
        at = (p // 4, lax.rem(p, 4))
        for x in range(0, 4, 2):
            for k in range(4):
                lanes = pl.ds(128 * k, 128)
                for dev in range(2):
                    w_e1[pl.ds(pl.multiple_of(96 * p, 32) + (24 * x + 32 * dev), 16), lanes] = grid[at[0], at[1], x + dev, k]
                    w_n1[pl.ds(pl.multiple_of(64 * p, 64) + 16 * (x + dev), 16), lanes] = grid[at[0], at[1], x + dev, 4 + k]
                for ref, first, tile, top in ((w_e1, pl.multiple_of(96 * p, 32) + (24 * x + 16), 8, 0), (w_e2, pl.multiple_of(32 * p, 32) + 8 * x, 8, 8), (w_n2, pl.multiple_of(32 * p, 32) + 8 * x, 12, 0)):
                    even = grid[at[0], at[1], x, tile + k].astype(F32)[top:top + 8]
                    odd = grid[at[0], at[1], x + 1, tile + k].astype(F32)[top:top + 8]
                    ref[pl.ds(first, 16), lanes] = jnp.concatenate([even, odd], axis=0).astype(BF16)
        return carry
    lax.fori_loop(0, 16, row, 0)
    for k in range(4):
        total = grid[k, 0, 0, 12].astype(F32)
        for d in range(1, 16):
            total = total + grid[k, d // 4, d % 4, 12].astype(F32)
        norms[:, 128 * k:128 * k + 128] = total[8:16]


def fill_columns(snd_rows, mask_rows, snd_col, mask_col):
    for rows, col in ((snd_rows, snd_col), (mask_rows, mask_col)):
        turned = rows[...].astype(F32).T
        for n in range(rows.shape[0]):
            col[128 * n:128 * n + 128, :] = turned[:, n:n + 1]


def pick_senders(snd_col, node_all, rows):
    ids = lax.broadcasted_iota(jnp.int32, (TILE, 512), 1)
    return dot(as_bf16(snd_col[rows].astype(jnp.int32) == ids), node_all[...]).astype(BF16)


def all_senders(snd_col, node_all, out):
    def tile(i, carry):
        rows = pl.ds(pl.multiple_of(i * TILE, TILE), TILE)
        out[rows] = pick_senders(snd_col, node_all, rows)
        return carry
    lax.fori_loop(0, out.shape[0] // TILE, tile, 0)


def edge_forward(layer_io, senders, hook, edge_out, pre_out, out_out, sums_out, w_e1, w_e2, norms, recv_terms):
    node_all, node_own, edge_in, snd_col, mask_col = layer_io
    for part, term in enumerate(split_three(dot(node_own[...], w_e1[1024:1536]))):
        recv_terms[part] = term

    def tile(i, carry):
        rows = pl.ds(pl.multiple_of(i * TILE, TILE), TILE)
        nodes = pl.ds(pl.multiple_of(i * NODE_TILE, NODE_TILE), NODE_TILE)
        sender = pick_senders(snd_col, node_all, rows) if senders is None else senders[rows]
        recv = jnp.concatenate([recv_terms[0, nodes], recv_terms[1, nodes], recv_terms[2, nodes]], axis=0)
        edge = edge_in[rows]
        pre = dot(edge, w_e1[0:512]) + dot(sender, w_e1[512:1024]) + dot(as_bf16(receiver_pick(3)), recv)
        branch, pre_b, out_b = mlp_forward(pre, w_e2[...], norms[0:1], norms[1:2])
        edge_new = (edge.astype(F32) + branch).astype(BF16)
        pre_out[rows] = pre_b
        out_out[rows] = out_b
        if edge_out is not None:
            edge_out[rows] = edge_new
        picked = jnp.where(receiver_pick(1), mask_col[rows], 0.0).astype(BF16)
        sums_out[nodes] = dot(picked, edge_new, 0, 0).astype(BF16)
        hook(i)
        return carry
    lax.fori_loop(0, edge_in.shape[0] // TILE, tile, 0)


def node_forward(node_own, sums, w_n1, w_n2, norms):
    pre = dot(node_own[...], w_n1[0:512]) + dot(sums[...], w_n1[512:1024])
    return mlp_forward(pre, w_n2[...], norms[2:3], norms[3:4])


def lane_tiles(values):
    return [values[:, 128 * k:128 * k + 128].reshape(-1, 8, 128) for k in range(4)]


def tile_at(tile):
    return tile + tile // 8 if tile < 16 else tile + 2


def store_square(grad_ref, values, first_tile):
    for k, tiles in enumerate(lane_tiles(values)):
        grad_ref[:, :, :, tile_at(first_tile + k)] = tiles.reshape(4, 4, 4, 8, 128)


def store_double(grad_ref, values, first_tile, part):
    for k, tiles in enumerate(lane_tiles(values)):
        tiles = tiles.reshape(2, 4, 4, 2, 8, 128)
        for r in range(2):
            grad_ref[2 * part:2 * part + 2, :, :, tile_at(first_tile + 4 * r + k)] = tiles[:, :, :, r]


def store_triple(grad_ref, values, first_pair):
    for n in range(values.shape[0] // 96):
        pair = first_pair + n
        for k, tiles in enumerate(lane_tiles(values[96 * n:96 * n + 96])):
            tiles = tiles.reshape(4, 3, 8, 128)
            for r in range(3):
                grad_ref[pair // 4, pair % 4, :, tile_at(4 * r + k)] = tiles[:, r]


def layer_back(layer_io, d_node_new, d_edge_new, pre_e, out_e, sums, pre_n, out_n, mats, norms, snd_rows, outs, scratch, after_nodes, hook, pass_on):
    node_all, node_own, edge_in, snd_col, mask_col = layer_io
    w_e1, w_e2, w_n1, w_n2 = mats
    grad_ref, d_edge, d_local, scattered = outs
    hidden_s, d_pre_s, d_out_s, d_sum_s, recv_s, gain_s = scratch
    d_out_n, hidden_n, d_pre_n, d_gain_n, d_bias_n = mlp_cotangents(d_node_new, pre_n, out_n, w_n2[...], norms[2:3])
    d_sum_s[...] = dot(d_pre_n, w_n1[512:1024], 1, 1).astype(BF16)
    d_local[...] = d_node_new + dot(d_pre_n, w_n1[0:512], 1, 1)
    store_square(grad_ref, dot(hidden_n, d_out_n, 0, 0), 24)
    store_double(grad_ref, dot(node_own[...], d_pre_n, 0, 0), 16, 0)
    store_double(grad_ref, dot(sums[...], d_pre_n, 0, 0), 16, 1)
    after_nodes()
    gain_s[...] = jnp.zeros_like(gain_s)

    def tile(i, carry):
        rows = pl.ds(pl.multiple_of(i * TILE, TILE), TILE)
        nodes = pl.ds(pl.multiple_of(i * NODE_TILE, NODE_TILE), NODE_TILE)
        pick = receiver_pick(1)
        picked = jnp.where(pick, mask_col[rows], 0.0).astype(BF16)
        d_res = (d_edge_new[rows].astype(F32) + dot(picked, d_sum_s[nodes])).astype(BF16).astype(F32)
        d_out, hidden, d_pre, d_gain, d_bias = mlp_cotangents(d_res, pre_e[rows], out_e[rows], w_e2[...], norms[0:1])
        gain_s[0] = gain_s[0] + d_gain
        gain_s[1] = gain_s[1] + d_bias
        hidden_s[rows] = hidden
        d_out_s[rows] = d_out
        d_pre_s[rows] = d_pre
        d_edge[rows] = d_res.astype(BF16)
        recv_s[nodes] = dot(as_bf16(pick), d_pre, 0, 0)
        hook(i)
        return carry
    lax.fori_loop(0, edge_in.shape[0] // TILE, tile, 0)
    store_square(grad_ref, dot(hidden_s[...], d_out_s[...], 0, 0), 12)
    upper = dot(edge_in[...], d_pre_s[...], 0, 0)
    store_triple(grad_ref, upper[0:480], 0)
    snd_row = jnp.concatenate([snd_rows[n:n + 1] for n in range(snd_rows.shape[0])], axis=1)
    for block in range(4):
        ids = lax.broadcasted_iota(jnp.int32, (128, edge_in.shape[0]), 0) + 128 * block
        scattered[128 * block:128 * block + 128] = dot(as_bf16(snd_row == ids), d_pre_s[...])
    pass_on()
    middle = dot_wide_rows(node_all[...], scattered[...])
    store_triple(grad_ref, jnp.concatenate([upper[480:512], middle[0:448]], axis=0), 5)
    lower = dot_wide_rows(node_own[...], recv_s[...])
    store_triple(grad_ref, jnp.concatenate([middle[448:512], lower], axis=0), 10)
    for part, (gain, bias) in enumerate(((gain_s[0], gain_s[1]), (d_gain_n, d_bias_n))):
        full = jnp.concatenate([gain.sum(axis=0, keepdims=True), bias.sum(axis=0, keepdims=True), jnp.zeros((6, 512), F32)], axis=0)
        for k in range(4):
            grad_ref[k, :, :, 8 + 9 * part] = jnp.broadcast_to(full[:, 128 * k:128 * k + 128], (4, 4, 8, 128))


def layer_back_late(w_e1, d_edge, d_local, scratch):
    d_pre_s, recv_s = scratch[1], scratch[4]

    def tile(i, carry):
        rows = pl.ds(pl.multiple_of(i * TILE, TILE), TILE)
        d_edge[rows] = (d_edge[rows].astype(F32) + dot(d_pre_s[rows], w_e1[0:512], 1, 1)).astype(BF16)
        return carry
    lax.fori_loop(0, d_edge.shape[0] // TILE, tile, 0)
    d_local[...] = d_local[...] + dot_wide(recv_s[...], w_e1[1024:1536], 1)


def half_of(ref, core):
    count = ref.shape[0] // 2
    return ref.at[pl.ds(pl.multiple_of(core * count, count), count)]


def no_hook(i):
    return None


def at_tile(plan):
    def hook(i):
        for tile, stages in plan.items():
            @pl.when(i == tile)
            def _():
                for plan_of, number in stages:
                    plan_of.stage(number)
    return hook


def pack_shard(layer, masters, shard, norm_pad):
    edge_one, edge_two, node_one, node_two, norm_rows = masters
    chip = lax.axis_index('dp')
    odd = lax.rem(chip, 2) == 1
    norm_pad[...] = jnp.zeros_like(norm_pad)
    norm_pad[0:4, 0:8] = norm_rows[layer]
    placed = pltpu.roll(norm_pad[...], lax.rem(chip, 16) * 8, 1)
    for k in range(4):
        lanes = slice(128 * k, 128 * k + 128)
        first, mid, last = edge_one[layer, 0:8, lanes], edge_one[layer, 8:16, lanes], edge_one[layer, 16:24, lanes]
        shard[k] = jnp.concatenate([jnp.where(odd, mid, first), jnp.where(odd, last, mid)], axis=0).astype(BF16)
        shard[4 + k] = node_one[layer, :, lanes].astype(BF16)
        shard[8 + k] = jnp.concatenate([jnp.where(odd, first, last), edge_two[layer, :, lanes]], axis=0).astype(BF16)
        shard[12 + k] = jnp.concatenate([node_two[layer, :, lanes], placed if k == 0 else jnp.zeros_like(placed)], axis=0).astype(BF16)


def node_cotangent(d_local, scattered, returned, w_above, core):
    return (d_local[...] + dot_wide(half_of(scattered, core)[...] + returned[...], w_above[512:1024], 1)).astype(BF16)


def pack_kernel(edge_one, edge_two, node_one, node_two, norm_rows, shard_low, shard_high, norm_pad):
    for layer, shard in enumerate((shard_low, shard_high)):
        pack_shard(layer, (edge_one, edge_two, node_one, node_two, norm_rows), shard, norm_pad)


def pack_call(masters):
    spec = pl.BlockSpec(memory_space=pltpu.VMEM)
    shard = jax.ShapeDtypeStruct((16, 16, 128), BF16)
    return pl.pallas_call(pack_kernel, out_shape=[shard, shard], in_specs=[spec] * 5, out_specs=[spec] * 2, scratch_shapes=[pltpu.VMEM((8, 128), F32)], compiler_params=pltpu.CompilerParams(vmem_limit_bytes=67043328), name='pack')(*masters)


def step_kernel(shard_low, shard_high, node_in, snd_rows, mask_rows, node_cot, edge_lat, edge_cot, grad_node, edge_out, total, d_edge, node_all, node_all_one, edge_in, pre_low, out_low, pre_high, out_high, d_pre, snd_col, mask_col, sums_low, sums_high, pre_node, out_node, recv_terms, d_sum, recv_sum, gain_sum, d_local, scattered_high, scattered_low, returned_high, returned_low, *rest):
    mats_low, norms_low, mats_high, norms_high = rest[0:4], rest[4], rest[5:9], rest[9]
    load_sem, credit_sem, peer_sem, send_sem, recv_sem = rest[10:]
    wire = Wire(send_sem, recv_sem)
    load_edge = lambda n: pltpu.make_async_copy(edge_lat, edge_in, load_sem.at[n])
    load_cot = lambda: pltpu.make_async_copy(edge_cot, d_edge, load_sem.at[1])
    store_edge = lambda: pltpu.make_async_copy(d_edge, edge_out, load_sem.at[3])
    load_edge(0).start()
    load_cot().start()

    def begin():
        place = Place()
        node_own = half_of(node_all, place.core)
        node_own_one = half_of(node_all_one, place.core)
        return place, (node_all, node_own, edge_in, snd_col, mask_col), (node_all_one, node_own_one, edge_in, snd_col, mask_col)

    def gather_and_first(grid_low, grid_high):
        place, low_io, high_io = begin()
        node_own, node_own_one = low_io[1], high_io[1]
        for shard, grid in ((shard_low, grid_low), (shard_high, grid_high)):
            grid[place.at[0], place.at[1], place.at[2]] = shard[...]
        node_own[...] = node_in[...]
        place.barrier()
        low = Gather('low', place, wire, shard_low, grid_low)
        high = Gather('high', place, wire, shard_high, grid_high)
        low.stage(0)
        high.stage(0)
        wire.start('node', lambda: node_in, lambda: half_of(node_all, place.core), place.partner)
        fill_columns(snd_rows, mask_rows, snd_col, mask_col)
        low.stage(1)
        high.stage(1)
        low.stage(2)
        wire.wait_recv('node')
        all_senders(snd_col, node_all, d_pre)
        low.stage(3)
        high.stage(2)
        low.stage(4)
        low.stage(5)
        unpack_weights(grid_low, *mats_low, norms_low)
        load_edge(0).wait()
        hook = at_tile({0: [(high, 3)], 2: [(high, 4)]})
        edge_forward(low_io, d_pre, hook, edge_in, pre_low, out_low, sums_low, mats_low[0], mats_low[1], norms_low, recv_terms)
        branch, pre_b, out_b = node_forward(node_own, sums_low, mats_low[2], mats_low[3], norms_low)
        pre_node[...] = pre_b
        out_node[...] = out_b
        node_own_one[...] = (node_own[...].astype(F32) + branch).astype(BF16)
        piece = lambda: half_of(node_all_one, place.core)
        wire.start('node_one', piece, piece, place.partner)
        high.stage(5)
        unpack_weights(grid_high, *mats_high, norms_high)
        wire.wait_recv('node_one')
        wire.finish()
        wire.parts.clear()

    def second_and_back(grad_high, grad_low, theirs_edge, theirs_node, *boxes):
        place, low_io, high_io = begin()
        node_own_one = high_io[1]
        peers = place.peers()
        for peer in peers:
            pl.semaphore_signal(peer_sem, inc=1, device_id=peer, device_id_type=MESH_ID)
        high_node = Reduce('high_node', place, wire, grad_high, 18, 12, (theirs_node,) + boxes[0:9], total, 24)
        high_edge = Reduce('high_edge', place, wire, grad_high, 0, 18, (theirs_edge,) + boxes[9:18], total, 0)
        low_node = Reduce('low_node', place, wire, grad_low, 18, 12, (theirs_node,) + boxes[18:27], total, 9)
        low_edge = Reduce('low_edge', place, wire, grad_low, 0, 18, (theirs_edge,) + boxes[27:36], total, 15)
        edge_forward(high_io, None, no_hook, None, pre_high, out_high, sums_high, mats_high[0], mats_high[1], norms_high, recv_terms)
        _, pre_n, out_n = node_forward(node_own_one, sums_high, mats_high[2], mats_high[3], norms_high)
        load_cot().wait()

        def pass_on_high():
            wire.start('scattered_high', lambda: half_of(scattered_high, 1 - place.core), lambda: returned_high, place.partner)

        def after_nodes_high():
            pl.semaphore_wait(peer_sem, len(peers))
            high_node.stage(0)
        hook = at_tile({1: [(high_node, 1)], 2: [(high_node, 2), (Credit(place, credit_sem.at[0]), 0)]})
        scratch = (pre_high, d_pre, out_high, d_sum, recv_sum, gain_sum)
        layer_back(high_io, node_cot[...].astype(F32), d_edge, pre_high, out_high, sums_high, pre_n, out_n, mats_high, norms_high, snd_rows, (grad_high, d_edge, d_local, scattered_high), scratch, after_nodes_high, hook, pass_on_high)
        load_edge(2).start()
        high_edge.stage(0)
        high_node.stage(3)
        layer_back_late(mats_high[0], d_edge, d_local, scratch)
        high_node.stage(5)
        wire.wait_recv('scattered_high')
        d_node = node_cotangent(d_local, scattered_high, returned_high, mats_high[0], place.core).astype(F32)
        load_edge(2).wait()

        def pass_on_low():
            wire.start('scattered_low', lambda: half_of(scattered_low, 1 - place.core), lambda: returned_low, place.partner)

        def after_nodes_low():
            high_edge.stage(1)
            pl.semaphore_wait(credit_sem.at[0], 1)
            low_node.stage(0)
        hook = at_tile({0: [(high_node, 6)], 1: [(low_node, 1)], 2: [(high_edge, 2), (Credit(place, credit_sem.at[1]), 0)]})
        scratch = (pre_low, d_pre, out_low, d_sum, recv_sum, gain_sum)
        layer_back(low_io, d_node, d_edge, pre_low, out_low, sums_low, pre_node[...], out_node[...], mats_low, norms_low, snd_rows, (grad_low, d_edge, d_local, scattered_low), scratch, after_nodes_low, hook, pass_on_low)
        pl.semaphore_wait(credit_sem.at[1], 1)
        low_edge.stage(0)
        high_edge.stage(3)
        low_node.stage(2)
        low_edge.stage(1)
        layer_back_late(mats_low[0], d_edge, d_local, scratch)
        store_edge().start()
        high_edge.stage(4)
        low_node.stage(3)
        wire.wait_recv('scattered_low')
        grad_node[...] = node_cotangent(d_local, scattered_low, returned_low, mats_low[0], place.core)
        low_edge.stage(2)
        high_edge.stage(5)
        low_node.stage(4)
        low_edge.stage(3)
        low_node.stage(5)
        high_edge.stage(6)
        low_edge.stage(4)
        low_node.stage(6)
        low_edge.stage(5)
        low_edge.stage(6)
        for plan in (high_node, high_edge, low_node, low_edge):
            plan.stage(7)
        store_edge().wait()
        wire.finish()

    grid = pltpu.VMEM((RING, RING, RING, 16, 16, 128), BF16)
    pl.run_scoped(gather_and_first, grid, grid)
    grad = pltpu.VMEM((RING, RING, RING, 30, 8, 128), F32)
    theirs = [pltpu.VMEM((RING, RING, RING, count, 8, 128), F32) for count in (9, 6)]
    boxes = [pltpu.VMEM(shape, F32) for count in (6, 9, 6, 9) for shape in box_shapes(count)]
    pl.run_scoped(second_and_back, grad, grad, *theirs, *boxes)


def step_call(vmem_inputs, hbm_inputs):
    spec = pl.BlockSpec(memory_space=pltpu.VMEM)
    anywhere = pl.BlockSpec(memory_space=pl.ANY)
    edge = ((2048, 512), BF16)
    node = ((256, 512), BF16)
    nodes = ((512, 512), BF16)
    column = ((2048, 1), F32)
    node_wide = ((256, 512), F32)
    nodes_wide = ((512, 512), F32)
    mats = [((1536, 512), BF16), ((512, 512), BF16), ((1024, 512), BF16), ((512, 512), BF16), ((8, 512), F32)]
    scratch = [edge, nodes, nodes, edge, edge, edge, edge, edge, edge, column, column, node, node, node, node, ((3, 256, 512), BF16), node, node_wide, ((2, 8, 512), F32), node_wide, nodes_wide, nodes_wide, node_wide, node_wide] + mats + mats
    copies = 2 * GATHER_COPIES + 4 * REDUCE_COPIES + 4
    return pl.pallas_call(
        step_kernel,
        out_shape=[jax.ShapeDtypeStruct(*node), jax.ShapeDtypeStruct(*edge), jax.ShapeDtypeStruct((2, 30, 8, 128), F32)],
        in_specs=[spec] * len(vmem_inputs) + [anywhere] * len(hbm_inputs),
        out_specs=[spec, anywhere, spec],
        scratch_shapes=[pltpu.VMEM(*entry) for entry in scratch] + [pltpu.SemaphoreType.DMA((4,)), pltpu.SemaphoreType.REGULAR((2,)), pltpu.SemaphoreType.REGULAR, pltpu.SemaphoreType.DMA((copies,)), pltpu.SemaphoreType.DMA((copies,))],
        compiler_params=pltpu.CompilerParams(collective_id=1, has_side_effects=True, vmem_limit_bytes=67043328),
        cost_estimate=pl.CostEstimate(flops=27 * 10 ** 9, bytes_accessed=20 * 2 ** 20, transcendentals=0),
        name='train_step',
    )(*vmem_inputs, *hbm_inputs)


def update_kernel(total, node_in, edge_in, *refs):
    refs[-2][...] = node_in[...]
    refs[-1][...] = edge_in[...]
    masters, ones, twos, new_masters, new_ones, new_twos = [refs[5 * n:5 * n + 5] for n in range(6)]

    def apply(slot, index, grad):
        master, one, two = adamw_update(masters[slot][index], grad, ones[slot][index], twos[slot][index])
        new_masters[slot][index] = master
        new_ones[slot][index] = one
        new_twos[slot][index] = two

    shift = lax.rem(16 - lax.rem(lax.axis_index('dp'), 16), 16) * 8
    for layer in range(2):
        edge_first = 15 if layer == 0 else 0
        for slot, (first, rows) in enumerate(((0, 3), (12, 1), (16, 2), (24, 1))):
            for r in range(rows):
                for k in range(4):
                    tile = first + 4 * r + k
                    if tile < 16:
                        grad = total[tile // 8, edge_first + tile % 8]
                    else:
                        grad = total[(tile - 16) // 6, 9 + 15 * layer + (tile - 16) % 6]
                    apply(slot, (layer, slice(8 * r, 8 * r + 8), slice(128 * k, 128 * k + 128)), grad)
        for part in range(2):
            turned = pltpu.roll(total[part, edge_first + 8], shift, 1)
            apply(4, (layer, slice(2 * part, 2 * part + 2), slice(0, 8)), turned[0:2, 0:8])


def update_call(total, grad_node, grad_edge, masters, ones, twos):
    spec = pl.BlockSpec(memory_space=pltpu.VMEM)
    shapes = [jax.ShapeDtypeStruct(array.shape, array.dtype) for array in masters + ones + twos + (grad_node, grad_edge)]
    return tuple(pl.pallas_call(update_kernel, out_shape=shapes, in_specs=[spec] * 18, out_specs=[spec] * 17, compiler_params=pltpu.CompilerParams(vmem_limit_bytes=67043328), name='update')(total, grad_node, grad_edge, *masters, *ones, *twos))


def adamw_update(master, grad_sum, moment_one, moment_two):
    corr_one = 1.0 - BETA_ONE ** STEP
    corr_two = 1.0 - BETA_TWO ** STEP
    one_new = BETA_ONE * moment_one + (1.0 - BETA_ONE) * grad_sum
    two_new = BETA_TWO * moment_two + (1.0 - BETA_TWO) * grad_sum * grad_sum
    direction = (one_new / corr_one) / (jnp.sqrt(two_new / corr_two) + ADAM_EPS)
    return master - LEARN_RATE * (direction + DECAY * master), one_new, two_new


def solution(mesh):
    lat_spec = P('dp', 'sp', None)
    edge_spec = P('sp')
    mat_spec = P(None, 'dp', None)
    norm_spec = P(None, None, 'dp')
    param_specs = (mat_spec, mat_spec, mat_spec, mat_spec, norm_spec)

    def train_step(node_lat, edge_lat, senders, edge_mask, node_cot, edge_cot, *params):
        masters, ones, twos = params[0:5], params[5:10], params[10:15]
        snd_rows = senders.reshape(-1, 128)
        mask_rows = edge_mask.reshape(-1, 128)
        grad_node, grad_edge, total = step_call(tuple(pack_call(masters)) + (node_lat[0], snd_rows, mask_rows, node_cot[0]), (edge_lat[0], edge_cot[0]))
        outs = update_call(total, grad_node, grad_edge, masters, ones, twos)
        return outs[:15] + (outs[15][None], outs[16][None])

    return jax.shard_map(train_step, mesh=mesh, in_specs=(lat_spec, lat_spec, edge_spec, edge_spec, lat_spec, lat_spec) + param_specs + param_specs + param_specs, out_specs=param_specs + param_specs + param_specs + (lat_spec, lat_spec), check_vma=False)
```
